32 devices in a mesh: gx: 2 (over y), gy: 4 (over z), gz: 4 (over x, core).
Axes of the slice: x: 2, y: 2, z: 4, core: 2. Of those that a mesh axis runs over, the one named last changes fastest.
Arguments:
- section: float32 [25, 8, 64, 256], P(None, 'gz', 'gy', 'gx'), may hold values from -0.4 to 1.4, as said below
- base: float32 [25, 8, 64, 256], P(None, 'gz', 'gy', 'gx'), may hold values from -0.4 to 1.4, as said below
- accum: float32 [25, 8, 64, 256], P(None, 'gz', 'gy', 'gx'), may hold values from -4 to 4
Outputs:
- next_section: float32 [25, 8, 64, 256], P(None, 'gz', 'gy', 'gx')
- next_accum: float32 [25, 8, 64, 256], P(None, 'gz', 'gy', 'gx')
- slab: float32 [25, 8, 64, 256], P(None, 'gz')
The draws below stay inside these ranges and needn't reach their ends.
Inputs may be any that keep to these rules, and one draw needn't show every extreme that they name: `section`: fields 0 and 17 (conformal factor and lapse) lie in 0.6 to 1.4; fields 1, 4 and 6 (the metric's diagonal) lie within 0.4 of 1; all other fields lie within 0.4 of 0. `base`: fields 0 and 17 (conformal factor and lapse) lie in 0.6 to 1.4; fields 1, 4 and 6 (the metric's diagonal) lie within 0.4 of 1; all other fields lie within 0.4 of 0.
All inputs are finite; a program needn't handle non-finite values.
Results may differ from the reference program's by a relative error of at most 0.0003.
Values sent between devices are 32-bit elements; how exact they have to be, the bound alone decides.
A program may use at most 64 MiB of HBM per device.

```python
import jax
import jax.numpy as jnp
from jax import lax

FIELDS = 25
CZ = 2
NZ = 8
NY = 64
NX = 256
N_GZ = 4


def draw_fields(key):
    subkeys = jax.random.split(key, 2)
    full_shape = (FIELDS, NZ, NY, NX)
    jitter = jnp.clip(0.1 * jax.random.normal(subkeys[0], full_shape, jnp.float32), -0.4, 0.4)
    positive = 1.0 + jnp.clip(0.15 * jax.random.normal(subkeys[1], full_shape, jnp.float32), -0.4, 0.4)
    field_slot = lax.broadcasted_iota(jnp.int32, full_shape, 0)
    unit_diag = (field_slot == 1) | (field_slot == 4) | (field_slot == 6)
    kept_positive = (field_slot == 0) | (field_slot == 17)
    values = jnp.where(unit_diag, 1.0 + jitter, jitter)
    return jnp.where(kept_positive, positive, values)


def draw_section(key, part):
    return draw_fields(jax.random.fold_in(key, 11))


def draw_base(key, part):
    return draw_fields(jax.random.fold_in(key, 23))


def shard_levels(key, dims, shards, smallest, high):
    gain, own = 1.0, jax.random.fold_in(key, 6)
    for dim, blocks in shards:
        steps = jnp.exp(jax.random.uniform(jax.random.fold_in(own, dim), (blocks,), jnp.float32, smallest / len(shards), high / len(shards)))
        gain = gain * jnp.repeat(steps, dims[dim] // blocks).reshape([-1 if axis == dim else 1 for axis in range(len(dims))])
    return gain


def centred(rng, shape, spread, reach, pieces=(), held_as=jnp.bfloat16):
    entries = jax.random.normal(rng, shape, jnp.float32) * spread
    if len(pieces) > 0:
        entries = shard_levels(rng, shape, pieces, -0.22, 0.18) * entries
    return jnp.clip(entries, min=-reach, max=reach).astype(held_as)


def setup_inputs(seed: int = 0) -> dict:
    streams_of = jax.random.split(jax.random.key(seed), 4)
    section = draw_section(jax.random.fold_in(streams_of[3], 71), 0)
    base = draw_base(jax.random.fold_in(streams_of[3], 71), 0)
    accum = centred(streams_of[2], (FIELDS, NZ, NY, NX), 0.5, 4.0, ((1, 4), (2, 4), (3, 2)), jnp.float32)
    return dict(section=section, base=base, accum=accum)


STEP_DT = 0.25
SPACING = 1.0
DISSIPATE = 0.1
DRIVER_ETA = 2.0
KAPPA_ONE = 0.1
FIRST_TAPS = (1.0 / 12.0, -8.0 / 12.0, 0.0, 8.0 / 12.0, -1.0 / 12.0)
SECOND_TAPS = (-1.0 / 12.0, 16.0 / 12.0, -30.0 / 12.0, 16.0 / 12.0, -1.0 / 12.0)
FOURTH_TAPS = (1.0, -4.0, 6.0, -4.0, 1.0)
PAIR_SLOT = ((0, 1, 2), (1, 3, 4), (2, 4, 5))
PAIR_LIST = ((0, 0), (0, 1), (0, 2), (1, 1), (1, 2), (2, 2))


def window(padded, shifts):
    interior = (padded.shape[1] - 4, padded.shape[2] - 4, padded.shape[3] - 4)
    corner = (2 + shifts[2], 2 + shifts[1], 2 + shifts[0])
    return padded[:, corner[0]:corner[0] + interior[0], corner[1]:corner[1] + interior[1], corner[2]:corner[2] + interior[2]]


def moved(direction, amount):
    shifts = [0, 0, 0]
    shifts[direction] = amount
    return shifts


def line_sum(padded, direction, weights):
    running = None
    for position in range(5):
        if weights[position] != 0.0:
            weighted = weights[position] * window(padded, moved(direction, position - 2))
            running = weighted if running is None else running + weighted
    return running


def cross_sum(padded, first_dir, second_dir):
    running = None
    for first_pos in range(5):
        for second_pos in range(5):
            factor = FIRST_TAPS[first_pos] * FIRST_TAPS[second_pos]
            if factor != 0.0:
                shifts = [0, 0, 0]
                shifts[first_dir] = first_pos - 2
                shifts[second_dir] = second_pos - 2
                weighted = factor * window(padded, shifts)
                running = weighted if running is None else running + weighted
    return running


def evolve_rate(padded):
    centre = window(padded, (0, 0, 0))
    gradients = [line_sum(padded, direction, FIRST_TAPS) / SPACING for direction in range(3)]
    curves = [line_sum(padded, direction, SECOND_TAPS) / (SPACING * SPACING) for direction in range(3)]
    smoothing = line_sum(padded, 0, FOURTH_TAPS) + line_sum(padded, 1, FOURTH_TAPS) + line_sum(padded, 2, FOURTH_TAPS)
    chosen = jnp.concatenate([padded[0:1], padded[17:21]], axis=0)
    mixed_terms = {}
    for dir_pair in ((0, 1), (0, 2), (1, 2)):
        mixed_terms[dir_pair] = cross_sum(chosen, dir_pair[0], dir_pair[1]) / (SPACING * SPACING)

    def second_of(chosen_slot, field_slot, axis_one, axis_two):
        if axis_one == axis_two:
            return curves[axis_one][field_slot]
        return mixed_terms[(min(axis_one, axis_two), max(axis_one, axis_two))][chosen_slot]

    def metric_of(axis_one, axis_two):
        return centre[1 + PAIR_SLOT[axis_one][axis_two]]

    def traceless_of(axis_one, axis_two):
        return centre[8 + PAIR_SLOT[axis_one][axis_two]]

    def inverse_of(axis_one, axis_two):
        return (2.0 if axis_one == axis_two else 0.0) - metric_of(axis_one, axis_two)

    def advect(field_slot):
        return centre[18] * gradients[0][field_slot] + centre[19] * gradients[1][field_slot] + centre[20] * gradients[2][field_slot]

    conformal = centre[0]
    trace_curv = centre[7]
    lapse_field = centre[17]
    theta_field = centre[24]
    divergence = gradients[0][18] + gradients[1][19] + gradients[2][20]
    lap_conformal = curves[0][0] + curves[1][0] + curves[2][0]
    squares_a = sum(traceless_of(axis_one, axis_two) ** 2 for axis_one in range(3) for axis_two in range(3))

    def lapse_dd(axis_one, axis_two):
        return second_of(1, 17, axis_one, axis_two)

    ricci_table = []
    for axis_one, axis_two in PAIR_LIST:
        field_slot = 1 + PAIR_SLOT[axis_one][axis_two]
        flat_part = curves[0][field_slot] + curves[1][field_slot] + curves[2][field_slot]
        conformal_part = second_of(0, 0, axis_one, axis_two) + (lap_conformal if axis_one == axis_two else 0.0)
        ricci_table.append(-0.5 * flat_part + 0.5 * (gradients[axis_one][14 + axis_two] + gradients[axis_two][14 + axis_one]) + conformal_part / (2.0 * conformal))

    def ricci_of(axis_one, axis_two):
        return ricci_table[PAIR_SLOT[axis_one][axis_two]]

    ricci_scalar = conformal * sum(inverse_of(axis_one, axis_two) * ricci_of(axis_one, axis_two) for axis_one in range(3) for axis_two in range(3))
    lapse_trace = sum(inverse_of(axis_one, axis_two) * lapse_dd(axis_one, axis_two) for axis_one in range(3) for axis_two in range(3))

    rates = [None] * 25
    rates[0] = advect(0) + (2.0 / 3.0) * conformal * (lapse_field * trace_curv - divergence)
    for axis_one, axis_two in PAIR_LIST:
        field_slot = PAIR_SLOT[axis_one][axis_two]
        lie_part = sum(metric_of(axis_one, axis_sum) * gradients[axis_two][18 + axis_sum] + metric_of(axis_two, axis_sum) * gradients[axis_one][18 + axis_sum] for axis_sum in range(3))
        rates[1 + field_slot] = advect(1 + field_slot) - 2.0 * lapse_field * traceless_of(axis_one, axis_two) + lie_part - (2.0 / 3.0) * metric_of(axis_one, axis_two) * divergence
    rates[7] = advect(7) - conformal * lapse_trace + lapse_field * (squares_a + trace_curv * trace_curv / 3.0) + KAPPA_ONE * lapse_field * theta_field

    def source_of(axis_one, axis_two):
        return -lapse_dd(axis_one, axis_two) + lapse_field * ricci_of(axis_one, axis_two)

    trace_part = sum(inverse_of(axis_one, axis_two) * source_of(axis_one, axis_two) for axis_one in range(3) for axis_two in range(3))
    for axis_one, axis_two in PAIR_LIST:
        field_slot = PAIR_SLOT[axis_one][axis_two]
        free_part = source_of(axis_one, axis_two) - metric_of(axis_one, axis_two) * trace_part / 3.0
        product_part = sum(traceless_of(axis_one, axis_sum) * traceless_of(axis_sum, axis_two) for axis_sum in range(3))
        lie_part = sum(traceless_of(axis_one, axis_sum) * gradients[axis_two][18 + axis_sum] + traceless_of(axis_two, axis_sum) * gradients[axis_one][18 + axis_sum] for axis_sum in range(3))
        rates[8 + field_slot] = (advect(8 + field_slot) + conformal * free_part
                                 + lapse_field * (trace_curv * traceless_of(axis_one, axis_two) - 2.0 * product_part)
                                 + lie_part - (2.0 / 3.0) * traceless_of(axis_one, axis_two) * divergence)
    for axis_one in range(3):
        gauge_part = (-2.0 * sum(traceless_of(axis_one, axis_two) * gradients[axis_two][17] for axis_two in range(3))
                      + 2.0 * lapse_field * (-(2.0 / 3.0) * sum(inverse_of(axis_one, axis_two) * gradients[axis_two][7] for axis_two in range(3))
                                             - 1.5 * sum(traceless_of(axis_one, axis_two) * gradients[axis_two][0] for axis_two in range(3)) / conformal)
                      + curves[0][18 + axis_one] + curves[1][18 + axis_one] + curves[2][18 + axis_one]
                      + sum(second_of(2 + axis_two, 18 + axis_two, axis_one, axis_two) for axis_two in range(3)) / 3.0
                      + (2.0 / 3.0) * centre[14 + axis_one] * divergence
                      - sum(centre[14 + axis_two] * gradients[axis_two][18 + axis_one] for axis_two in range(3)))
        rates[14 + axis_one] = advect(14 + axis_one) + gauge_part
        rates[18 + axis_one] = advect(18 + axis_one) + 0.75 * centre[21 + axis_one]
        rates[21 + axis_one] = advect(21 + axis_one) + gauge_part - DRIVER_ETA * centre[21 + axis_one]
    rates[17] = advect(17) - 2.0 * lapse_field * (trace_curv - 2.0 * theta_field)
    rates[24] = (advect(24) + 0.5 * lapse_field * (ricci_scalar + (2.0 / 3.0) * trace_curv * trace_curv - squares_a)
                 - 2.0 * KAPPA_ONE * lapse_field * theta_field)
    return jnp.stack(rates, axis=0) + (-DISSIPATE / 16.0) * smoothing


def reference(section, base, accum):
    padded = jnp.pad(section, ((0, 0), (2, 2), (2, 2), (2, 2)), mode="wrap")

    def one_block(block_index):
        start_plane = (block_index * CZ).astype(jnp.int32)
        piece_block = lax.dynamic_slice_in_dim(padded, start_plane, CZ + 4, 1)
        return evolve_rate(piece_block)

    blocks = lax.map(one_block, jnp.arange(N_GZ, dtype=jnp.int32))
    rates = jnp.moveaxis(blocks, 0, 1).reshape(FIELDS, NZ, NY, NX)
    next_section = base + (0.5 * STEP_DT) * rates
    next_accum = accum + (STEP_DT / 3.0) * rates
    return next_section, next_accum, next_section
```

```python
import functools

import jax
import jax.numpy as jnp
from jax import lax
from jax.experimental import pallas as pl
from jax.experimental.pallas import tpu as pltpu
from jax.sharding import PartitionSpec as P

STEP_DT = 0.25
DISSIPATE = 0.1
DRIVER_ETA = 2.0
KAPPA_ONE = 0.1
PAIR_SLOT = ((0, 1, 2), (1, 3, 4), (2, 4, 5))
PAIR_LIST = ((0, 0), (0, 1), (0, 2), (1, 1), (1, 2), (2, 2))
MESH = pl.DeviceIdType.MESH
RUNS = ((17, 4), (0, 8), (14, 3), (8, 6), (21, 4))
ORDER = tuple(first + n for first, size in RUNS for n in range(size))
PLACE = tuple(ORDER.index(field) for field in range(len(ORDER)))
MIXED = (17, 18, 19, 20, 0)
SIZES = (1, 4, 3, 3, 2, 4, 4, 4)
STAGES = len(SIZES)
FIRST = tuple(sum(SIZES[:s]) for s in range(STAGES + 1))
MIX_STAGE = 4
TURNED = 3
TURN_LAG = 6
Y_GROUPS = ((0, 1), (1, 2), (2, STAGES))
PAD = 8


def first_of(m2, m1, p1, p2):
    return (8.0 / 12.0) * (p1 - m1) - (1.0 / 12.0) * (p2 - m2)


def rates_of_plane(plane, rows, lanes, xb, tb, emit):
    lane = lax.broadcasted_iota(jnp.int32, (rows, lanes), 1)
    quad = lane & 3
    edge_one = (lane < 1) | (lane >= lanes - 1)
    edge_two = (lane < 2) | (lane >= lanes - 2)

    def cell(field, dz=0, dy=0):
        return xb[PLACE[field], plane + 2 + dz, PAD + dy : PAD + dy + rows, :]

    def strip(dz=0, dy=0):
        def side(slot):
            return tb[slot, plane + 2 + dz, PAD + dy : PAD + dy + rows, :]

        if tb.shape[0] == 1:
            return side(0)
        return jnp.where(quad < 2, side(1), side(0))

    def inner(edge):
        return jnp.where(
            quad == 1, pltpu.roll(edge, 1, 1), pltpu.roll(edge, lanes - 1, 1)
        )

    def x_line(field, value, edge, edge_in):
        turn = (lanes - 2 - 4 * field) % lanes
        two = pltpu.roll(edge, turn, 1)
        one = pltpu.roll(edge_in, turn, 1)
        m2 = jnp.where(edge_two & (lane < 64), two, pltpu.roll(value, 2, 1))
        m1 = jnp.where(edge_one & (lane < 64), one, pltpu.roll(value, 1, 1))
        p1 = jnp.where(edge_one & (lane >= 64), one, pltpu.roll(value, lanes - 1, 1))
        p2 = jnp.where(edge_two & (lane >= 64), two, pltpu.roll(value, lanes - 2, 1))
        return m2, m1, p1, p2

    def y_line(read):
        return tuple(read(0, dy) for dy in (-2, -1, 1, 2))

    def z_line(read):
        return tuple(read(dz, 0) for dz in (-2, -1, 1, 2))

    edge = strip()
    edge_in = inner(edge)

    centre, grad, curve, lap, mixed = {}, {}, {}, {}, {}
    need_lap = (0, 1, 2, 3, 4, 5, 6, 17, 18, 19, 20)
    shift = [cell(18), cell(19), cell(20)]
    advected = {}
    for field in range(len(ORDER)):
        centre[field] = cell(field)

    def differentiate(field):
        value = centre[field]
        read = functools.partial(cell, field)
        lines = [x_line(field, value, edge, edge_in), y_line(read), z_line(read)]
        near = [m1 + p1 for _, m1, p1, _ in lines]
        far = [m2 + p2 for m2, _, _, p2 in lines]
        near_sum = near[0] + near[1] + near[2]
        far_sum = far[0] + far[1] + far[2]
        smooth = far_sum - 4.0 * near_sum + 18.0 * value
        grads = [first_of(*line) for line in lines]
        grad[field] = grads
        advected[field] = (
            shift[0] * grads[0] + shift[1] * grads[1] + shift[2] * grads[2]
            - (DISSIPATE / 16.0) * smooth
        )
        if field in need_lap:
            lap[field] = (16.0 / 12.0) * near_sum - (1.0 / 12.0) * far_sum - 7.5 * value
        if field in MIXED:
            for axis in range(3):
                if field in (0, 17) or field == 18 + axis:
                    curve[field, axis] = (
                        (16.0 / 12.0) * near[axis] - (1.0 / 12.0) * far[axis] - 2.5 * value
                    )

    def mix():
        edge_y = first_of(*y_line(strip))
        edge_y_in = inner(edge_y)
        edge_z = first_of(*z_line(strip))
        edge_z_in = inner(edge_z)
        for field in MIXED:
            grads = grad[field]
            if field != 20:
                mixed[field, 0, 1] = first_of(*x_line(field, grads[1], edge_y, edge_y_in))
            if field != 19:
                mixed[field, 0, 2] = first_of(*x_line(field, grads[2], edge_z, edge_z_in))
            if field != 18:
                mixed[field, 1, 2] = first_of(
                    *(
                        first_of(*(cell(field, dz, dy) for dy in (-2, -1, 1, 2)))
                        for dz in (-2, -1, 1, 2)
                    )
                )

    def second(field, one, two):
        if one == two:
            return curve[field, one]
        return mixed[field, min(one, two), max(one, two)]

    def sym(table, one, two):
        return table[PAIR_SLOT[one][two]]

    metric = [centre[1 + k] for k in range(6)]
    traceless = [centre[8 + k] for k in range(6)]
    inverse = [
        (2.0 - metric[k]) if one == two else -metric[k]
        for k, (one, two) in enumerate(PAIR_LIST)
    ]

    def contract(left, right):
        diag = left[0] * right[0] + left[3] * right[3] + left[5] * right[5]
        off = left[1] * right[1] + left[2] * right[2] + left[4] * right[4]
        return diag + 2.0 * off

    def lie_of(table, one, two):
        total = None
        for k in range(3):
            if one == two:
                term = 2.0 * (sym(table, one, k) * grad[18 + k][one])
            else:
                term = (
                    sym(table, one, k) * grad[18 + k][two]
                    + sym(table, two, k) * grad[18 + k][one]
                )
            total = term if total is None else total + term
        return total

    def begin(stage):
        for field in ORDER[FIRST[stage] : FIRST[stage + 1]]:
            differentiate(field)

    chi, trace, lapse, theta = centre[0], centre[7], centre[17], centre[24]

    begin(0)
    emit(17, advected[17] - 2.0 * lapse * (trace - 2.0 * theta))
    yield

    begin(1)
    div = grad[18][0] + grad[19][1] + grad[20][2]
    third_div = (2.0 / 3.0) * div
    for one in range(3):
        emit(18 + one, advected[18 + one] + 0.75 * centre[21 + one])
    emit(0, advected[0] + (2.0 / 3.0) * chi * (lapse * trace) - chi * third_div)
    yield

    def metric_rate(k):
        one, two = PAIR_LIST[k]
        emit(
            1 + k,
            advected[1 + k]
            - 2.0 * lapse * traceless[k]
            + lie_of(metric, one, two)
            - metric[k] * third_div,
        )

    for stage in (2, 3):
        begin(stage)
        for field in ORDER[FIRST[stage] : FIRST[stage + 1]]:
            metric_rate(field - 1)
        yield

    begin(4)
    mix()
    over_chi = 1.0 / chi
    half_over = 0.5 * over_chi
    squares = contract(traceless, traceless)
    lapse_dd = [second(17, one, two) for one, two in PAIR_LIST]
    lapse_trace = contract(inverse, lapse_dd)
    emit(
        7,
        advected[7]
        - chi * lapse_trace
        + lapse * (squares + trace * trace * (1.0 / 3.0))
        + KAPPA_ONE * lapse * theta,
    )
    gauges = []

    def connection_rate(one):
        a_lapse = sum(sym(traceless, one, k) * grad[17][k] for k in range(3))
        a_chi = sum(sym(traceless, one, k) * grad[0][k] for k in range(3))
        g_trace = sum(sym(inverse, one, k) * grad[7][k] for k in range(3))
        b_mixed = sum(second(18 + k, one, k) for k in range(3))
        g_shift = sum(centre[14 + k] * grad[18 + one][k] for k in range(3))
        gauge = (
            -2.0 * a_lapse
            - lapse * ((4.0 / 3.0) * g_trace + 3.0 * (a_chi * over_chi))
            + lap[18 + one]
            + b_mixed * (1.0 / 3.0)
            + centre[14 + one] * third_div
            - g_shift
        )
        gauges.append(gauge)
        emit(14 + one, advected[14 + one] + gauge)

    connection_rate(0)
    yield

    begin(5)
    connection_rate(1)
    connection_rate(2)
    ricci = []
    for k, (one, two) in enumerate(PAIR_LIST):
        conf = second(0, one, two)
        if one == two:
            conf = conf + lap[0]
            grads_g = grad[14 + one][one]
        else:
            grads_g = 0.5 * (grad[14 + two][one] + grad[14 + one][two])
        ricci.append(-0.5 * lap[1 + k] + grads_g + conf * half_over)
    ricci_trace = contract(inverse, ricci)
    third_trace = (lapse * ricci_trace - lapse_trace) * (1.0 / 3.0)

    def traceless_rate(k):
        one, two = PAIR_LIST[k]
        free = lapse * ricci[k] - lapse_dd[k] - metric[k] * third_trace
        product = sum(
            sym(traceless, one, m) * sym(traceless, m, two) for m in range(3)
        )
        emit(
            8 + k,
            advected[8 + k]
            + chi * free
            + lapse * (trace * traceless[k] - 2.0 * product)
            + lie_of(traceless, one, two)
            - traceless[k] * third_div,
        )

    traceless_rate(0)
    traceless_rate(1)
    yield

    begin(6)
    for k in range(2, 6):
        traceless_rate(k)
    yield

    begin(7)
    for one in range(3):
        emit(21 + one, advected[21 + one] + gauges[one] - DRIVER_ETA * centre[21 + one])
    emit(
        24,
        advected[24]
        + 0.5 * lapse * (chi * ricci_trace + (2.0 / 3.0) * trace * trace - squares)
        - 2.0 * KAPPA_ONE * lapse * theta,
    )
    yield


def section_kernel(
    sizes, section, base, accum, ns_out, na_out, slab,
    xb, tb, tile, bb, ab, local_sem, halo_send, halo_recv,
    line_send, gather_recv,
):
    gx, gy, gz = sizes
    fields, planes, rows, lanes = section.shape
    i, j, k = (lax.axis_index(name) for name in ("gx", "gy", "gz"))

    def device(dx=0, dy=0, dz=0):
        return (
            lax.rem(i + dx + gx, gx),
            lax.rem(j + dy + gy, gy),
            lax.rem(k + dz + gz, gz),
        )

    x_steps = (1,) if gx == 2 else (1, -1)

    copies = []

    def halo(delta, src, dst):
        m = len(copies)
        copies.append(
            pltpu.make_async_remote_copy(
                src_ref=src, dst_ref=dst, send_sem=halo_send.at[m], recv_sem=halo_recv.at[m],
                device_id=device(*delta), device_id_type=MESH,
            )
        )
        return copies[-1]

    own_planes, own_rows = pl.ds(2, planes), pl.ds(PAD, rows)

    def planes_of(dz):
        if dz == 1:
            return pl.ds(planes, 2), pl.ds(0, 2)
        return pl.ds(2, 2), pl.ds(2 + planes, 2)

    def rows_of(dy):
        if dy == 1:
            return pl.ds(PAD + rows - 2, 2), pl.ds(PAD - 2, 2)
        return pl.ds(PAD, 2), pl.ds(PAD + rows, 2)

    def run_of(low, high):
        return pl.ds(FIRST[low], FIRST[high] - FIRST[low])

    def z_face(stage, dz):
        run = run_of(stage, stage + 1)
        src, dst = planes_of(dz)
        return halo((0, 0, dz), xb.at[run, src, own_rows, :], xb.at[run, dst, own_rows, :])

    def y_face(group, dy):
        run = run_of(*group)
        src, dst = rows_of(dy)
        return halo((0, dy, 0), xb.at[run, own_planes, src, :], xb.at[run, own_planes, dst, :])

    def yz_edge(dy, side):
        run = pl.ds(0, len(MIXED))
        src, dst = rows_of(dy)
        cut = pl.ds(0, 2) if side == 0 else pl.ds(2 + planes, 2)
        return halo((0, dy, 0), xb.at[run, cut, src, :], xb.at[run, cut, dst, :])

    def xy_edge(slot, dy):
        src, dst = rows_of(dy)
        return halo((0, dy, 0), tb.at[slot, own_planes, src, :], tb.at[slot, own_planes, dst, :])

    def xz_edge(slot, dz):
        src, dst = planes_of(dz)
        return halo((0, 0, dz), tb.at[slot, src, own_rows, :], tb.at[slot, dst, own_rows, :])

    z_faces = [[z_face(s, dz) for dz in (1, -1)] for s in range(STAGES)]
    y_faces = [[y_face(g, dy) for dy in (1, -1)] for g in Y_GROUPS]
    yz_edges = [yz_edge(dy, side) for dy in (1, -1) for side in (0, 1)]
    x_faces = [
        halo((dx, 0, 0), tile.at[0], tb.at[slot, own_planes, own_rows, :])
        for slot, dx in enumerate(x_steps)
    ]
    slots = range(len(x_steps))
    xy_edges = [xy_edge(slot, dy) for slot in slots for dy in (1, -1)]
    xz_edges = [xz_edge(slot, dz) for slot in slots for dz in (1, -1)]

    def start(some):
        for copy in some:
            copy.start()

    def await_recv(some):
        for copy in some:
            copy.wait_recv()

    loads = []
    place = 0
    for first, size in RUNS:
        loads.append(
            pltpu.make_async_copy(
                section.at[pl.ds(first, size)],
                xb.at[pl.ds(place, size), own_planes, own_rows, :],
                local_sem.at[2 + len(loads)],
            )
        )
        place += size
    load_base = pltpu.make_async_copy(base, bb, local_sem.at[0])
    load_accum = pltpu.make_async_copy(accum, ab, local_sem.at[1])
    partners = [(0, 0, 1), (0, 0, -1)] + [(dx, 0, 0) for dx in x_steps] + [(0, 1, 0), (0, -1, 0)]
    start(loads)
    barrier = pltpu.get_barrier_semaphore()
    for delta in partners:
        pl.semaphore_signal(barrier, inc=1, device_id=device(*delta), device_id_type=MESH)
    load_base.start()
    load_accum.start()

    lane = lax.broadcasted_iota(jnp.int32, (rows, lanes), 1)

    def pack(plane, carry):
        packed = jnp.zeros((rows, lanes), jnp.float32)
        for field in range(fields):
            value = xb[PLACE[field], plane + 2, PAD : PAD + rows, :]
            ends = jnp.where(lane < 2, value, pltpu.roll(value, 4, 1))
            if field:
                ends = pltpu.roll(ends, 4 * field, 1)
            packed = jnp.where((lane >> 2) == field, ends, packed)
        tile[0, plane] = packed
        return carry

    for load in loads:
        load.wait()
    pl.semaphore_wait(barrier, len(partners))
    start(z_faces[0] + y_faces[0] + z_faces[1] + y_faces[1])
    lax.fori_loop(0, planes, pack, 0)
    start(x_faces + z_faces[2] + y_faces[2])
    load_base.wait()
    load_accum.wait()

    own_y = pl.ds(pl.multiple_of(j * rows, rows), rows)
    own_x = pl.ds(pl.multiple_of(i * lanes, lanes), lanes)
    paired = gx == 2 and gy % 2 == 0
    turned = TURNED if paired else 0
    kept = STAGES - turned
    pair = j + 1 - 2 * lax.rem(j, 2)
    other = 1 - i
    towards = ((0, 1), (0, -1), (1, 0), (-1, 0))
    BULK, BULK_TURNED = STAGES, STAGES + 1

    def piece(bi, bj, low, high):
        return slab.at[
            run_of(low, high),
            :,
            pl.ds(pl.multiple_of(bj * rows, rows), rows),
            pl.ds(pl.multiple_of(bi * lanes, lanes), lanes),
        ]

    def line(link, bi, bj, low, high, slot):
        dx, dy = towards[link]
        part = piece(bi, bj, low, high)
        return pltpu.make_async_remote_copy(
            src_ref=part,
            dst_ref=part,
            send_sem=line_send.at[link, bi, bj, 0 if low < kept else 1],
            recv_sem=gather_recv.at[bi, bj, slot],
            device_id=device(dx, dy, 0),
            device_id_type=MESH,
        )

    def send(link, bi, bj, c, own=False):
        slot = c
        if paired and link == 2:
            if c < kept:
                slot = BULK
            elif not own:
                slot = BULK_TURNED
        line(link, bi, bj, c, c + 1, slot).start()

    def arrive(bi, bj, c):
        line(0, bi, bj, c, c + 1, c).wait_recv()

    def x_links(body):
        if paired:
            body(2)
            return

        @pl.when(i + 1 < gx)
        def _():
            body(2)

        @pl.when(i > 0)
        def _():
            body(3)

    def send_own(c):
        @pl.when(j + 1 < gy)
        def _():
            send(0, i, j, c)

        @pl.when(j > 0)
        def _():
            send(1, i, j, c)

        x_links(lambda link: send(link, i, j, c, True))

    def crossed(d, bj, c):
        def cross():
            x_links(lambda link: send(link, i, bj, c))

        if d == 1 and c >= kept:
            pl.when(bj != pair)(cross)
        else:
            cross()

    def pass_on(d, c):
        @pl.when(j - d >= 0)
        def _():
            bj = j - d
            arrive(i, bj, c)

            @pl.when(j + 1 < gy)
            def _():
                send(0, i, bj, c)

            crossed(d, bj, c)

        @pl.when(j + d < gy)
        def _():
            bj = j + d
            arrive(i, bj, c)

            @pl.when(j > 0)
            def _():
                send(1, i, bj, c)

            crossed(d, bj, c)

    def turn(c):
        arrive(other, j, c)

        @pl.when(pair > j)
        def _():
            line(0, other, j, c, c + 1, BULK_TURNED).start()

        @pl.when(pair < j)
        def _():
            line(1, other, j, c, c + 1, BULK_TURNED).start()

    def emit_at(plane):
        def emit(field, rate):
            moved = bb[field, plane] + (0.5 * STEP_DT) * rate
            slab[PLACE[field], plane, own_y, own_x] = moved
            ns_out[field, plane] = moved
            na_out[field, plane] = ab[field, plane] + (STEP_DT / 3.0) * rate

        return emit

    await_recv(x_faces)
    start(xz_edges + xy_edges)
    for s in range(3, STAGES):
        start(z_faces[s])
    await_recv(z_faces[0])
    work = [
        rates_of_plane(plane, rows, lanes, xb, tb, emit_at(plane))
        for plane in range(planes)
    ]

    def own_stage(s):
        if s:
            await_recv(z_faces[s])
        if s == 1:
            start(yz_edges)
        if s < len(Y_GROUPS):
            await_recv(y_faces[s])
        if s == MIX_STAGE:
            await_recv(xy_edges + xz_edges + yz_edges)
        for part in work:
            next(part)
        send_own(s)

    LAG = tuple(1 + 2 * d for d in range(gy))
    for v in range(STAGES + max(LAG)):
        if v < STAGES:
            own_stage(v)
        for d in range(1, gy):
            if 0 <= v - LAG[d] < STAGES:
                pass_on(d, v - LAG[d])
        if kept <= v - TURN_LAG < STAGES:
            turn(v - TURN_LAG)

    def over_blocks(body):
        lax.fori_loop(0, gy, lambda bj, carry: (body(bj), carry)[1], 0)

    for copy in copies:
        copy.wait_send()

    if paired:
        def last(bj):
            line(2, other, bj, 0, kept, BULK).wait_recv()
            if turned:
                @pl.when(bj != j)
                def _():
                    line(2, other, bj, kept, STAGES, BULK_TURNED).wait_recv()

        over_blocks(last)
    else:
        for d in range(1, gx):
            def row(bj, d=d):
                @pl.when(i - d >= 0)
                def _():
                    for c in range(STAGES):
                        arrive(i - d, bj, c)

                        @pl.when(i + 1 < gx)
                        def _():
                            send(2, i - d, bj, c)

                @pl.when(i + d < gx)
                def _():
                    for c in range(STAGES):
                        arrive(i + d, bj, c)

                        @pl.when(i > 0)
                        def _():
                            send(3, i + d, bj, c)

            over_blocks(row)

    def drain(bj):
        def sent(link, bi, low=0, high=STAGES):
            if low < kept:
                line(link, bi, bj, low, min(high, kept), 0).wait_send()
            if high > kept:
                line(link, bi, bj, kept, high, 0).wait_send()

        @pl.when((bj <= j) & (j + 1 < gy))
        def _():
            sent(0, i)

        @pl.when((bj >= j) & (j > 0))
        def _():
            sent(1, i)

        if paired:
            sent(2, i, 0, kept)
            if turned:
                @pl.when(bj != pair)
                def _():
                    sent(2, i, kept, STAGES)
        else:
            x_links(lambda link: sent(link, i))
            for d in range(1, gx):
                @pl.when((i - d >= 0) & (i + 1 < gx))
                def _():
                    sent(2, i - d)

                @pl.when((i + d < gx) & (i > 0))
                def _():
                    sent(3, i + d)

    over_blocks(drain)
    if turned:
        @pl.when(pair > j)
        def _():
            line(0, other, j, kept, STAGES, 0).wait_send()

        @pl.when(pair < j)
        def _():
            line(1, other, j, kept, STAGES, 0).wait_send()


def put_out(ns_in, na_in, slab_in, ns_out, na_out, slab_out, sem):
    pairs = []
    place = 0
    for first, size in RUNS:
        pairs.append((slab_in.at[pl.ds(place, size)], slab_out.at[pl.ds(first, size)]))
        place += size
    pairs += [(ns_in, ns_out), (na_in, na_out)]
    copies = [pltpu.make_async_copy(a, b, sem.at[n]) for n, (a, b) in enumerate(pairs)]
    for copy in copies:
        copy.start()
    for copy in copies:
        copy.wait()


def shards(sizes, section, base, accum):
    gx, gy, gz = sizes
    fields, planes, rows, lanes = section.shape
    slots = 1 if gx == 2 else 2
    n_messages = 2 * STAGES + 2 * len(Y_GROUPS) + 4 + 5 * slots
    any_spec = pl.BlockSpec(memory_space=pl.ANY)
    block = jax.ShapeDtypeStruct(section.shape, jnp.float32)
    slab = jax.ShapeDtypeStruct((fields, planes, gy * rows, gx * lanes), jnp.float32)
    dma = pltpu.SemaphoreType.DMA
    staged = pl.pallas_call(
        functools.partial(section_kernel, sizes),
        out_shape=tuple(pltpu.VMEM(a.shape, a.dtype) for a in (block, block, slab)),
        in_specs=[pl.BlockSpec(memory_space=pltpu.HBM)] * 3,
        out_specs=(pl.BlockSpec(memory_space=pltpu.VMEM),) * 3,
        scratch_shapes=[
            pltpu.VMEM((fields, planes + 4, rows + 2 * PAD, lanes), jnp.float32),
            pltpu.VMEM((slots, planes + 4, rows + 2 * PAD, lanes), jnp.float32),
            pltpu.VMEM((1, planes, rows, lanes), jnp.float32),
            pltpu.VMEM(section.shape, jnp.float32),
            pltpu.VMEM(section.shape, jnp.float32),
            dma((2 + len(RUNS),)),
            dma((n_messages,)),
            dma((n_messages,)),
            dma((4, gx, gy, 2)),
            dma((gx, gy, STAGES + 2)),
        ],
        compiler_params=pltpu.CompilerParams(collective_id=0, has_side_effects=True, vmem_limit_bytes=24 << 20),
    )(*(pltpu.with_memory_space_constraint(x, pltpu.HBM) for x in (section, base, accum)))
    return pl.pallas_call(
        put_out,
        out_shape=(block, block, slab),
        in_specs=[pl.BlockSpec(memory_space=pltpu.VMEM)] * 3,
        out_specs=(any_spec,) * 3,
        scratch_shapes=[dma((2 + len(RUNS),))],
        compiler_params=pltpu.CompilerParams(vmem_limit_bytes=8 << 20),
    )(*staged)


def solution(mesh):
    sizes = tuple(mesh.shape[name] for name in ("gx", "gy", "gz"))
    spec = P(None, "gz", "gy", "gx")
    return jax.shard_map(
        functools.partial(shards, sizes),
        mesh=mesh,
        in_specs=(spec, spec, spec),
        out_specs=(spec, spec, P(None, "gz", None, None)),
        check_vma=False,
    )
```

```python
import functools

import jax
import jax.numpy as jnp
from jax import lax
from jax.experimental import pallas as pl
from jax.experimental.pallas import tpu as pltpu
from jax.sharding import PartitionSpec as P

STEP_DT = 0.25
DISSIPATE = 0.1
DRIVER_ETA = 2.0
KAPPA_ONE = 0.1
PAIR_SLOT = ((0, 1, 2), (1, 3, 4), (2, 4, 5))
PAIR_LIST = ((0, 0), (0, 1), (0, 2), (1, 1), (1, 2), (2, 2))
MESH = pl.DeviceIdType.MESH
RUNS = ((17, 4), (0, 8), (14, 3), (8, 6), (21, 4))
ORDER = tuple(first + n for first, size in RUNS for n in range(size))
PLACE = tuple(ORDER.index(field) for field in range(len(ORDER)))
MIXED = (17, 18, 19, 20, 0)
SIZES = (1, 4, 3, 3, 2, 4, 4, 4)
STAGES = len(SIZES)
FIRST = tuple(sum(SIZES[:s]) for s in range(STAGES + 1))
MIX_STAGE = 4
TURNED = 3
TURN_LAG = 6
Y_GROUPS = ((0, 1), (1, 2), (2, STAGES))
PAD = 8


def first_of(m2, m1, p1, p2):
    return (8.0 / 12.0) * (p1 - m1) - (1.0 / 12.0) * (p2 - m2)


def rates_of_plane(plane, rows, lanes, xb, tb, emit):
    lane = lax.broadcasted_iota(jnp.int32, (rows, lanes), 1)
    quad = lane & 3
    edge_one = (lane < 1) | (lane >= lanes - 1)
    edge_two = (lane < 2) | (lane >= lanes - 2)

    def cell(field, dz=0, dy=0):
        return xb[PLACE[field], plane + 2 + dz, PAD + dy : PAD + dy + rows, :]

    def strip(dz=0, dy=0):
        def side(slot):
            return tb[slot, plane + 2 + dz, PAD + dy : PAD + dy + rows, :]

        if tb.shape[0] == 1:
            return side(0)
        return jnp.where(quad < 2, side(0), side(1))

    def facing(edge):
        return jnp.where(
            quad < 2, pltpu.roll(edge, lanes - 2, 1), pltpu.roll(edge, 2, 1)
        )

    def inner(edge):
        return jnp.where(
            quad == 1, pltpu.roll(edge, 1, 1), pltpu.roll(edge, lanes - 1, 1)
        )

    def x_line(field, value, edge, edge_in):
        turn = (lanes - 2 - 4 * field) % lanes
        two = pltpu.roll(edge, turn, 1)
        one = pltpu.roll(edge_in, turn, 1)
        m2 = jnp.where(edge_two & (lane < 64), two, pltpu.roll(value, 2, 1))
        m1 = jnp.where(edge_one & (lane < 64), one, pltpu.roll(value, 1, 1))
        p1 = jnp.where(edge_one & (lane >= 64), one, pltpu.roll(value, lanes - 1, 1))
        p2 = jnp.where(edge_two & (lane >= 64), two, pltpu.roll(value, lanes - 2, 1))
        return m2, m1, p1, p2

    def y_line(read):
        return tuple(read(0, dy) for dy in (-2, -1, 1, 2))

    def z_line(read):
        return tuple(read(dz, 0) for dz in (-2, -1, 1, 2))

    edge = facing(strip())
    edge_in = inner(edge)

    centre, grad, curve, lap, mixed = {}, {}, {}, {}, {}
    need_lap = (0, 1, 2, 3, 4, 5, 6, 17, 18, 19, 20)
    shift = [cell(18), cell(19), cell(20)]
    advected = {}
    for field in range(len(ORDER)):
        centre[field] = cell(field)

    def differentiate(field):
        value = centre[field]
        read = functools.partial(cell, field)
        lines = [x_line(field, value, edge, edge_in), y_line(read), z_line(read)]
        near = [m1 + p1 for _, m1, p1, _ in lines]
        far = [m2 + p2 for m2, _, _, p2 in lines]
        near_sum = near[0] + near[1] + near[2]
        far_sum = far[0] + far[1] + far[2]
        smooth = far_sum - 4.0 * near_sum + 18.0 * value
        grads = [first_of(*line) for line in lines]
        grad[field] = grads
        advected[field] = (
            shift[0] * grads[0] + shift[1] * grads[1] + shift[2] * grads[2]
            - (DISSIPATE / 16.0) * smooth
        )
        if field in need_lap:
            lap[field] = (16.0 / 12.0) * near_sum - (1.0 / 12.0) * far_sum - 7.5 * value
        if field in MIXED:
            for axis in range(3):
                if field in (0, 17) or field == 18 + axis:
                    curve[field, axis] = (
                        (16.0 / 12.0) * near[axis] - (1.0 / 12.0) * far[axis] - 2.5 * value
                    )

    def mix():
        edge_y = facing(first_of(*y_line(strip)))
        edge_y_in = inner(edge_y)
        edge_z = facing(first_of(*z_line(strip)))
        edge_z_in = inner(edge_z)
        for field in MIXED:
            grads = grad[field]
            if field != 20:
                mixed[field, 0, 1] = first_of(*x_line(field, grads[1], edge_y, edge_y_in))
            if field != 19:
                mixed[field, 0, 2] = first_of(*x_line(field, grads[2], edge_z, edge_z_in))
            if field != 18:
                mixed[field, 1, 2] = first_of(
                    *(
                        first_of(*(cell(field, dz, dy) for dy in (-2, -1, 1, 2)))
                        for dz in (-2, -1, 1, 2)
                    )
                )

    def second(field, one, two):
        if one == two:
            return curve[field, one]
        return mixed[field, min(one, two), max(one, two)]

    def sym(table, one, two):
        return table[PAIR_SLOT[one][two]]

    metric = [centre[1 + k] for k in range(6)]
    traceless = [centre[8 + k] for k in range(6)]
    inverse = [
        (2.0 - metric[k]) if one == two else -metric[k]
        for k, (one, two) in enumerate(PAIR_LIST)
    ]

    def contract(left, right):
        diag = left[0] * right[0] + left[3] * right[3] + left[5] * right[5]
        off = left[1] * right[1] + left[2] * right[2] + left[4] * right[4]
        return diag + 2.0 * off

    def lie_of(table, one, two):
        total = None
        for k in range(3):
            if one == two:
                term = 2.0 * (sym(table, one, k) * grad[18 + k][one])
            else:
                term = (
                    sym(table, one, k) * grad[18 + k][two]
                    + sym(table, two, k) * grad[18 + k][one]
                )
            total = term if total is None else total + term
        return total

    def begin(stage):
        for field in ORDER[FIRST[stage] : FIRST[stage + 1]]:
            differentiate(field)

    chi, trace, lapse, theta = centre[0], centre[7], centre[17], centre[24]

    begin(0)
    emit(17, advected[17] - 2.0 * lapse * (trace - 2.0 * theta))
    yield

    begin(1)
    div = grad[18][0] + grad[19][1] + grad[20][2]
    third_div = (2.0 / 3.0) * div
    for one in range(3):
        emit(18 + one, advected[18 + one] + 0.75 * centre[21 + one])
    emit(0, advected[0] + (2.0 / 3.0) * chi * (lapse * trace) - chi * third_div)
    yield

    def metric_rate(k):
        one, two = PAIR_LIST[k]
        emit(
            1 + k,
            advected[1 + k]
            - 2.0 * lapse * traceless[k]
            + lie_of(metric, one, two)
            - metric[k] * third_div,
        )

    for stage in (2, 3):
        begin(stage)
        for field in ORDER[FIRST[stage] : FIRST[stage + 1]]:
            metric_rate(field - 1)
        yield

    begin(4)
    mix()
    over_chi = 1.0 / chi
    half_over = 0.5 * over_chi
    squares = contract(traceless, traceless)
    lapse_dd = [second(17, one, two) for one, two in PAIR_LIST]
    lapse_trace = contract(inverse, lapse_dd)
    emit(
        7,
        advected[7]
        - chi * lapse_trace
        + lapse * (squares + trace * trace * (1.0 / 3.0))
        + KAPPA_ONE * lapse * theta,
    )
    gauges = []

    def connection_rate(one):
        a_lapse = sum(sym(traceless, one, k) * grad[17][k] for k in range(3))
        a_chi = sum(sym(traceless, one, k) * grad[0][k] for k in range(3))
        g_trace = sum(sym(inverse, one, k) * grad[7][k] for k in range(3))
        b_mixed = sum(second(18 + k, one, k) for k in range(3))
        g_shift = sum(centre[14 + k] * grad[18 + one][k] for k in range(3))
        gauge = (
            -2.0 * a_lapse
            - lapse * ((4.0 / 3.0) * g_trace + 3.0 * (a_chi * over_chi))
            + lap[18 + one]
            + b_mixed * (1.0 / 3.0)
            + centre[14 + one] * third_div
            - g_shift
        )
        gauges.append(gauge)
        emit(14 + one, advected[14 + one] + gauge)

    connection_rate(0)
    yield

    begin(5)
    connection_rate(1)
    connection_rate(2)
    ricci = []
    for k, (one, two) in enumerate(PAIR_LIST):
        conf = second(0, one, two)
        if one == two:
            conf = conf + lap[0]
            grads_g = grad[14 + one][one]
        else:
            grads_g = 0.5 * (grad[14 + two][one] + grad[14 + one][two])
        ricci.append(-0.5 * lap[1 + k] + grads_g + conf * half_over)
    ricci_trace = contract(inverse, ricci)
    third_trace = (lapse * ricci_trace - lapse_trace) * (1.0 / 3.0)

    def traceless_rate(k):
        one, two = PAIR_LIST[k]
        free = lapse * ricci[k] - lapse_dd[k] - metric[k] * third_trace
        product = sum(
            sym(traceless, one, m) * sym(traceless, m, two) for m in range(3)
        )
        emit(
            8 + k,
            advected[8 + k]
            + chi * free
            + lapse * (trace * traceless[k] - 2.0 * product)
            + lie_of(traceless, one, two)
            - traceless[k] * third_div,
        )

    traceless_rate(0)
    traceless_rate(1)
    yield

    begin(6)
    for k in range(2, 6):
        traceless_rate(k)
    yield

    begin(7)
    for one in range(3):
        emit(21 + one, advected[21 + one] + gauges[one] - DRIVER_ETA * centre[21 + one])
    emit(
        24,
        advected[24]
        + 0.5 * lapse * (chi * ricci_trace + (2.0 / 3.0) * trace * trace - squares)
        - 2.0 * KAPPA_ONE * lapse * theta,
    )
    yield


def section_kernel(
    sizes, section, base, accum, ns_out, na_out, slab,
    xb, tb, tile, bb, ab, local_sem, halo_send, halo_recv,
    line_send, gather_recv,
):
    gx, gy, gz = sizes
    fields, planes, rows, lanes = section.shape
    i, j, k = (lax.axis_index(name) for name in ("gx", "gy", "gz"))

    def device(dx=0, dy=0, dz=0):
        return (
            lax.rem(i + dx + gx, gx),
            lax.rem(j + dy + gy, gy),
            lax.rem(k + dz + gz, gz),
        )

    x_steps = (1,) if gx == 2 else (1, -1)

    def landed(sem, ref):
        pltpu.make_async_remote_copy(
            src_ref=ref, dst_ref=ref, send_sem=sem, recv_sem=sem,
            device_id=device(0, 1, 0), device_id_type=MESH,
        ).wait_recv()

    def left(sem, ref):
        pltpu.make_async_remote_copy(
            src_ref=ref, dst_ref=ref, send_sem=sem, recv_sem=sem,
            device_id=device(0, 1, 0), device_id_type=MESH,
        ).wait_send()

    own_planes, own_rows = pl.ds(2, planes), pl.ds(PAD, rows)
    SENT = dict(z=0, y=1, yz=2, x=3, xy=4, xz=5)
    GOT_Z, GOT_Y = 0, STAGES
    GOT_YZ = STAGES + len(Y_GROUPS)
    GOT_X, GOT_XY, GOT_XZ = GOT_YZ + 1, GOT_YZ + 2, GOT_YZ + 3

    def halo(delta, kind, got, src, dst):
        return pltpu.make_async_remote_copy(
            src_ref=src, dst_ref=dst,
            send_sem=halo_send.at[SENT[kind]], recv_sem=halo_recv.at[got],
            device_id=device(*delta), device_id_type=MESH,
        )

    def planes_of(dz):
        if dz == 1:
            return pl.ds(planes, 2), pl.ds(0, 2)
        return pl.ds(2, 2), pl.ds(2 + planes, 2)

    def rows_of(dy):
        if dy == 1:
            return pl.ds(PAD + rows - 2, 2), pl.ds(PAD - 2, 2)
        return pl.ds(PAD, 2), pl.ds(PAD + rows, 2)

    def run_of(low, high):
        return pl.ds(FIRST[low], FIRST[high] - FIRST[low])

    def z_face(stage, dz):
        run = run_of(stage, stage + 1)
        src, dst = planes_of(dz)
        return halo(
            (0, 0, dz), "z", GOT_Z + stage,
            xb.at[run, src, own_rows, :], xb.at[run, dst, own_rows, :],
        )

    def y_face(group, dy):
        run = run_of(*Y_GROUPS[group])
        src, dst = rows_of(dy)
        return halo(
            (0, dy, 0), "y", GOT_Y + group,
            xb.at[run, own_planes, src, :], xb.at[run, own_planes, dst, :],
        )

    def yz_edge(dy, side):
        run = pl.ds(0, len(MIXED))
        src, dst = rows_of(dy)
        cut = pl.ds(0, 2) if side == 0 else pl.ds(2 + planes, 2)
        return halo((0, dy, 0), "yz", GOT_YZ, xb.at[run, cut, src, :], xb.at[run, cut, dst, :])

    def xy_edge(slot, dy):
        src, dst = rows_of(dy)
        return halo(
            (0, dy, 0), "xy", GOT_XY,
            tb.at[slot, own_planes, src, :], tb.at[slot, own_planes, dst, :],
        )

    def xz_edge(slot, dz):
        src, dst = planes_of(dz)
        return halo(
            (0, 0, dz), "xz", GOT_XZ,
            tb.at[slot, src, own_rows, :], tb.at[slot, dst, own_rows, :],
        )

    steps, slots = (1, -1), range(len(x_steps))
    z_faces = [[z_face(s, dz) for dz in steps] for s in range(STAGES)]
    y_faces = [[y_face(g, dy) for dy in steps] for g in range(len(Y_GROUPS))]
    yz_edges = [yz_edge(dy, side) for dy in steps for side in (0, 1)]
    x_faces = [
        halo((dx, 0, 0), "x", GOT_X, tile.at[0], tb.at[slot, own_planes, own_rows, :])
        for slot, dx in enumerate(x_steps)
    ]
    xy_edges = [xy_edge(slot, dy) for slot in slots for dy in steps]
    xz_edges = [xz_edge(slot, dz) for slot in slots for dz in steps]

    def z_landed(s):
        landed(halo_recv.at[GOT_Z + s], xb.at[run_of(s, s + 1), pl.ds(0, 4), own_rows, :])

    def y_landed(g):
        landed(halo_recv.at[GOT_Y + g], xb.at[run_of(*Y_GROUPS[g]), own_planes, pl.ds(0, 4), :])

    every = pl.ds(0, len(x_steps))

    def x_landed():
        landed(halo_recv.at[GOT_X], tb.at[every, own_planes, own_rows, :])

    def edges_landed():
        landed(halo_recv.at[GOT_YZ], xb.at[pl.ds(0, len(MIXED)), pl.ds(0, 4), pl.ds(0, 4), :])
        landed(halo_recv.at[GOT_XY], tb.at[every, own_planes, pl.ds(0, 4), :])
        landed(halo_recv.at[GOT_XZ], tb.at[every, pl.ds(0, 4), own_rows, :])

    def halos_left():
        left(halo_send.at[SENT["z"]], slab.at[:, pl.ds(0, 2), pl.ds(0, 2 * rows), pl.ds(0, lanes)])
        left(halo_send.at[SENT["y"]], xb.at[:, own_planes, pl.ds(0, 4), :])
        left(halo_send.at[SENT["yz"]], xb.at[pl.ds(0, len(MIXED)), pl.ds(0, 4), pl.ds(0, 4), :])
        left(halo_send.at[SENT["x"]], tb.at[every, own_planes, own_rows, :])
        left(halo_send.at[SENT["xy"]], tb.at[every, own_planes, pl.ds(0, 4), :])
        left(halo_send.at[SENT["xz"]], tb.at[every, pl.ds(0, 4), own_rows, :])

    def start(some):
        for copy in some:
            copy.start()

    loads = []
    place = 0
    for first, size in RUNS:
        loads.append(
            pltpu.make_async_copy(
                section.at[pl.ds(first, size)],
                xb.at[pl.ds(place, size), own_planes, own_rows, :],
                local_sem.at[0],
            )
        )
        place += size
    load_base = pltpu.make_async_copy(base, bb, local_sem.at[1])
    load_accum = pltpu.make_async_copy(accum, ab, local_sem.at[2])
    partners = [(0, 0, 1), (0, 0, -1)] + [(dx, 0, 0) for dx in x_steps] + [(0, 1, 0), (0, -1, 0)]
    start(loads)
    barrier = pltpu.get_barrier_semaphore()
    for delta in partners:
        pl.semaphore_signal(barrier, inc=1, device_id=device(*delta), device_id_type=MESH)
    load_base.start()
    load_accum.start()

    lane = lax.broadcasted_iota(jnp.int32, (rows, lanes), 1)

    own_cells = xb.at[:, own_planes, own_rows, :]
    pltpu.make_async_copy(own_cells, own_cells, local_sem.at[0]).wait()
    for plane in range(planes):
        packed = jnp.zeros((rows, lanes), jnp.float32)
        for field in range(fields):
            value = xb[PLACE[field], plane + 2, PAD : PAD + rows, :]
            ends = pltpu.roll(value, (4 * field + 2) % lanes, 1)
            packed = jnp.where((lane >> 2) == field, ends, packed)
        tile[0, plane] = packed
    pl.semaphore_wait(barrier, len(partners))
    start(z_faces[0] + y_faces[0] + x_faces)
    start(z_faces[1] + y_faces[1] + z_faces[2] + y_faces[2] + z_faces[3])
    load_base.wait()
    load_accum.wait()

    own_y = pl.ds(pl.multiple_of(j * rows, rows), rows)
    own_x = pl.ds(pl.multiple_of(i * lanes, lanes), lanes)
    paired = gx == 2 and gy % 2 == 0
    turned = TURNED if paired else 0
    kept = STAGES - turned
    pair = j + 1 - 2 * lax.rem(j, 2)
    other = 1 - i
    towards = ((0, 1), (0, -1), (1, 0), (-1, 0))
    TURN, BULK, BULK_TURNED, PAIR_TURNED = (gy * STAGES + n for n in (0, turned, turned + 1, turned + 2))
    SENT_PAIR, SENT_TURNED = 4, 5

    def piece(bi, bj, low, high):
        return slab.at[
            run_of(low, high),
            :,
            pl.ds(pl.multiple_of(bj * rows, rows), rows),
            pl.ds(pl.multiple_of(bi * lanes, lanes), lanes),
        ]

    def line(link, bi, bj, c, sent, got):
        dx, dy = towards[link]
        part = piece(bi, bj, c, c + 1)
        pltpu.make_async_remote_copy(
            src_ref=part,
            dst_ref=part,
            send_sem=line_send.at[sent],
            recv_sem=gather_recv.at[got],
            device_id=device(dx, dy, 0),
            device_id_type=MESH,
        ).start()

    def number(bi, bj, c):
        return (bj if paired else bi * gy + bj) * STAGES + c

    def send(link, bi, bj, c):
        line(link, bi, bj, c, link, number(bi, bj, c))

    def arrive(bi, bj, c):
        landed(gather_recv.at[number(bi, bj, c)], piece(bi, bj, c, c + 1))

    def x_links(body):
        @pl.when(i + 1 < gx)
        def _():
            body(2)

        @pl.when(i > 0)
        def _():
            body(3)

    def cross(bj, c, distance):
        if not paired:
            x_links(lambda link: send(link, i, bj, c))
        elif c < kept:
            if distance == 1:
                line(2, i, bj, c, jnp.where(bj == pair, SENT_PAIR, 2), BULK)
            else:
                line(2, i, bj, c, 2, BULK)
        elif distance == 0:
            line(2, i, bj, c, 2, TURN + c - kept)
        elif distance == 1:
            pl.when(bj != pair)(lambda: line(2, i, bj, c, 2, BULK_TURNED))
        else:
            line(2, i, bj, c, 2, BULK_TURNED)

    def send_own(c):
        @pl.when(j + 1 < gy)
        def _():
            send(0, i, j, c)

        @pl.when(j > 0)
        def _():
            send(1, i, j, c)

        cross(j, c, 0)

    def pass_on(d, c):
        @pl.when(j - d >= 0)
        def _():
            bj = j - d
            arrive(i, bj, c)

            @pl.when(j + 1 < gy)
            def _():
                send(0, i, bj, c)

            cross(bj, c, d)

        @pl.when(j + d < gy)
        def _():
            bj = j + d
            arrive(i, bj, c)

            @pl.when(j > 0)
            def _():
                send(1, i, bj, c)

            cross(bj, c, d)

    def turn(c):
        landed(gather_recv.at[TURN + c - kept], piece(other, j, c, c + 1))

        @pl.when(pair > j)
        def _():
            line(0, other, j, c, SENT_TURNED, PAIR_TURNED)

        @pl.when(pair < j)
        def _():
            line(1, other, j, c, SENT_TURNED, PAIR_TURNED)

    def emit_at(plane):
        def emit(field, rate):
            moved = bb[field, plane] + (0.5 * STEP_DT) * rate
            slab[PLACE[field], plane, own_y, own_x] = moved
            ns_out[field, plane] = moved
            na_out[field, plane] = ab[field, plane] + (STEP_DT / 3.0) * rate

        return emit

    x_landed()
    start(xz_edges + xy_edges)
    for s in range(4, STAGES):
        start(z_faces[s])
    z_landed(0)
    work = [
        rates_of_plane(plane, rows, lanes, xb, tb, emit_at(plane))
        for plane in range(planes)
    ]

    def own_stage(s):
        if s:
            z_landed(s)
        if s == 1:
            start(yz_edges)
        if s < len(Y_GROUPS):
            y_landed(s)
        if s == MIX_STAGE:
            edges_landed()
        for part in work:
            next(part)
        send_own(s)

    LAG = tuple(1 + 2 * d for d in range(gy))
    for v in range(STAGES + max(LAG)):
        if v < STAGES:
            own_stage(v)
        for d in range(1, gy):
            if 0 <= v - LAG[d] < STAGES:
                pass_on(d, v - LAG[d])
        if kept <= v - TURN_LAG < STAGES:
            turn(v - TURN_LAG)

    halos_left()

    def whole(n_rows, n_lanes, low=0, high=STAGES):
        return slab.at[run_of(low, high), :, pl.ds(0, n_rows), pl.ds(0, n_lanes)]

    if paired:
        if turned:
            landed(gather_recv.at[PAIR_TURNED], whole(rows, lanes, kept))
        landed(gather_recv.at[BULK], whole(gy * rows, lanes, 0, kept))
        if turned and gy > 2:
            landed(gather_recv.at[BULK_TURNED], whole((gy - 2) * rows, lanes, kept))
    else:
        for d in range(1, gx):
            def row(bj, carry, d=d):
                @pl.when(i - d >= 0)
                def _():
                    for c in range(STAGES):
                        arrive(i - d, bj, c)

                        @pl.when(i + 1 < gx)
                        def _():
                            send(2, i - d, bj, c)

                @pl.when(i + d < gx)
                def _():
                    for c in range(STAGES):
                        arrive(i + d, bj, c)

                        @pl.when(i > 0)
                        def _():
                            send(3, i + d, bj, c)

                return carry

            lax.fori_loop(0, gy, row, 0)

    for n in range(1, gy):
        @pl.when(j == n - 1)
        def _():
            left(line_send.at[0], whole(n * rows, lanes))

        @pl.when(j == gy - n)
        def _():
            left(line_send.at[1], whole(n * rows, lanes))

    if paired:
        left(line_send.at[2], whole((gy - 1) * rows, lanes))
        left(line_send.at[SENT_PAIR], whole(rows, lanes, 0, kept))
        if turned:
            left(line_send.at[SENT_TURNED], whole(rows, lanes, kept))
    else:
        for n in range(1, gx):
            @pl.when(i == n - 1)
            def _():
                left(line_send.at[2], whole(gy * rows, n * lanes))

            @pl.when(i == gx - n)
            def _():
                left(line_send.at[3], whole(gy * rows, n * lanes))


def put_out(ns_in, na_in, slab_in, ns_out, na_out, slab_out, sem):
    place = 0
    for first, size in RUNS:
        pltpu.make_async_copy(
            slab_in.at[pl.ds(place, size)], slab_out.at[pl.ds(first, size)], sem.at[0]
        ).start()
        place += size
    pltpu.make_async_copy(ns_in, ns_out, sem.at[1]).start()
    pltpu.make_async_copy(na_in, na_out, sem.at[2]).start()
    pltpu.make_async_copy(slab_in, slab_out, sem.at[0]).wait()
    pltpu.make_async_copy(ns_in, ns_out, sem.at[1]).wait()
    pltpu.make_async_copy(na_in, na_out, sem.at[2]).wait()


def shards(sizes, section, base, accum):
    gx, gy, gz = sizes
    fields, planes, rows, lanes = section.shape
    slots = 1 if gx == 2 else 2
    arrivals = gy * STAGES + TURNED + 3 if gx == 2 and gy % 2 == 0 else gx * gy * STAGES
    any_spec = pl.BlockSpec(memory_space=pl.ANY)
    block = jax.ShapeDtypeStruct(section.shape, jnp.float32)
    slab = jax.ShapeDtypeStruct((fields, planes, gy * rows, gx * lanes), jnp.float32)
    dma = pltpu.SemaphoreType.DMA
    staged = pl.pallas_call(
        functools.partial(section_kernel, sizes),
        out_shape=tuple(pltpu.VMEM(a.shape, a.dtype) for a in (block, block, slab)),
        in_specs=[pl.BlockSpec(memory_space=pltpu.HBM)] * 3,
        out_specs=(pl.BlockSpec(memory_space=pltpu.VMEM),) * 3,
        scratch_shapes=[
            pltpu.VMEM((fields, planes + 4, rows + 2 * PAD, lanes), jnp.float32),
            pltpu.VMEM((slots, planes + 4, rows + 2 * PAD, lanes), jnp.float32),
            pltpu.VMEM((1, planes, rows, lanes), jnp.float32),
            pltpu.VMEM(section.shape, jnp.float32),
            pltpu.VMEM(section.shape, jnp.float32),
            dma((3,)),
            dma((6,)),
            dma((STAGES + len(Y_GROUPS) + 4,)),
            dma((6,)),
            dma((arrivals,)),
        ],
        compiler_params=pltpu.CompilerParams(collective_id=0, has_side_effects=True, vmem_limit_bytes=24 << 20),
    )(*(pltpu.with_memory_space_constraint(x, pltpu.HBM) for x in (section, base, accum)))
    return pl.pallas_call(
        put_out,
        out_shape=(block, block, slab),
        in_specs=[pl.BlockSpec(memory_space=pltpu.VMEM)] * 3,
        out_specs=(any_spec,) * 3,
        scratch_shapes=[dma((3,))],
        compiler_params=pltpu.CompilerParams(vmem_limit_bytes=8 << 20),
    )(*staged)


def solution(mesh):
    sizes = tuple(mesh.shape[name] for name in ("gx", "gy", "gz"))
    spec = P(None, "gz", "gy", "gx")
    return jax.shard_map(
        functools.partial(shards, sizes),
        mesh=mesh,
        in_specs=(spec, spec, spec),
        out_specs=(spec, spec, P(None, "gz", None, None)),
        check_vma=False,
    )
```

```python
import functools

import jax
import jax.numpy as jnp
from jax import lax
from jax.experimental import pallas as pl
from jax.experimental.pallas import tpu as pltpu
from jax.sharding import PartitionSpec as P

STEP_DT = 0.25
DISSIPATE = 0.1
DRIVER_ETA = 2.0
KAPPA_ONE = 0.1
PAIR_SLOT = ((0, 1, 2), (1, 3, 4), (2, 4, 5))
PAIR_LIST = ((0, 0), (0, 1), (0, 2), (1, 1), (1, 2), (2, 2))
MESH = pl.DeviceIdType.MESH
RUNS = ((17, 4), (0, 8), (14, 3), (8, 6), (21, 4))
ORDER = tuple(first + n for first, size in RUNS for n in range(size))
PLACE = tuple(ORDER.index(field) for field in range(len(ORDER)))
MIXED = (17, 18, 19, 20, 0)
SIZES = (1, 4, 3, 3, 1, 4, 5, 4)
STAGES = len(SIZES)
FIRST = tuple(sum(SIZES[:s]) for s in range(STAGES + 1))
MIX_STAGE = 4
TURNED = 3
FINAL = 0
Y_GROUPS = ((0, 1), (1, 2), (2, STAGES))
PAD = 8


def first_of(m2, m1, p1, p2):
    return (8.0 / 12.0) * (p1 - m1) - (1.0 / 12.0) * (p2 - m2)


def rates_of_plane(plane, rows, lanes, xb, tb, emit):
    lane = lax.broadcasted_iota(jnp.int32, (rows, lanes), 1)
    quad = lane & 3
    edge_one = (lane < 1) | (lane >= lanes - 1)
    edge_two = (lane < 2) | (lane >= lanes - 2)

    def cell(field, dz=0, dy=0):
        return xb[PLACE[field], plane + 2 + dz, PAD + dy : PAD + dy + rows, :]

    def strip(dz=0, dy=0):
        def side(slot):
            return tb[slot, plane + 2 + dz, PAD + dy : PAD + dy + rows, :]

        if tb.shape[0] == 1:
            return side(0)
        return jnp.where(quad < 2, side(0), side(1))

    def facing(edge):
        return jnp.where(
            quad < 2, pltpu.roll(edge, lanes - 2, 1), pltpu.roll(edge, 2, 1)
        )

    def inner(edge):
        return jnp.where(
            quad == 1, pltpu.roll(edge, 1, 1), pltpu.roll(edge, lanes - 1, 1)
        )

    def x_line(field, value, edge, edge_in):
        turn = (lanes - 2 - 4 * field) % lanes
        two = pltpu.roll(edge, turn, 1)
        one = pltpu.roll(edge_in, turn, 1)
        m2 = jnp.where(edge_two & (lane < 64), two, pltpu.roll(value, 2, 1))
        m1 = jnp.where(edge_one & (lane < 64), one, pltpu.roll(value, 1, 1))
        p1 = jnp.where(edge_one & (lane >= 64), one, pltpu.roll(value, lanes - 1, 1))
        p2 = jnp.where(edge_two & (lane >= 64), two, pltpu.roll(value, lanes - 2, 1))
        return m2, m1, p1, p2

    def y_line(read):
        return tuple(read(0, dy) for dy in (-2, -1, 1, 2))

    def z_line(read):
        return tuple(read(dz, 0) for dz in (-2, -1, 1, 2))

    edge = facing(strip())
    edge_in = inner(edge)

    centre, grad, curve, lap, mixed = {}, {}, {}, {}, {}
    need_lap = (0, 1, 2, 3, 4, 5, 6, 17, 18, 19, 20)
    shift = [cell(18), cell(19), cell(20)]
    advected = {}
    for field in range(len(ORDER)):
        centre[field] = cell(field)

    def differentiate(field):
        value = centre[field]
        read = functools.partial(cell, field)
        lines = [x_line(field, value, edge, edge_in), y_line(read), z_line(read)]
        near = [m1 + p1 for _, m1, p1, _ in lines]
        far = [m2 + p2 for m2, _, _, p2 in lines]
        near_sum = near[0] + near[1] + near[2]
        far_sum = far[0] + far[1] + far[2]
        smooth = far_sum - 4.0 * near_sum + 18.0 * value
        grads = [first_of(*line) for line in lines]
        grad[field] = grads
        advected[field] = (
            shift[0] * grads[0] + shift[1] * grads[1] + shift[2] * grads[2]
            - (DISSIPATE / 16.0) * smooth
        )
        if field in need_lap:
            lap[field] = (16.0 / 12.0) * near_sum - (1.0 / 12.0) * far_sum - 7.5 * value
        if field in MIXED:
            for axis in range(3):
                if field in (0, 17) or field == 18 + axis:
                    curve[field, axis] = (
                        (16.0 / 12.0) * near[axis] - (1.0 / 12.0) * far[axis] - 2.5 * value
                    )

    def mix():
        edge_y = facing(first_of(*y_line(strip)))
        edge_y_in = inner(edge_y)
        edge_z = facing(first_of(*z_line(strip)))
        edge_z_in = inner(edge_z)
        for field in MIXED:
            grads = grad[field]
            if field != 20:
                mixed[field, 0, 1] = first_of(*x_line(field, grads[1], edge_y, edge_y_in))
            if field != 19:
                mixed[field, 0, 2] = first_of(*x_line(field, grads[2], edge_z, edge_z_in))
            if field != 18:
                mixed[field, 1, 2] = first_of(
                    *(
                        first_of(*(cell(field, dz, dy) for dy in (-2, -1, 1, 2)))
                        for dz in (-2, -1, 1, 2)
                    )
                )

    def second(field, one, two):
        if one == two:
            return curve[field, one]
        return mixed[field, min(one, two), max(one, two)]

    def sym(table, one, two):
        return table[PAIR_SLOT[one][two]]

    metric = [centre[1 + k] for k in range(6)]
    traceless = [centre[8 + k] for k in range(6)]
    inverse = [
        (2.0 - metric[k]) if one == two else -metric[k]
        for k, (one, two) in enumerate(PAIR_LIST)
    ]

    def contract(left, right):
        diag = left[0] * right[0] + left[3] * right[3] + left[5] * right[5]
        off = left[1] * right[1] + left[2] * right[2] + left[4] * right[4]
        return diag + 2.0 * off

    def lie_of(table, one, two):
        total = None
        for k in range(3):
            if one == two:
                term = 2.0 * (sym(table, one, k) * grad[18 + k][one])
            else:
                term = (
                    sym(table, one, k) * grad[18 + k][two]
                    + sym(table, two, k) * grad[18 + k][one]
                )
            total = term if total is None else total + term
        return total

    def begin(stage):
        for field in ORDER[FIRST[stage] : FIRST[stage + 1]]:
            differentiate(field)

    chi, trace, lapse, theta = centre[0], centre[7], centre[17], centre[24]

    begin(0)
    emit(17, advected[17] - 2.0 * lapse * (trace - 2.0 * theta))
    yield

    begin(1)
    div = grad[18][0] + grad[19][1] + grad[20][2]
    third_div = (2.0 / 3.0) * div
    for one in range(3):
        emit(18 + one, advected[18 + one] + 0.75 * centre[21 + one])
    emit(0, advected[0] + (2.0 / 3.0) * chi * (lapse * trace) - chi * third_div)
    yield

    def metric_rate(k):
        one, two = PAIR_LIST[k]
        emit(
            1 + k,
            advected[1 + k]
            - 2.0 * lapse * traceless[k]
            + lie_of(metric, one, two)
            - metric[k] * third_div,
        )

    for stage in (2, 3):
        begin(stage)
        for field in ORDER[FIRST[stage] : FIRST[stage + 1]]:
            metric_rate(field - 1)
        yield

    begin(4)
    mix()
    over_chi = 1.0 / chi
    half_over = 0.5 * over_chi
    squares = contract(traceless, traceless)
    lapse_dd = [second(17, one, two) for one, two in PAIR_LIST]
    lapse_trace = contract(inverse, lapse_dd)
    emit(
        7,
        advected[7]
        - chi * lapse_trace
        + lapse * (squares + trace * trace * (1.0 / 3.0))
        + KAPPA_ONE * lapse * theta,
    )
    gauges = []

    def connection_rate(one):
        a_lapse = sum(sym(traceless, one, k) * grad[17][k] for k in range(3))
        a_chi = sum(sym(traceless, one, k) * grad[0][k] for k in range(3))
        g_trace = sum(sym(inverse, one, k) * grad[7][k] for k in range(3))
        b_mixed = sum(second(18 + k, one, k) for k in range(3))
        g_shift = sum(centre[14 + k] * grad[18 + one][k] for k in range(3))
        gauge = (
            -2.0 * a_lapse
            - lapse * ((4.0 / 3.0) * g_trace + 3.0 * (a_chi * over_chi))
            + lap[18 + one]
            + b_mixed * (1.0 / 3.0)
            + centre[14 + one] * third_div
            - g_shift
        )
        gauges.append(gauge)
        emit(14 + one, advected[14 + one] + gauge)

    yield

    begin(5)
    for one in range(3):
        connection_rate(one)
    ricci = []
    for k, (one, two) in enumerate(PAIR_LIST):
        conf = second(0, one, two)
        if one == two:
            conf = conf + lap[0]
            grads_g = grad[14 + one][one]
        else:
            grads_g = 0.5 * (grad[14 + two][one] + grad[14 + one][two])
        ricci.append(-0.5 * lap[1 + k] + grads_g + conf * half_over)
    ricci_trace = contract(inverse, ricci)
    third_trace = (lapse * ricci_trace - lapse_trace) * (1.0 / 3.0)

    def traceless_rate(k):
        one, two = PAIR_LIST[k]
        free = lapse * ricci[k] - lapse_dd[k] - metric[k] * third_trace
        product = sum(
            sym(traceless, one, m) * sym(traceless, m, two) for m in range(3)
        )
        emit(
            8 + k,
            advected[8 + k]
            + chi * free
            + lapse * (trace * traceless[k] - 2.0 * product)
            + lie_of(traceless, one, two)
            - traceless[k] * third_div,
        )

    traceless_rate(0)
    yield

    begin(6)
    for k in range(1, 6):
        traceless_rate(k)
    yield

    begin(7)
    for one in range(3):
        emit(21 + one, advected[21 + one] + gauges[one] - DRIVER_ETA * centre[21 + one])
    emit(
        24,
        advected[24]
        + 0.5 * lapse * (chi * ricci_trace + (2.0 / 3.0) * trace * trace - squares)
        - 2.0 * KAPPA_ONE * lapse * theta,
    )
    yield


def section_kernel(
    sizes, section, base, accum, ns_out, na_out, slab,
    xb, tb, eb, tile, bb, ab, local_sem, halo_send, halo_recv,
    line_send, gather_recv,
):
    gx, gy, gz = sizes
    fields, planes, rows, lanes = section.shape
    i, j, k = (lax.axis_index(name) for name in ("gx", "gy", "gz"))

    def device(dx=0, dy=0, dz=0):
        return (
            lax.rem(i + dx + gx, gx),
            lax.rem(j + dy + gy, gy),
            lax.rem(k + dz + gz, gz),
        )

    x_steps = (1,) if gx == 2 else (1, -1)

    def landed(sem, ref):
        pltpu.make_async_remote_copy(
            src_ref=ref, dst_ref=ref, send_sem=sem, recv_sem=sem,
            device_id=device(0, 1, 0), device_id_type=MESH,
        ).wait_recv()

    def left(sem, ref):
        pltpu.make_async_remote_copy(
            src_ref=ref, dst_ref=ref, send_sem=sem, recv_sem=sem,
            device_id=device(0, 1, 0), device_id_type=MESH,
        ).wait_send()

    own_planes, own_rows = pl.ds(2, planes), pl.ds(PAD, rows)
    SENT = dict(z=0, y=1, yz=2, x=3, xy=4, xz=5, ze=6)
    GOT_Z, GOT_Y = 0, STAGES
    GOT_YZ = STAGES + len(Y_GROUPS)
    GOT_X, GOT_XY, GOT_XZ, GOT_ZE = (GOT_YZ + n for n in (1, 2, 3, 4))
    mixed = pl.ds(0, len(MIXED))

    def halo(delta, kind, got, src, dst):
        return pltpu.make_async_remote_copy(
            src_ref=src, dst_ref=dst,
            send_sem=halo_send.at[SENT[kind]], recv_sem=halo_recv.at[got],
            device_id=device(*delta), device_id_type=MESH,
        )

    def planes_of(dz):
        if dz == 1:
            return pl.ds(planes, 2), pl.ds(0, 2)
        return pl.ds(2, 2), pl.ds(2 + planes, 2)

    def rows_of(dy):
        if dy == 1:
            return pl.ds(PAD + rows - 2, 2), pl.ds(PAD - 2, 2)
        return pl.ds(PAD, 2), pl.ds(PAD + rows, 2)

    def run_of(low, high):
        return pl.ds(FIRST[low], FIRST[high] - FIRST[low])

    def z_face(stage, dz):
        run = run_of(stage, stage + 1)
        src, dst = planes_of(dz)
        return halo(
            (0, 0, dz), "z", GOT_Z + stage,
            xb.at[run, src, own_rows, :], xb.at[run, dst, own_rows, :],
        )

    def y_face(group, dy):
        run = run_of(*Y_GROUPS[group])
        src, dst = rows_of(dy)
        return halo(
            (0, dy, 0), "y", GOT_Y + group,
            xb.at[run, own_planes, src, :], xb.at[run, own_planes, dst, :],
        )

    def z_edge(dz, dy):
        src, _ = planes_of(dz)
        cut, _ = rows_of(dy)
        place = pl.ds(0 if dz == 1 else 2, 2), pl.ds(0 if dy == 1 else 2, 2)
        return halo(
            (0, 0, dz), "ze", GOT_ZE,
            xb.at[mixed, src, cut, :], eb.at[mixed, place[0], place[1], :],
        )

    def yz_edge(dy, side):
        _, dst = rows_of(dy)
        cut = pl.ds(0, 2) if side == 0 else pl.ds(2 + planes, 2)
        return halo(
            (0, dy, 0), "yz", GOT_YZ,
            eb.at[mixed, pl.ds(2 * side, 2), pl.ds(0 if dy == 1 else 2, 2), :],
            xb.at[mixed, cut, dst, :],
        )

    def xy_edge(slot, dy):
        src, dst = rows_of(dy)
        return halo(
            (0, dy, 0), "xy", GOT_XY,
            tb.at[slot, own_planes, src, :], tb.at[slot, own_planes, dst, :],
        )

    def xz_edge(slot, dz):
        src, dst = planes_of(dz)
        return halo(
            (0, 0, dz), "xz", GOT_XZ,
            tb.at[slot, src, own_rows, :], tb.at[slot, dst, own_rows, :],
        )

    steps, slots = (1, -1), range(len(x_steps))
    z_faces = [[z_face(s, dz) for dz in steps] for s in range(STAGES)]
    y_faces = [[y_face(g, dy) for dy in steps] for g in range(len(Y_GROUPS))]
    z_edges = [z_edge(dz, dy) for dz in steps for dy in steps]
    yz_edges = [yz_edge(dy, side) for dy in steps for side in (0, 1)]
    x_faces = [
        halo((dx, 0, 0), "x", GOT_X, tile.at[0], tb.at[slot, own_planes, own_rows, :])
        for slot, dx in enumerate(x_steps)
    ]
    xy_edges = [xy_edge(slot, dy) for slot in slots for dy in steps]
    xz_edges = [xz_edge(slot, dz) for slot in slots for dz in steps]

    def z_landed(s):
        landed(halo_recv.at[GOT_Z + s], xb.at[run_of(s, s + 1), pl.ds(0, 4), own_rows, :])

    def y_landed(g):
        landed(halo_recv.at[GOT_Y + g], xb.at[run_of(*Y_GROUPS[g]), own_planes, pl.ds(0, 4), :])

    every = pl.ds(0, len(x_steps))

    def x_landed():
        landed(halo_recv.at[GOT_X], tb.at[every, own_planes, own_rows, :])

    def edges_landed():
        landed(halo_recv.at[GOT_YZ], xb.at[mixed, pl.ds(0, 4), pl.ds(0, 4), :])
        landed(halo_recv.at[GOT_XY], tb.at[every, own_planes, pl.ds(0, 4), :])
        landed(halo_recv.at[GOT_XZ], tb.at[every, pl.ds(0, 4), own_rows, :])

    def halos_left():
        left(halo_send.at[SENT["z"]], slab.at[:, pl.ds(0, 2), pl.ds(0, 2 * rows), pl.ds(0, lanes)])
        left(halo_send.at[SENT["y"]], xb.at[:, own_planes, pl.ds(0, 4), :])
        left(halo_send.at[SENT["ze"]], xb.at[mixed, pl.ds(0, 4), pl.ds(0, 4), :])
        left(halo_send.at[SENT["yz"]], xb.at[mixed, pl.ds(0, 4), pl.ds(0, 4), :])
        left(halo_send.at[SENT["x"]], tb.at[every, own_planes, own_rows, :])
        left(halo_send.at[SENT["xy"]], tb.at[every, own_planes, pl.ds(0, 4), :])
        left(halo_send.at[SENT["xz"]], tb.at[every, pl.ds(0, 4), own_rows, :])

    def start(some):
        for copy in some:
            copy.start()

    loads = []
    place = 0
    for first, size in RUNS:
        loads.append(
            pltpu.make_async_copy(
                section.at[pl.ds(first, size)],
                xb.at[pl.ds(place, size), own_planes, own_rows, :],
                local_sem.at[0],
            )
        )
        place += size
    load_base = pltpu.make_async_copy(base, bb, local_sem.at[1])
    load_accum = pltpu.make_async_copy(accum, ab, local_sem.at[2])
    partners = [(0, 0, 1), (0, 0, -1)] + [(dx, 0, 0) for dx in x_steps] + [(0, 1, 0), (0, -1, 0)]
    start(loads)
    barrier = pltpu.get_barrier_semaphore()
    for delta in partners:
        pl.semaphore_signal(barrier, inc=1, device_id=device(*delta), device_id_type=MESH)
    load_base.start()
    load_accum.start()

    lane = lax.broadcasted_iota(jnp.int32, (rows, lanes), 1)

    own_cells = xb.at[:, own_planes, own_rows, :]
    pltpu.make_async_copy(own_cells, own_cells, local_sem.at[0]).wait()
    for plane in range(planes):
        packed = jnp.zeros((rows, lanes), jnp.float32)
        for field in range(fields):
            value = xb[PLACE[field], plane + 2, PAD : PAD + rows, :]
            ends = pltpu.roll(value, (4 * field + 2) % lanes, 1)
            packed = jnp.where((lane >> 2) == field, ends, packed)
        tile[0, plane] = packed
    pl.semaphore_wait(barrier, len(partners))
    start(z_faces[0] + y_faces[0] + x_faces + z_edges)
    start(z_faces[1] + y_faces[1] + z_faces[2] + y_faces[2] + z_faces[3])
    load_base.wait()
    load_accum.wait()

    own_y = pl.ds(pl.multiple_of(j * rows, rows), rows)
    own_x = pl.ds(pl.multiple_of(i * lanes, lanes), lanes)
    paired = gx == 2 and gy % 2 == 0
    turned = TURNED if paired else 0
    kept = STAGES - turned
    pair = j + 1 - 2 * lax.rem(j, 2)
    other = 1 - i
    towards = ((0, 1), (0, -1), (1, 0), (-1, 0))
    TURN, BULK, BULK_TURNED, PAIR_TURNED = ((gy - 1) * STAGES + n for n in (0, turned, turned + 1, turned + 2))
    SENT_PAIR, SENT_TURNED = 4, 5

    def piece(bi, bj, low, high):
        return slab.at[
            run_of(low, high),
            :,
            pl.ds(pl.multiple_of(bj * rows, rows), rows),
            pl.ds(pl.multiple_of(bi * lanes, lanes), lanes),
        ]

    def line(link, bi, bj, c, sent, got):
        dx, dy = towards[link]
        part = piece(bi, bj, c, c + 1)
        pltpu.make_async_remote_copy(
            src_ref=part,
            dst_ref=part,
            send_sem=line_send.at[sent],
            recv_sem=gather_recv.at[got],
            device_id=device(dx, dy, 0),
            device_id_type=MESH,
        ).start()

    def number(link, bi, bj, c):
        if paired:
            return (bj - link) * STAGES + c
        return (bi * gy + bj) * STAGES + c

    def send(link, bi, bj, c):
        line(link, bi, bj, c, link, number(link, bi, bj, c))

    def arrive(link, bi, bj, c):
        landed(gather_recv.at[number(link, bi, bj, c)], piece(bi, bj, c, c + 1))

    def x_links(body):
        @pl.when(i + 1 < gx)
        def _():
            body(2)

        @pl.when(i > 0)
        def _():
            body(3)

    def cross(bj, c, distance):
        if not paired:
            x_links(lambda link: send(link, i, bj, c))
        elif c < kept:
            if distance == 1:
                line(2, i, bj, c, jnp.where(bj == pair, SENT_PAIR, 2), BULK)
            else:
                line(2, i, bj, c, 2, BULK)
        elif distance == 0:
            line(2, i, bj, c, 2, TURN + c - kept)
        elif distance == 1:
            pl.when(bj != pair)(lambda: line(2, i, bj, c, 2, BULK_TURNED))
        else:
            line(2, i, bj, c, 2, BULK_TURNED)

    def held(c, ahead):
        if c < kept:
            return False
        return (pair == j + ahead) & ((pair == 0) | (pair == gy - 1))

    def send_own(c):
        @pl.when((j + 1 < gy) & jnp.logical_not(held(c, 1)))
        def _():
            send(0, i, j, c)

        @pl.when((j > 0) & jnp.logical_not(held(c, -1)))
        def _():
            send(1, i, j, c)

        cross(j, c, 0)

    def send_held(c):
        def go(link, ahead):
            pl.when(held(c, ahead))(
                lambda: line(link, i, j, c, link, number(link, i, j, kept))
            )

        go(0, 1)
        go(1, -1)

    def pass_on(d, c):
        ended = d == 1 and c >= kept

        @pl.when((j - d >= 0) & (j + 1 < gy) if ended else j - d >= 0)
        def _():
            bj = j - d
            arrive(0, i, bj, c)

            @pl.when(j + 1 < gy)
            def _():
                send(0, i, bj, c)

            cross(bj, c, d)

        @pl.when((j + d < gy) & (j > 0) if ended else j + d < gy)
        def _():
            bj = j + d
            arrive(1, i, bj, c)

            @pl.when(j > 0)
            def _():
                send(1, i, bj, c)

            cross(bj, c, d)

    def turn(c):
        landed(gather_recv.at[TURN + c - kept], piece(other, j, c, c + 1))

        @pl.when(pair > j)
        def _():
            line(0, other, j, c, SENT_TURNED, PAIR_TURNED)

        @pl.when(pair < j)
        def _():
            line(1, other, j, c, SENT_TURNED, PAIR_TURNED)

    def emit_at(plane):
        def emit(field, rate):
            moved = bb[field, plane] + (0.5 * STEP_DT) * rate
            slab[PLACE[field], plane, own_y, own_x] = moved
            ns_out[field, plane] = moved
            na_out[field, plane] = ab[field, plane] + (STEP_DT / 3.0) * rate

        return emit

    x_landed()
    start(xz_edges + xy_edges)
    for s in range(4, STAGES):
        start(z_faces[s])
    z_landed(0)
    work = [
        rates_of_plane(plane, rows, lanes, xb, tb, emit_at(plane))
        for plane in range(planes)
    ]

    def own_stage(s):
        if s:
            z_landed(s)
        else:
            landed(halo_recv.at[GOT_ZE], eb.at[mixed, pl.ds(0, 4), pl.ds(0, 4), :])
            start(yz_edges)
        if s < len(Y_GROUPS):
            y_landed(s)
        if s == MIX_STAGE:
            edges_landed()
        for part in work:
            next(part)
        send_own(s)

    LAG = tuple(3 * d for d in range(gy))
    final = STAGES - 1 + LAG[gy - 2] + FINAL
    for v in range(STAGES + LAG[gy - 1]):
        if v < STAGES:
            own_stage(v)
        for d in range(1, gy):
            if 0 <= v - LAG[d] < STAGES:
                pass_on(d, v - LAG[d])
        for c in range(kept, STAGES):
            if v == final - (c == kept):
                send_held(c)
        if v == final:
            for c in range(kept, STAGES):
                turn(c)

    halos_left()

    def whole(n_rows, n_lanes, low=0, high=STAGES):
        return slab.at[run_of(low, high), :, pl.ds(0, n_rows), pl.ds(0, n_lanes)]

    if paired:
        if turned:
            landed(gather_recv.at[PAIR_TURNED], whole(rows, lanes, kept))

            for link, end in ((1, 0), (0, gy - 1)):
                @pl.when(j == end)
                def _():
                    slot = gather_recv.at[number(link, i, pair, kept)]
                    landed(slot, whole(rows, lanes, kept))
        landed(gather_recv.at[BULK], whole(gy * rows, lanes, 0, kept))
        if turned and gy > 2:
            landed(gather_recv.at[BULK_TURNED], whole((gy - 2) * rows, lanes, kept))
    else:
        for d in range(1, gx):
            def row(bj, carry, d=d):
                @pl.when(i - d >= 0)
                def _():
                    for c in range(STAGES):
                        arrive(2, i - d, bj, c)

                        @pl.when(i + 1 < gx)
                        def _():
                            send(2, i - d, bj, c)

                @pl.when(i + d < gx)
                def _():
                    for c in range(STAGES):
                        arrive(3, i + d, bj, c)

                        @pl.when(i > 0)
                        def _():
                            send(3, i + d, bj, c)

                return carry

            lax.fori_loop(0, gy, row, 0)

    for n in range(1, gy):
        @pl.when(j == n - 1)
        def _():
            left(line_send.at[0], whole(n * rows, lanes))

        @pl.when(j == gy - n)
        def _():
            left(line_send.at[1], whole(n * rows, lanes))

    if paired:
        left(line_send.at[2], whole((gy - 1) * rows, lanes))
        left(line_send.at[SENT_PAIR], whole(rows, lanes, 0, kept))
        if turned:
            left(line_send.at[SENT_TURNED], whole(rows, lanes, kept))
    else:
        for n in range(1, gx):
            @pl.when(i == n - 1)
            def _():
                left(line_send.at[2], whole(gy * rows, n * lanes))

            @pl.when(i == gx - n)
            def _():
                left(line_send.at[3], whole(gy * rows, n * lanes))


def put_out(ns_in, na_in, slab_in, ns_out, na_out, slab_out, sem):
    place = 0
    for first, size in RUNS:
        pltpu.make_async_copy(
            slab_in.at[pl.ds(place, size)], slab_out.at[pl.ds(first, size)], sem.at[0]
        ).start()
        place += size
    pltpu.make_async_copy(ns_in, ns_out, sem.at[1]).start()
    pltpu.make_async_copy(na_in, na_out, sem.at[2]).start()
    pltpu.make_async_copy(slab_in, slab_out, sem.at[0]).wait()
    pltpu.make_async_copy(ns_in, ns_out, sem.at[1]).wait()
    pltpu.make_async_copy(na_in, na_out, sem.at[2]).wait()


def shards(sizes, section, base, accum):
    gx, gy, gz = sizes
    fields, planes, rows, lanes = section.shape
    slots = 1 if gx == 2 else 2
    arrivals = (gy - 1) * STAGES + TURNED + 3 if gx == 2 and gy % 2 == 0 else gx * gy * STAGES
    any_spec = pl.BlockSpec(memory_space=pl.ANY)
    block = jax.ShapeDtypeStruct(section.shape, jnp.float32)
    slab = jax.ShapeDtypeStruct((fields, planes, gy * rows, gx * lanes), jnp.float32)
    dma = pltpu.SemaphoreType.DMA
    staged = pl.pallas_call(
        functools.partial(section_kernel, sizes),
        out_shape=tuple(pltpu.VMEM(a.shape, a.dtype) for a in (block, block, slab)),
        in_specs=[pl.BlockSpec(memory_space=pltpu.HBM)] * 3,
        out_specs=(pl.BlockSpec(memory_space=pltpu.VMEM),) * 3,
        scratch_shapes=[
            pltpu.VMEM((fields, planes + 4, rows + 2 * PAD, lanes), jnp.float32),
            pltpu.VMEM((slots, planes + 4, rows + 2 * PAD, lanes), jnp.float32),
            pltpu.VMEM((len(MIXED), 4, 8, lanes), jnp.float32),
            pltpu.VMEM((1, planes, rows, lanes), jnp.float32),
            pltpu.VMEM(section.shape, jnp.float32),
            pltpu.VMEM(section.shape, jnp.float32),
            dma((3,)),
            dma((7,)),
            dma((STAGES + len(Y_GROUPS) + 5,)),
            dma((6,)),
            dma((arrivals,)),
        ],
        compiler_params=pltpu.CompilerParams(collective_id=0, has_side_effects=True, vmem_limit_bytes=24 << 20),
    )(*(pltpu.with_memory_space_constraint(x, pltpu.HBM) for x in (section, base, accum)))
    return pl.pallas_call(
        put_out,
        out_shape=(block, block, slab),
        in_specs=[pl.BlockSpec(memory_space=pltpu.VMEM)] * 3,
        out_specs=(any_spec,) * 3,
        scratch_shapes=[dma((3,))],
        compiler_params=pltpu.CompilerParams(vmem_limit_bytes=8 << 20),
    )(*staged)


def solution(mesh):
    sizes = tuple(mesh.shape[name] for name in ("gx", "gy", "gz"))
    spec = P(None, "gz", "gy", "gx")
    return jax.shard_map(
        functools.partial(shards, sizes),
        mesh=mesh,
        in_specs=(spec, spec, spec),
        out_specs=(spec, spec, P(None, "gz", None, None)),
        check_vma=False,
    )
```

```python
import functools

import jax
import jax.numpy as jnp
from jax import lax
from jax.experimental import pallas as pl
from jax.experimental.pallas import tpu as pltpu
from jax.sharding import PartitionSpec as P

STEP_DT = 0.25
DISSIPATE = 0.1
DRIVER_ETA = 2.0
KAPPA_ONE = 0.1
PAIR_SLOT = ((0, 1, 2), (1, 3, 4), (2, 4, 5))
PAIR_LIST = ((0, 0), (0, 1), (0, 2), (1, 1), (1, 2), (2, 2))
MESH = pl.DeviceIdType.MESH
RUNS = ((17, 4), (0, 8), (14, 3), (8, 6), (21, 4))
ORDER = tuple(first + n for first, size in RUNS for n in range(size))
PLACE = tuple(ORDER.index(field) for field in range(len(ORDER)))
MIXED = (17, 18, 19, 20, 0)
SIZES = (1, 4, 3, 3, 1, 4, 5, 4)
STAGES = len(SIZES)
FIRST = tuple(sum(SIZES[:s]) for s in range(STAGES + 1))
MIX_STAGE = next(s for s in range(STAGES) if FIRST[s + 1] > PLACE[7])
TURNED = 3
FINAL = 0
Y_GROUPS = ((0, 1), (1, 2), (2, STAGES))
EARLY = 4
PAD = 8


def first_of(m2, m1, p1, p2):
    return (8.0 / 12.0) * (p1 - m1) - (1.0 / 12.0) * (p2 - m2)


def rates_of_plane(plane, rows, lanes, xb, tb, emit):
    lane = lax.broadcasted_iota(jnp.int32, (rows, lanes), 1)
    quad = lane & 3
    edge_one = (lane < 1) | (lane >= lanes - 1)
    edge_two = (lane < 2) | (lane >= lanes - 2)

    def cell(field, dz=0, dy=0):
        return xb[PLACE[field], plane + 2 + dz, PAD + dy : PAD + dy + rows, :]

    def strip(dz=0, dy=0):
        def side(slot):
            return tb[slot, plane + 2 + dz, PAD + dy : PAD + dy + rows, :]

        if tb.shape[0] == 1:
            return side(0)
        return jnp.where(quad < 2, side(0), side(1))

    def facing(edge):
        return jnp.where(
            quad < 2, pltpu.roll(edge, lanes - 2, 1), pltpu.roll(edge, 2, 1)
        )

    def inner(edge):
        return jnp.where(
            quad == 1, pltpu.roll(edge, 1, 1), pltpu.roll(edge, lanes - 1, 1)
        )

    def x_line(field, value, edge, edge_in):
        turn = (lanes - 2 - 4 * field) % lanes
        two = pltpu.roll(edge, turn, 1)
        one = pltpu.roll(edge_in, turn, 1)
        m2 = jnp.where(edge_two & (lane < 64), two, pltpu.roll(value, 2, 1))
        m1 = jnp.where(edge_one & (lane < 64), one, pltpu.roll(value, 1, 1))
        p1 = jnp.where(edge_one & (lane >= 64), one, pltpu.roll(value, lanes - 1, 1))
        p2 = jnp.where(edge_two & (lane >= 64), two, pltpu.roll(value, lanes - 2, 1))
        return m2, m1, p1, p2

    def y_line(read):
        return tuple(read(0, dy) for dy in (-2, -1, 1, 2))

    def z_line(read):
        return tuple(read(dz, 0) for dz in (-2, -1, 1, 2))

    edge = facing(strip())
    edge_in = inner(edge)

    centre, grad, curve, lap, mixed = {}, {}, {}, {}, {}
    need_lap = (0, 1, 2, 3, 4, 5, 6, 17, 18, 19, 20)
    shift = [cell(18), cell(19), cell(20)]
    advected = {}
    for field in range(len(ORDER)):
        centre[field] = cell(field)

    def differentiate(field):
        value = centre[field]
        read = functools.partial(cell, field)
        lines = [x_line(field, value, edge, edge_in), y_line(read), z_line(read)]
        near = [m1 + p1 for _, m1, p1, _ in lines]
        far = [m2 + p2 for m2, _, _, p2 in lines]
        near_sum = near[0] + near[1] + near[2]
        far_sum = far[0] + far[1] + far[2]
        smooth = far_sum - 4.0 * near_sum + 18.0 * value
        grads = [first_of(*line) for line in lines]
        grad[field] = grads
        advected[field] = (
            shift[0] * grads[0] + shift[1] * grads[1] + shift[2] * grads[2]
            - (DISSIPATE / 16.0) * smooth
        )
        if field in need_lap:
            lap[field] = (16.0 / 12.0) * near_sum - (1.0 / 12.0) * far_sum - 7.5 * value
        if field in MIXED:
            for axis in range(3):
                if field in (0, 17) or field == 18 + axis:
                    curve[field, axis] = (
                        (16.0 / 12.0) * near[axis] - (1.0 / 12.0) * far[axis] - 2.5 * value
                    )

    def mix():
        edge_y = facing(first_of(*y_line(strip)))
        edge_y_in = inner(edge_y)
        edge_z = facing(first_of(*z_line(strip)))
        edge_z_in = inner(edge_z)
        for field in MIXED:
            grads = grad[field]
            if field != 20:
                mixed[field, 0, 1] = first_of(*x_line(field, grads[1], edge_y, edge_y_in))
            if field != 19:
                mixed[field, 0, 2] = first_of(*x_line(field, grads[2], edge_z, edge_z_in))
            if field != 18:
                mixed[field, 1, 2] = first_of(
                    *(
                        first_of(*(cell(field, dz, dy) for dy in (-2, -1, 1, 2)))
                        for dz in (-2, -1, 1, 2)
                    )
                )

    def second(field, one, two):
        if one == two:
            return curve[field, one]
        return mixed[field, min(one, two), max(one, two)]

    def sym(table, one, two):
        return table[PAIR_SLOT[one][two]]

    metric = [centre[1 + k] for k in range(6)]
    traceless = [centre[8 + k] for k in range(6)]
    inverse = [
        (2.0 - metric[k]) if one == two else -metric[k]
        for k, (one, two) in enumerate(PAIR_LIST)
    ]

    def contract(left, right):
        diag = left[0] * right[0] + left[3] * right[3] + left[5] * right[5]
        off = left[1] * right[1] + left[2] * right[2] + left[4] * right[4]
        return diag + 2.0 * off

    def lie_of(table, one, two):
        total = None
        for k in range(3):
            if one == two:
                term = 2.0 * (sym(table, one, k) * grad[18 + k][one])
            else:
                term = (
                    sym(table, one, k) * grad[18 + k][two]
                    + sym(table, two, k) * grad[18 + k][one]
                )
            total = term if total is None else total + term
        return total

    chi, trace, lapse, theta = centre[0], centre[7], centre[17], centre[24]
    shared, gauges = {}, {}

    def once(name, make):
        if name not in shared:
            shared[name] = make()
        return shared[name]

    def third_div():
        div = grad[18][0] + grad[19][1] + grad[20][2]
        return (2.0 / 3.0) * div

    def lapse_terms():
        mix()
        lapse_dd = [second(17, one, two) for one, two in PAIR_LIST]
        return lapse_dd, contract(inverse, lapse_dd)

    def ricci_terms():
        half_over = 0.5 * once("over", lambda: 1.0 / chi)
        ricci = []
        for k, (one, two) in enumerate(PAIR_LIST):
            conf = second(0, one, two)
            if one == two:
                conf = conf + lap[0]
                grads_g = grad[14 + one][one]
            else:
                grads_g = 0.5 * (grad[14 + two][one] + grad[14 + one][two])
            ricci.append(-0.5 * lap[1 + k] + grads_g + conf * half_over)
        return ricci, contract(inverse, ricci)

    def rate_of(field):
        rate = advected[field]
        if field == 17:
            return rate - 2.0 * lapse * (trace - 2.0 * theta)
        third = once("div", third_div)
        if field in (18, 19, 20):
            return rate + 0.75 * centre[field + 3]
        if field == 0:
            return rate + (2.0 / 3.0) * chi * (lapse * trace) - chi * third
        if field in range(1, 7):
            k = field - 1
            one, two = PAIR_LIST[k]
            lie = lie_of(metric, one, two)
            return rate - 2.0 * lapse * traceless[k] + lie - metric[k] * third
        lapse_dd, lapse_trace = once("lapse", lapse_terms)
        squares = once("squares", lambda: contract(traceless, traceless))
        if field == 7:
            return (
                rate
                - chi * lapse_trace
                + lapse * (squares + trace * trace * (1.0 / 3.0))
                + KAPPA_ONE * lapse * theta
            )
        if field in (14, 15, 16):
            one = field - 14
            a_lapse = sum(sym(traceless, one, k) * grad[17][k] for k in range(3))
            a_chi = sum(sym(traceless, one, k) * grad[0][k] for k in range(3))
            g_trace = sum(sym(inverse, one, k) * grad[7][k] for k in range(3))
            b_mixed = sum(second(18 + k, one, k) for k in range(3))
            g_shift = sum(centre[14 + k] * grad[18 + one][k] for k in range(3))
            over_chi = once("over", lambda: 1.0 / chi)
            gauges[one] = (
                -2.0 * a_lapse
                - lapse * ((4.0 / 3.0) * g_trace + 3.0 * (a_chi * over_chi))
                + lap[18 + one]
                + b_mixed * (1.0 / 3.0)
                + centre[14 + one] * third
                - g_shift
            )
            return rate + gauges[one]
        if field in (21, 22, 23):
            return rate + gauges[field - 21] - DRIVER_ETA * centre[field]
        ricci, ricci_trace = once("ricci", ricci_terms)
        if field == 24:
            return (
                rate
                + 0.5 * lapse * (chi * ricci_trace + (2.0 / 3.0) * trace * trace - squares)
                - 2.0 * KAPPA_ONE * lapse * theta
            )
        k = field - 8
        one, two = PAIR_LIST[k]
        third_trace = once("trace", lambda: (lapse * ricci_trace - lapse_trace) * (1.0 / 3.0))
        free = lapse * ricci[k] - lapse_dd[k] - metric[k] * third_trace
        product = sum(
            sym(traceless, one, m) * sym(traceless, m, two) for m in range(3)
        )
        return (
            rate
            + chi * free
            + lapse * (trace * traceless[k] - 2.0 * product)
            + lie_of(traceless, one, two)
            - traceless[k] * third
        )

    for stage in range(STAGES):
        for field in ORDER[FIRST[stage] : FIRST[stage + 1]]:
            differentiate(field)
        for field in ORDER[FIRST[stage] : FIRST[stage + 1]]:
            emit(field, rate_of(field))
        yield


def section_kernel(
    sizes, section, base, accum, ns_out, na_out, slab,
    xb, tb, eb, tile, bb, ab, local_sem, halo_send, halo_recv,
    line_send, gather_recv, chain,
):
    gx, gy, gz = sizes
    fields, planes, rows, lanes = section.shape
    i, j, k = (lax.axis_index(name) for name in ("gx", "gy", "gz"))

    def device(dx=0, dy=0, dz=0):
        return (
            lax.rem(i + dx + gx, gx),
            lax.rem(j + dy + gy, gy),
            lax.rem(k + dz + gz, gz),
        )

    x_steps = (1,) if gx == 2 else (1, -1)

    def landed(sem, ref):
        pltpu.make_async_remote_copy(
            src_ref=ref, dst_ref=ref, send_sem=sem, recv_sem=sem,
            device_id=device(0, 1, 0), device_id_type=MESH,
        ).wait_recv()

    def left(sem, ref):
        pltpu.make_async_remote_copy(
            src_ref=ref, dst_ref=ref, send_sem=sem, recv_sem=sem,
            device_id=device(0, 1, 0), device_id_type=MESH,
        ).wait_send()

    own_planes, own_rows = pl.ds(2, planes), pl.ds(PAD, rows)
    SENT = dict(z=0, y=1, yz=2, x=3, xy=4, xz=5, ze=6)
    GOT_Z, GOT_Y = 0, STAGES
    GOT_YZ = STAGES + len(Y_GROUPS)
    GOT_X, GOT_XY, GOT_XZ, GOT_ZE = (GOT_YZ + n for n in (1, 2, 3, 4))
    mixed = pl.ds(0, len(MIXED))

    def halo(delta, kind, got, src, dst):
        return pltpu.make_async_remote_copy(
            src_ref=src, dst_ref=dst,
            send_sem=halo_send.at[SENT[kind]], recv_sem=halo_recv.at[got],
            device_id=device(*delta), device_id_type=MESH,
        )

    def planes_of(dz):
        if dz == 1:
            return pl.ds(planes, 2), pl.ds(0, 2)
        return pl.ds(2, 2), pl.ds(2 + planes, 2)

    def rows_of(dy):
        if dy == 1:
            return pl.ds(PAD + rows - 2, 2), pl.ds(PAD - 2, 2)
        return pl.ds(PAD, 2), pl.ds(PAD + rows, 2)

    def run_of(low, high):
        return pl.ds(FIRST[low], FIRST[high] - FIRST[low])

    def z_face(stage, dz):
        run = run_of(stage, stage + 1)
        src, dst = planes_of(dz)
        return halo(
            (0, 0, dz), "z", GOT_Z + stage,
            xb.at[run, src, own_rows, :], xb.at[run, dst, own_rows, :],
        )

    def y_face(group, dy):
        run = run_of(*Y_GROUPS[group])
        src, dst = rows_of(dy)
        return halo(
            (0, dy, 0), "y", GOT_Y + group,
            xb.at[run, own_planes, src, :], xb.at[run, own_planes, dst, :],
        )

    def z_edge(dz, dy):
        src, _ = planes_of(dz)
        cut, _ = rows_of(dy)
        place = pl.ds(0 if dz == 1 else 2, 2), pl.ds(0 if dy == 1 else 2, 2)
        return halo(
            (0, 0, dz), "ze", GOT_ZE,
            xb.at[mixed, src, cut, :], eb.at[mixed, place[0], place[1], :],
        )

    def yz_edge(dy, side):
        _, dst = rows_of(dy)
        cut = pl.ds(0, 2) if side == 0 else pl.ds(2 + planes, 2)
        return halo(
            (0, dy, 0), "yz", GOT_YZ,
            eb.at[mixed, pl.ds(2 * side, 2), pl.ds(0 if dy == 1 else 2, 2), :],
            xb.at[mixed, cut, dst, :],
        )

    def xy_edge(slot, dy):
        src, dst = rows_of(dy)
        return halo(
            (0, dy, 0), "xy", GOT_XY,
            tb.at[slot, own_planes, src, :], tb.at[slot, own_planes, dst, :],
        )

    def xz_edge(slot, dz):
        src, dst = planes_of(dz)
        return halo(
            (0, 0, dz), "xz", GOT_XZ,
            tb.at[slot, src, own_rows, :], tb.at[slot, dst, own_rows, :],
        )

    steps, slots = (1, -1), range(len(x_steps))
    z_faces = [[z_face(s, dz) for dz in steps] for s in range(STAGES)]
    y_faces = [[y_face(g, dy) for dy in steps] for g in range(len(Y_GROUPS))]
    z_edges = [z_edge(dz, dy) for dz in steps for dy in steps]
    yz_edges = [yz_edge(dy, side) for dy in steps for side in (0, 1)]
    x_faces = [
        halo((dx, 0, 0), "x", GOT_X, tile.at[0], tb.at[slot, own_planes, own_rows, :])
        for slot, dx in enumerate(x_steps)
    ]
    xy_edges = [xy_edge(slot, dy) for slot in slots for dy in steps]
    xz_edges = [xz_edge(slot, dz) for slot in slots for dz in steps]

    def z_landed(s):
        landed(halo_recv.at[GOT_Z + s], xb.at[run_of(s, s + 1), pl.ds(0, 4), own_rows, :])

    def y_landed(g):
        landed(halo_recv.at[GOT_Y + g], xb.at[run_of(*Y_GROUPS[g]), own_planes, pl.ds(0, 4), :])

    every = pl.ds(0, len(x_steps))

    def x_landed():
        landed(halo_recv.at[GOT_X], tb.at[every, own_planes, own_rows, :])

    def edges_landed():
        landed(halo_recv.at[GOT_YZ], xb.at[mixed, pl.ds(0, 4), pl.ds(0, 4), :])
        landed(halo_recv.at[GOT_XY], tb.at[every, own_planes, pl.ds(0, 4), :])
        landed(halo_recv.at[GOT_XZ], tb.at[every, pl.ds(0, 4), own_rows, :])

    def halos_left():
        left(halo_send.at[SENT["z"]], slab.at[:, pl.ds(0, 2), pl.ds(0, 2 * rows), pl.ds(0, lanes)])
        left(halo_send.at[SENT["y"]], xb.at[:, own_planes, pl.ds(0, 4), :])
        left(halo_send.at[SENT["ze"]], xb.at[mixed, pl.ds(0, 4), pl.ds(0, 4), :])
        left(halo_send.at[SENT["yz"]], xb.at[mixed, pl.ds(0, 4), pl.ds(0, 4), :])
        left(halo_send.at[SENT["x"]], tb.at[every, own_planes, own_rows, :])
        left(halo_send.at[SENT["xy"]], tb.at[every, own_planes, pl.ds(0, 4), :])
        left(halo_send.at[SENT["xz"]], tb.at[every, pl.ds(0, 4), own_rows, :])

    def start(some):
        for copy in some:
            copy.start()

    loads = []
    place = 0
    for first, size in RUNS:
        loads.append(
            pltpu.make_async_copy(
                section.at[pl.ds(first, size)],
                xb.at[pl.ds(place, size), own_planes, own_rows, :],
                local_sem.at[0],
            )
        )
        place += size
    load_base = pltpu.make_async_copy(base, bb, local_sem.at[1])
    load_accum = pltpu.make_async_copy(accum, ab, local_sem.at[2])
    chained = gy > 2
    faces = [(0, 0, 1), (0, 0, -1)] + [(dx, 0, 0) for dx in x_steps]
    barrier = pltpu.get_barrier_semaphore()

    def greet(sem, delta):
        pl.semaphore_signal(sem, inc=1, device_id=device(*delta), device_id_type=MESH)

    for delta in faces + [(0, -1, 0)]:
        greet(barrier, delta)
    if chained:
        pl.when(j + 1 < gy)(lambda: greet(barrier, (0, 1, 0)))
    else:
        greet(barrier, (0, 1, 0))
    start(loads)
    load_base.start()
    load_accum.start()

    lane = lax.broadcasted_iota(jnp.int32, (rows, lanes), 1)

    own_cells = xb.at[:, own_planes, own_rows, :]
    pltpu.make_async_copy(own_cells, own_cells, local_sem.at[0]).wait()
    for plane in range(planes):
        packed = jnp.zeros((rows, lanes), jnp.float32)
        for field in range(fields):
            value = xb[PLACE[field], plane + 2, PAD : PAD + rows, :]
            ends = pltpu.roll(value, (4 * field + 2) % lanes, 1)
            packed = jnp.where((lane >> 2) == field, ends, packed)
        tile[0, plane] = packed
    if chained:
        pl.when(j == 0)(lambda: pl.semaphore_wait(barrier, len(faces) + 1))
        pl.when(j > 0)(lambda: pl.semaphore_wait(barrier, len(faces) + 2))
    else:
        pl.semaphore_wait(barrier, len(faces) + 2)
    def far(some):
        pl.when(j == 0)(lambda: start(some))

    def near(some):
        up, down = some[::2], some[1::2]
        start(up)
        pl.when(j > 0)(lambda: start(down))

    if not chained:
        near = start
    else:
        pl.when(j == gy - 2)(lambda: greet(chain, (0, -1, 0)))
    start(z_faces[0])
    near(y_faces[0])
    start(x_faces + z_edges + z_faces[1])
    near(y_faces[1])
    start(z_faces[2])
    near(y_faces[2])
    for s in range(3, EARLY):
        start(z_faces[s])
    if chained:
        @pl.when(j < gy - 2)
        def _():
            pl.semaphore_wait(chain, 1)
            pl.when(j > 0)(lambda: greet(chain, (0, -1, 0)))

        for faces_of in y_faces:
            far(faces_of[1::2])
    load_base.wait()
    load_accum.wait()

    own_y = pl.ds(pl.multiple_of(j * rows, rows), rows)
    own_x = pl.ds(pl.multiple_of(i * lanes, lanes), lanes)
    paired = gx == 2 and gy % 2 == 0
    turned = TURNED if paired else 0
    kept = STAGES - turned
    pair = j + 1 - 2 * lax.rem(j, 2)
    other = 1 - i
    towards = ((0, 1), (0, -1), (1, 0), (-1, 0))
    TURN, BULK, BULK_TURNED, PAIR_TURNED = ((gy - 1) * STAGES + n for n in (0, turned, turned + 1, turned + 2))
    SENT_PAIR, SENT_TURNED = 4, 5

    def piece(bi, bj, low, high):
        return slab.at[
            run_of(low, high),
            :,
            pl.ds(pl.multiple_of(bj * rows, rows), rows),
            pl.ds(pl.multiple_of(bi * lanes, lanes), lanes),
        ]

    def line(link, bi, bj, c, sent, got):
        dx, dy = towards[link]
        part = piece(bi, bj, c, c + 1)
        pltpu.make_async_remote_copy(
            src_ref=part,
            dst_ref=part,
            send_sem=line_send.at[sent],
            recv_sem=gather_recv.at[got],
            device_id=device(dx, dy, 0),
            device_id_type=MESH,
        ).start()

    def number(link, bi, bj, c):
        if paired:
            return (bj - link) * STAGES + c
        return (bi * gy + bj) * STAGES + c

    def send(link, bi, bj, c):
        line(link, bi, bj, c, link, number(link, bi, bj, c))

    def arrive(link, bi, bj, c):
        landed(gather_recv.at[number(link, bi, bj, c)], piece(bi, bj, c, c + 1))

    def x_links(body):
        @pl.when(i + 1 < gx)
        def _():
            body(2)

        @pl.when(i > 0)
        def _():
            body(3)

    def cross(bj, c, distance):
        if not paired:
            x_links(lambda link: send(link, i, bj, c))
        elif c < kept:
            if distance == 1:
                line(2, i, bj, c, jnp.where(bj == pair, SENT_PAIR, 2), BULK)
            else:
                line(2, i, bj, c, 2, BULK)
        elif distance == 0:
            line(2, i, bj, c, 2, TURN + c - kept)
        elif distance == 1:
            pl.when(bj != pair)(lambda: line(2, i, bj, c, 2, BULK_TURNED))
        else:
            line(2, i, bj, c, 2, BULK_TURNED)

    def held(c, ahead):
        if c < kept:
            return False
        return (pair == j + ahead) & ((pair == 0) | (pair == gy - 1))

    def send_own(c):
        @pl.when((j + 1 < gy) & jnp.logical_not(held(c, 1)))
        def _():
            send(0, i, j, c)

        @pl.when((j > 0) & jnp.logical_not(held(c, -1)))
        def _():
            send(1, i, j, c)

        cross(j, c, 0)

    def send_held(c):
        def go(link, ahead):
            pl.when(held(c, ahead))(
                lambda: line(link, i, j, c, link, number(link, i, j, kept))
            )

        go(0, 1)
        go(1, -1)

    def pass_on(d, c):
        ended = d == 1 and c >= kept

        @pl.when((j - d >= 0) & (j + 1 < gy) if ended else j - d >= 0)
        def _():
            bj = j - d
            arrive(0, i, bj, c)

            @pl.when(j + 1 < gy)
            def _():
                send(0, i, bj, c)

            cross(bj, c, d)

        @pl.when((j + d < gy) & (j > 0) if ended else j + d < gy)
        def _():
            bj = j + d
            arrive(1, i, bj, c)

            @pl.when(j > 0)
            def _():
                send(1, i, bj, c)

            cross(bj, c, d)

    def turn(c):
        landed(gather_recv.at[TURN + c - kept], piece(other, j, c, c + 1))

        @pl.when(pair > j)
        def _():
            line(0, other, j, c, SENT_TURNED, PAIR_TURNED)

        @pl.when(pair < j)
        def _():
            line(1, other, j, c, SENT_TURNED, PAIR_TURNED)

    def emit_at(plane):
        def emit(field, rate):
            moved = bb[field, plane] + (0.5 * STEP_DT) * rate
            slab[PLACE[field], plane, own_y, own_x] = moved
            ns_out[field, plane] = moved
            na_out[field, plane] = ab[field, plane] + (STEP_DT / 3.0) * rate

        return emit

    x_landed()
    start(xz_edges + xy_edges)
    for s in range(EARLY, STAGES):
        start(z_faces[s])
    z_landed(0)
    work = [
        rates_of_plane(plane, rows, lanes, xb, tb, emit_at(plane))
        for plane in range(planes)
    ]

    def own_stage(s):
        if s:
            z_landed(s)
        else:
            landed(halo_recv.at[GOT_ZE], eb.at[mixed, pl.ds(0, 4), pl.ds(0, 4), :])
            start(yz_edges)
        if s < len(Y_GROUPS):
            y_landed(s)
        if s == MIX_STAGE:
            edges_landed()
        for part in work:
            next(part)
        send_own(s)

    LAG = tuple(3 * d for d in range(gy))
    final = STAGES - 1 + LAG[gy - 2] + FINAL
    for v in range(STAGES + LAG[gy - 1]):
        if v < STAGES:
            own_stage(v)
        for d in range(1, gy):
            if 0 <= v - LAG[d] < STAGES:
                pass_on(d, v - LAG[d])
        for c in range(kept, STAGES):
            if v == final - (c == kept):
                send_held(c)
        if v == final:
            for c in range(kept, STAGES):
                turn(c)

    halos_left()

    def whole(n_rows, n_lanes, low=0, high=STAGES):
        return slab.at[run_of(low, high), :, pl.ds(0, n_rows), pl.ds(0, n_lanes)]

    if paired:
        if turned:
            landed(gather_recv.at[PAIR_TURNED], whole(rows, lanes, kept))

            for link, end in ((1, 0), (0, gy - 1)):
                @pl.when(j == end)
                def _():
                    slot = gather_recv.at[number(link, i, pair, kept)]
                    landed(slot, whole(rows, lanes, kept))
        landed(gather_recv.at[BULK], whole(gy * rows, lanes, 0, kept))
        if turned and gy > 2:
            landed(gather_recv.at[BULK_TURNED], whole((gy - 2) * rows, lanes, kept))
    else:
        for d in range(1, gx):
            def row(bj, carry, d=d):
                @pl.when(i - d >= 0)
                def _():
                    for c in range(STAGES):
                        arrive(2, i - d, bj, c)

                        @pl.when(i + 1 < gx)
                        def _():
                            send(2, i - d, bj, c)

                @pl.when(i + d < gx)
                def _():
                    for c in range(STAGES):
                        arrive(3, i + d, bj, c)

                        @pl.when(i > 0)
                        def _():
                            send(3, i + d, bj, c)

                return carry

            lax.fori_loop(0, gy, row, 0)

    for n in range(1, gy):
        @pl.when(j == n - 1)
        def _():
            left(line_send.at[0], whole(n * rows, lanes))

        @pl.when(j == gy - n)
        def _():
            left(line_send.at[1], whole(n * rows, lanes))

    if paired:
        left(line_send.at[2], whole((gy - 1) * rows, lanes))
        left(line_send.at[SENT_PAIR], whole(rows, lanes, 0, kept))
        if turned:
            left(line_send.at[SENT_TURNED], whole(rows, lanes, kept))
    else:
        for n in range(1, gx):
            @pl.when(i == n - 1)
            def _():
                left(line_send.at[2], whole(gy * rows, n * lanes))

            @pl.when(i == gx - n)
            def _():
                left(line_send.at[3], whole(gy * rows, n * lanes))


def put_out(ns_in, na_in, slab_in, ns_out, na_out, slab_out, sem):
    place = 0
    for first, size in RUNS:
        pltpu.make_async_copy(
            slab_in.at[pl.ds(place, size)], slab_out.at[pl.ds(first, size)], sem.at[0]
        ).start()
        place += size
    pltpu.make_async_copy(ns_in, ns_out, sem.at[1]).start()
    pltpu.make_async_copy(na_in, na_out, sem.at[2]).start()
    pltpu.make_async_copy(slab_in, slab_out, sem.at[0]).wait()
    pltpu.make_async_copy(ns_in, ns_out, sem.at[1]).wait()
    pltpu.make_async_copy(na_in, na_out, sem.at[2]).wait()


def shards(sizes, section, base, accum):
    gx, gy, gz = sizes
    fields, planes, rows, lanes = section.shape
    slots = 1 if gx == 2 else 2
    arrivals = (gy - 1) * STAGES + TURNED + 3 if gx == 2 and gy % 2 == 0 else gx * gy * STAGES
    any_spec = pl.BlockSpec(memory_space=pl.ANY)
    block = jax.ShapeDtypeStruct(section.shape, jnp.float32)
    slab = jax.ShapeDtypeStruct((fields, planes, gy * rows, gx * lanes), jnp.float32)
    dma = pltpu.SemaphoreType.DMA
    staged = pl.pallas_call(
        functools.partial(section_kernel, sizes),
        out_shape=tuple(pltpu.VMEM(a.shape, a.dtype) for a in (block, block, slab)),
        in_specs=[pl.BlockSpec(memory_space=pltpu.HBM)] * 3,
        out_specs=(pl.BlockSpec(memory_space=pltpu.VMEM),) * 3,
        scratch_shapes=[
            pltpu.VMEM((fields, planes + 4, rows + 2 * PAD, lanes), jnp.float32),
            pltpu.VMEM((slots, planes + 4, rows + 2 * PAD, lanes), jnp.float32),
            pltpu.VMEM((len(MIXED), 4, 8, lanes), jnp.float32),
            pltpu.VMEM((1, planes, rows, lanes), jnp.float32),
            pltpu.VMEM(section.shape, jnp.float32),
            pltpu.VMEM(section.shape, jnp.float32),
            dma((3,)),
            dma((7,)),
            dma((STAGES + len(Y_GROUPS) + 5,)),
            dma((6,)),
            dma((arrivals,)),
            pltpu.SemaphoreType.REGULAR,
        ],
        compiler_params=pltpu.CompilerParams(collective_id=0, has_side_effects=True, vmem_limit_bytes=24 << 20),
    )(*(pltpu.with_memory_space_constraint(x, pltpu.HBM) for x in (section, base, accum)))
    return pl.pallas_call(
        put_out,
        out_shape=(block, block, slab),
        in_specs=[pl.BlockSpec(memory_space=pltpu.VMEM)] * 3,
        out_specs=(any_spec,) * 3,
        scratch_shapes=[dma((3,))],
        compiler_params=pltpu.CompilerParams(vmem_limit_bytes=8 << 20),
    )(*staged)


def solution(mesh):
    sizes = tuple(mesh.shape[name] for name in ("gx", "gy", "gz"))
    spec = P(None, "gz", "gy", "gx")
    return jax.shard_map(
        functools.partial(shards, sizes),
        mesh=mesh,
        in_specs=(spec, spec, spec),
        out_specs=(spec, spec, P(None, "gz", None, None)),
        check_vma=False,
    )
```

```python
import functools

import jax
import jax.numpy as jnp
from jax import lax
from jax.experimental import pallas as pl
from jax.experimental.pallas import tpu as pltpu
from jax.sharding import PartitionSpec as P

STEP_DT = 0.25
DISSIPATE = 0.1
DRIVER_ETA = 2.0
KAPPA_ONE = 0.1
PAIR_SLOT = ((0, 1, 2), (1, 3, 4), (2, 4, 5))
PAIR_LIST = ((0, 0), (0, 1), (0, 2), (1, 1), (1, 2), (2, 2))
MESH = pl.DeviceIdType.MESH
RUNS = ((17, 1), (19, 2), (0, 1), (18, 1), (1, 7), (14, 3), (8, 6), (21, 4))
ORDER = tuple(first + n for first, size in RUNS for n in range(size))
PLACE = tuple(ORDER.index(field) for field in range(len(ORDER)))
MIXED = (17, 19, 20, 0, 18)
MIXED_YZ = 4
SIZES = (1, 4, 3, 3, 1, 4, 5, 4)
STAGES = len(SIZES)
FIRST = tuple(sum(SIZES[:s]) for s in range(STAGES + 1))
MIX_STAGE = next(s for s in range(STAGES) if FIRST[s + 1] > PLACE[7])
TURNED = 3
FINAL = 0
Y_GROUPS = ((0, 1), (1, 2), (2, STAGES))
EARLY = 4
PAD = 8


def first_of(m2, m1, p1, p2):
    return (8.0 / 12.0) * (p1 - m1) - (1.0 / 12.0) * (p2 - m2)


def rates_of_plane(plane, rows, lanes, xb, tb, emit):
    lane = lax.broadcasted_iota(jnp.int32, (rows, lanes), 1)
    quad = lane & 3
    edge_one = (lane < 1) | (lane >= lanes - 1)
    edge_two = (lane < 2) | (lane >= lanes - 2)

    def cell(field, dz=0, dy=0):
        return xb[PLACE[field], plane + 2 + dz, PAD + dy : PAD + dy + rows, :]

    def strip(dz=0, dy=0):
        def side(slot):
            return tb[slot, plane + 2 + dz, PAD + dy : PAD + dy + rows, :]

        if tb.shape[0] == 1:
            return side(0)
        return jnp.where(quad < 2, side(0), side(1))

    def facing(edge):
        return jnp.where(
            quad < 2, pltpu.roll(edge, lanes - 2, 1), pltpu.roll(edge, 2, 1)
        )

    def inner(edge):
        return jnp.where(
            quad == 1, pltpu.roll(edge, 1, 1), pltpu.roll(edge, lanes - 1, 1)
        )

    def x_line(field, value, edge, edge_in):
        turn = (lanes - 2 - 4 * field) % lanes
        two = pltpu.roll(edge, turn, 1)
        one = pltpu.roll(edge_in, turn, 1)
        m2 = jnp.where(edge_two & (lane < 64), two, pltpu.roll(value, 2, 1))
        m1 = jnp.where(edge_one & (lane < 64), one, pltpu.roll(value, 1, 1))
        p1 = jnp.where(edge_one & (lane >= 64), one, pltpu.roll(value, lanes - 1, 1))
        p2 = jnp.where(edge_two & (lane >= 64), two, pltpu.roll(value, lanes - 2, 1))
        return m2, m1, p1, p2

    def y_line(read):
        return tuple(read(0, dy) for dy in (-2, -1, 1, 2))

    def z_line(read):
        return tuple(read(dz, 0) for dz in (-2, -1, 1, 2))

    edge = facing(strip())
    edge_in = inner(edge)

    centre, grad, curve, lap, mixed = {}, {}, {}, {}, {}
    need_lap = (0, 1, 2, 3, 4, 5, 6, 17, 18, 19, 20)
    shift = [cell(18), cell(19), cell(20)]
    advected = {}
    for field in range(len(ORDER)):
        centre[field] = cell(field)

    def differentiate(field):
        value = centre[field]
        read = functools.partial(cell, field)
        lines = [x_line(field, value, edge, edge_in), y_line(read), z_line(read)]
        near = [m1 + p1 for _, m1, p1, _ in lines]
        far = [m2 + p2 for m2, _, _, p2 in lines]
        near_sum = near[0] + near[1] + near[2]
        far_sum = far[0] + far[1] + far[2]
        smooth = far_sum - 4.0 * near_sum + 18.0 * value
        grads = [first_of(*line) for line in lines]
        grad[field] = grads
        advected[field] = (
            shift[0] * grads[0] + shift[1] * grads[1] + shift[2] * grads[2]
            - (DISSIPATE / 16.0) * smooth
        )
        if field in need_lap:
            lap[field] = (16.0 / 12.0) * near_sum - (1.0 / 12.0) * far_sum - 7.5 * value
        if field in MIXED:
            for axis in range(3):
                if field in (0, 17) or field == 18 + axis:
                    curve[field, axis] = (
                        (16.0 / 12.0) * near[axis] - (1.0 / 12.0) * far[axis] - 2.5 * value
                    )

    def mix():
        edge_y = facing(first_of(*y_line(strip)))
        edge_y_in = inner(edge_y)
        edge_z = facing(first_of(*z_line(strip)))
        edge_z_in = inner(edge_z)
        for field in MIXED:
            grads = grad[field]
            if field != 20:
                mixed[field, 0, 1] = first_of(*x_line(field, grads[1], edge_y, edge_y_in))
            if field != 19:
                mixed[field, 0, 2] = first_of(*x_line(field, grads[2], edge_z, edge_z_in))
            if field != 18:
                mixed[field, 1, 2] = first_of(
                    *(
                        first_of(*(cell(field, dz, dy) for dy in (-2, -1, 1, 2)))
                        for dz in (-2, -1, 1, 2)
                    )
                )

    def second(field, one, two):
        if one == two:
            return curve[field, one]
        return mixed[field, min(one, two), max(one, two)]

    def sym(table, one, two):
        return table[PAIR_SLOT[one][two]]

    metric = [centre[1 + k] for k in range(6)]
    traceless = [centre[8 + k] for k in range(6)]
    inverse = [
        (2.0 - metric[k]) if one == two else -metric[k]
        for k, (one, two) in enumerate(PAIR_LIST)
    ]

    def contract(left, right):
        diag = left[0] * right[0] + left[3] * right[3] + left[5] * right[5]
        off = left[1] * right[1] + left[2] * right[2] + left[4] * right[4]
        return diag + 2.0 * off

    def lie_of(table, one, two):
        total = None
        for k in range(3):
            if one == two:
                term = 2.0 * (sym(table, one, k) * grad[18 + k][one])
            else:
                term = (
                    sym(table, one, k) * grad[18 + k][two]
                    + sym(table, two, k) * grad[18 + k][one]
                )
            total = term if total is None else total + term
        return total

    chi, trace, lapse, theta = centre[0], centre[7], centre[17], centre[24]
    shared, gauges = {}, {}

    def once(name, make):
        if name not in shared:
            shared[name] = make()
        return shared[name]

    def third_div():
        div = grad[18][0] + grad[19][1] + grad[20][2]
        return (2.0 / 3.0) * div

    def lapse_terms():
        mix()
        lapse_dd = [second(17, one, two) for one, two in PAIR_LIST]
        return lapse_dd, contract(inverse, lapse_dd)

    def ricci_terms():
        half_over = 0.5 * once("over", lambda: 1.0 / chi)
        ricci = []
        for k, (one, two) in enumerate(PAIR_LIST):
            conf = second(0, one, two)
            if one == two:
                conf = conf + lap[0]
                grads_g = grad[14 + one][one]
            else:
                grads_g = 0.5 * (grad[14 + two][one] + grad[14 + one][two])
            ricci.append(-0.5 * lap[1 + k] + grads_g + conf * half_over)
        return ricci, contract(inverse, ricci)

    def rate_of(field):
        rate = advected[field]
        if field == 17:
            return rate - 2.0 * lapse * (trace - 2.0 * theta)
        if field in (18, 19, 20):
            return rate + 0.75 * centre[field + 3]
        third = once("div", third_div)
        if field == 0:
            return rate + (2.0 / 3.0) * chi * (lapse * trace) - chi * third
        if field in range(1, 7):
            k = field - 1
            one, two = PAIR_LIST[k]
            lie = lie_of(metric, one, two)
            return rate - 2.0 * lapse * traceless[k] + lie - metric[k] * third
        lapse_dd, lapse_trace = once("lapse", lapse_terms)
        squares = once("squares", lambda: contract(traceless, traceless))
        if field == 7:
            return (
                rate
                - chi * lapse_trace
                + lapse * (squares + trace * trace * (1.0 / 3.0))
                + KAPPA_ONE * lapse * theta
            )
        if field in (14, 15, 16):
            one = field - 14
            a_lapse = sum(sym(traceless, one, k) * grad[17][k] for k in range(3))
            a_chi = sum(sym(traceless, one, k) * grad[0][k] for k in range(3))
            g_trace = sum(sym(inverse, one, k) * grad[7][k] for k in range(3))
            b_mixed = sum(second(18 + k, one, k) for k in range(3))
            g_shift = sum(centre[14 + k] * grad[18 + one][k] for k in range(3))
            over_chi = once("over", lambda: 1.0 / chi)
            gauges[one] = (
                -2.0 * a_lapse
                - lapse * ((4.0 / 3.0) * g_trace + 3.0 * (a_chi * over_chi))
                + lap[18 + one]
                + b_mixed * (1.0 / 3.0)
                + centre[14 + one] * third
                - g_shift
            )
            return rate + gauges[one]
        if field in (21, 22, 23):
            return rate + gauges[field - 21] - DRIVER_ETA * centre[field]
        ricci, ricci_trace = once("ricci", ricci_terms)
        if field == 24:
            return (
                rate
                + 0.5 * lapse * (chi * ricci_trace + (2.0 / 3.0) * trace * trace - squares)
                - 2.0 * KAPPA_ONE * lapse * theta
            )
        k = field - 8
        one, two = PAIR_LIST[k]
        third_trace = once("trace", lambda: (lapse * ricci_trace - lapse_trace) * (1.0 / 3.0))
        free = lapse * ricci[k] - lapse_dd[k] - metric[k] * third_trace
        product = sum(
            sym(traceless, one, m) * sym(traceless, m, two) for m in range(3)
        )
        return (
            rate
            + chi * free
            + lapse * (trace * traceless[k] - 2.0 * product)
            + lie_of(traceless, one, two)
            - traceless[k] * third
        )

    for stage in range(STAGES):
        for field in ORDER[FIRST[stage] : FIRST[stage + 1]]:
            differentiate(field)
        for field in ORDER[FIRST[stage] : FIRST[stage + 1]]:
            emit(field, rate_of(field))
        yield


def section_kernel(
    sizes, section, base, accum, ns_out, na_out, slab,
    xb, tb, eb, tile, inputs, local_sem, halo_send, halo_recv,
    line_send, gather_recv, chain,
):
    gx, gy, gz = sizes
    fields, planes, rows, lanes = section.shape
    i, j, k = (lax.axis_index(name) for name in ("gx", "gy", "gz"))

    def device(dx=0, dy=0, dz=0):
        return (
            lax.rem(i + dx + gx, gx),
            lax.rem(j + dy + gy, gy),
            lax.rem(k + dz + gz, gz),
        )

    x_steps = (1,) if gx == 2 else (1, -1)

    def landed(sem, ref):
        pltpu.make_async_remote_copy(
            src_ref=ref, dst_ref=ref, send_sem=sem, recv_sem=sem,
            device_id=device(0, 1, 0), device_id_type=MESH,
        ).wait_recv()

    def left(sem, ref):
        pltpu.make_async_remote_copy(
            src_ref=ref, dst_ref=ref, send_sem=sem, recv_sem=sem,
            device_id=device(0, 1, 0), device_id_type=MESH,
        ).wait_send()

    own_planes, own_rows = pl.ds(2, planes), pl.ds(PAD, rows)
    SENT = dict(z=0, y=0, yz=1, ze=1, x=2, xy=2, xz=2)
    GOT_Z, GOT_Y = 0, STAGES
    GOT_YZ = STAGES + len(Y_GROUPS)
    GOT_X, GOT_XY, GOT_XZ, GOT_ZE = (GOT_YZ + n for n in (1, 2, 3, 4))
    mixed = pl.ds(0, MIXED_YZ)

    def halo(delta, kind, got, src, dst):
        return pltpu.make_async_remote_copy(
            src_ref=src, dst_ref=dst,
            send_sem=halo_send.at[SENT[kind]], recv_sem=halo_recv.at[got],
            device_id=device(*delta), device_id_type=MESH,
        )

    def planes_of(dz):
        if dz == 1:
            return pl.ds(planes, 2), pl.ds(0, 2)
        return pl.ds(2, 2), pl.ds(2 + planes, 2)

    def rows_of(dy):
        if dy == 1:
            return pl.ds(PAD + rows - 2, 2), pl.ds(PAD - 2, 2)
        return pl.ds(PAD, 2), pl.ds(PAD + rows, 2)

    def run_of(low, high):
        return pl.ds(FIRST[low], FIRST[high] - FIRST[low])

    def z_face(stage, dz):
        run = run_of(stage, stage + 1)
        src, dst = planes_of(dz)
        return halo(
            (0, 0, dz), "z", GOT_Z + stage,
            xb.at[run, src, own_rows, :], xb.at[run, dst, own_rows, :],
        )

    def y_face(group, dy):
        run = run_of(*Y_GROUPS[group])
        src, dst = rows_of(dy)
        return halo(
            (0, dy, 0), "y", GOT_Y + group,
            xb.at[run, own_planes, src, :], xb.at[run, own_planes, dst, :],
        )

    def z_edge(dz, dy):
        src, _ = planes_of(dz)
        cut, _ = rows_of(dy)
        place = pl.ds(0 if dz == 1 else 2, 2), pl.ds(0 if dy == 1 else 2, 2)
        return halo(
            (0, 0, dz), "ze", GOT_ZE,
            xb.at[mixed, src, cut, :], eb.at[mixed, place[0], place[1], :],
        )

    def yz_edge(dy, side):
        _, dst = rows_of(dy)
        cut = pl.ds(0, 2) if side == 0 else pl.ds(2 + planes, 2)
        return halo(
            (0, dy, 0), "yz", GOT_YZ,
            eb.at[mixed, pl.ds(2 * side, 2), pl.ds(0 if dy == 1 else 2, 2), :],
            xb.at[mixed, cut, dst, :],
        )

    def xy_edge(slot, dy):
        src, dst = rows_of(dy)
        return halo(
            (0, dy, 0), "xy", GOT_XY,
            tb.at[slot, own_planes, src, :], tb.at[slot, own_planes, dst, :],
        )

    def xz_edge(slot, dz):
        src, dst = planes_of(dz)
        return halo(
            (0, 0, dz), "xz", GOT_XZ,
            tb.at[slot, src, own_rows, :], tb.at[slot, dst, own_rows, :],
        )

    steps, slots = (1, -1), range(len(x_steps))
    z_faces = [[z_face(s, dz) for dz in steps] for s in range(STAGES)]
    y_faces = [[y_face(g, dy) for dy in steps] for g in range(len(Y_GROUPS))]
    z_edges = [z_edge(dz, dy) for dz in steps for dy in steps]
    yz_edges = [yz_edge(dy, side) for dy in steps for side in (0, 1)]
    x_faces = [
        halo((dx, 0, 0), "x", GOT_X, tile.at[0], tb.at[slot, own_planes, own_rows, :])
        for slot, dx in enumerate(x_steps)
    ]
    xy_edges = [xy_edge(slot, dy) for slot in slots for dy in steps]
    xz_edges = [xz_edge(slot, dz) for slot in slots for dz in steps]

    def z_landed(s):
        landed(halo_recv.at[GOT_Z + s], xb.at[run_of(s, s + 1), pl.ds(0, 4), own_rows, :])

    def y_landed(g):
        landed(halo_recv.at[GOT_Y + g], xb.at[run_of(*Y_GROUPS[g]), own_planes, pl.ds(0, 4), :])

    every = pl.ds(0, len(x_steps))

    def x_landed():
        landed(halo_recv.at[GOT_X], tb.at[every, own_planes, own_rows, :])

    def edges_landed():
        landed(halo_recv.at[GOT_YZ], xb.at[mixed, pl.ds(0, 4), pl.ds(0, 4), :])
        landed(halo_recv.at[GOT_XY], tb.at[every, own_planes, pl.ds(0, 4), :])
        landed(halo_recv.at[GOT_XZ], tb.at[every, pl.ds(0, 4), own_rows, :])

    def halos_left():
        left(halo_send.at[SENT["z"]], xb.at[:, pl.ds(0, 4), pl.ds(0, rows + planes), :])
        left(halo_send.at[SENT["yz"]], xb.at[mixed, pl.ds(0, 4), pl.ds(0, 8), :])
        tiles = tb.at[every, pl.ds(0, 4), pl.ds(0, planes * rows // 4 + planes + rows), :]
        left(halo_send.at[SENT["x"]], tiles)

    def start(some):
        for copy in some:
            copy.start()

    loads = []
    place = 0
    for first, size in RUNS:
        loads.append(
            pltpu.make_async_copy(
                section.at[pl.ds(first, size)],
                xb.at[pl.ds(place, size), own_planes, own_rows, :],
                local_sem.at[0],
            )
        )
        place += size
    load_base = pltpu.make_async_copy(base, inputs.at[0], local_sem.at[1])
    load_accum = pltpu.make_async_copy(accum, inputs.at[1], local_sem.at[1])
    chained = gy > 2
    faces = [(0, 0, 1), (0, 0, -1)] + [(dx, 0, 0) for dx in x_steps]
    barrier = pltpu.get_barrier_semaphore()

    def greet(sem, delta):
        pl.semaphore_signal(sem, inc=1, device_id=device(*delta), device_id_type=MESH)

    for delta in faces + [(0, -1, 0)]:
        greet(barrier, delta)
    if chained:
        pl.when(j + 1 < gy)(lambda: greet(barrier, (0, 1, 0)))
    else:
        greet(barrier, (0, 1, 0))
    start(loads)
    load_base.start()
    load_accum.start()

    lane = lax.broadcasted_iota(jnp.int32, (rows, lanes), 1)

    own_cells = xb.at[:, own_planes, own_rows, :]
    pltpu.make_async_copy(own_cells, own_cells, local_sem.at[0]).wait()
    for plane in range(planes):
        packed = jnp.zeros((rows, lanes), jnp.float32)
        for field in range(fields):
            value = xb[PLACE[field], plane + 2, PAD : PAD + rows, :]
            ends = pltpu.roll(value, (4 * field + 2) % lanes, 1)
            packed = jnp.where((lane >> 2) == field, ends, packed)
        tile[0, plane] = packed
    if chained:
        pl.when(j == 0)(lambda: pl.semaphore_wait(barrier, len(faces) + 1))
        pl.when(j > 0)(lambda: pl.semaphore_wait(barrier, len(faces) + 2))
    else:
        pl.semaphore_wait(barrier, len(faces) + 2)
    def far(some):
        pl.when(j == 0)(lambda: start(some))

    def near(some):
        up, down = some[::2], some[1::2]
        start(up)
        pl.when(j > 0)(lambda: start(down))

    if not chained:
        near = start
    else:
        pl.when(j == gy - 2)(lambda: greet(chain, (0, -1, 0)))
    start(z_faces[0])
    near(y_faces[0])
    start(x_faces + z_edges + z_faces[1])
    near(y_faces[1])
    start(z_faces[2])
    near(y_faces[2])
    for s in range(3, EARLY):
        start(z_faces[s])
    if chained:
        @pl.when(j < gy - 2)
        def _():
            pl.semaphore_wait(chain, 1)
            pl.when(j > 0)(lambda: greet(chain, (0, -1, 0)))

        for faces_of in y_faces:
            far(faces_of[1::2])
    pltpu.make_async_copy(inputs, inputs, local_sem.at[1]).wait()

    own_y = pl.ds(pl.multiple_of(j * rows, rows), rows)
    own_x = pl.ds(pl.multiple_of(i * lanes, lanes), lanes)
    paired = gx == 2 and gy % 2 == 0
    turned = TURNED if paired else 0
    kept = STAGES - turned
    pair = j + 1 - 2 * lax.rem(j, 2)
    other = 1 - i
    towards = ((0, 1), (0, -1), (1, 0), (-1, 0))
    TURN, BULK, BULK_TURNED, PAIR_TURNED = ((gy - 1) * STAGES + n for n in range(4))
    SENT_PAIR, SENT_TURNED = 3, 4

    def piece(bi, bj, low, high):
        return slab.at[
            run_of(low, high),
            :,
            pl.ds(pl.multiple_of(bj * rows, rows), rows),
            pl.ds(pl.multiple_of(bi * lanes, lanes), lanes),
        ]

    def line(link, bi, bj, c, sent, got):
        dx, dy = towards[link]
        part = piece(bi, bj, c, c + 1)
        pltpu.make_async_remote_copy(
            src_ref=part,
            dst_ref=part,
            send_sem=line_send.at[sent],
            recv_sem=gather_recv.at[got],
            device_id=device(dx, dy, 0),
            device_id_type=MESH,
        ).start()

    def number(link, bi, bj, c):
        if paired:
            return (bj - link) * STAGES + c
        return (bi * gy + bj) * STAGES + c

    def send(link, bi, bj, c):
        line(link, bi, bj, c, link, number(link, bi, bj, c))

    def arrive(link, bi, bj, c):
        landed(gather_recv.at[number(link, bi, bj, c)], piece(bi, bj, c, c + 1))

    def x_links(body):
        @pl.when(i + 1 < gx)
        def _():
            body(2)

        @pl.when(i > 0)
        def _():
            body(3)

    def cross(bj, c, distance):
        if not paired:
            x_links(lambda link: send(link, i, bj, c))
        elif c < kept:
            if distance == 1:
                line(2, i, bj, c, jnp.where(bj == pair, SENT_PAIR, 2), BULK)
            else:
                line(2, i, bj, c, 2, BULK)
        elif distance == 0:
            line(2, i, bj, c, 2, TURN)
        elif distance == 1:
            pl.when(bj != pair)(lambda: line(2, i, bj, c, 2, BULK_TURNED))
        else:
            line(2, i, bj, c, 2, BULK_TURNED)

    def held(c, ahead):
        if c < kept:
            return False
        return (pair == j + ahead) & ((pair == 0) | (pair == gy - 1))

    def send_own(c):
        @pl.when((j + 1 < gy) & jnp.logical_not(held(c, 1)))
        def _():
            send(0, i, j, c)

        @pl.when((j > 0) & jnp.logical_not(held(c, -1)))
        def _():
            send(1, i, j, c)

        cross(j, c, 0)

    def send_held(c):
        def go(link, ahead):
            pl.when(held(c, ahead))(
                lambda: line(link, i, j, c, link, number(link, i, j, kept))
            )

        go(0, 1)
        go(1, -1)

    def pass_on(d, c):
        ended = d == 1 and c >= kept

        @pl.when((j - d >= 0) & (j + 1 < gy) if ended else j - d >= 0)
        def _():
            bj = j - d
            arrive(0, i, bj, c)

            @pl.when(j + 1 < gy)
            def _():
                send(0, i, bj, c)

            cross(bj, c, d)

        @pl.when((j + d < gy) & (j > 0) if ended else j + d < gy)
        def _():
            bj = j + d
            arrive(1, i, bj, c)

            @pl.when(j > 0)
            def _():
                send(1, i, bj, c)

            cross(bj, c, d)

    def turn():
        landed(gather_recv.at[TURN], piece(other, j, kept, STAGES))
        for c in range(kept, STAGES):
            @pl.when(pair > j)
            def _():
                line(0, other, j, c, SENT_TURNED, PAIR_TURNED)

            @pl.when(pair < j)
            def _():
                line(1, other, j, c, SENT_TURNED, PAIR_TURNED)

    def emit_at(plane):
        def emit(field, rate):
            moved = inputs[0, field, plane] + (0.5 * STEP_DT) * rate
            slab[PLACE[field], plane, own_y, own_x] = moved
            ns_out[field, plane] = moved
            na_out[field, plane] = inputs[1, field, plane] + (STEP_DT / 3.0) * rate

        return emit

    x_landed()
    start(xz_edges + xy_edges)
    for s in range(EARLY, STAGES):
        start(z_faces[s])
    z_landed(0)
    work = [
        rates_of_plane(plane, rows, lanes, xb, tb, emit_at(plane))
        for plane in range(planes)
    ]

    def own_stage(s):
        if s:
            z_landed(s)
        else:
            landed(halo_recv.at[GOT_ZE], eb.at[mixed, pl.ds(0, 4), pl.ds(0, 4), :])
            start(yz_edges)
        if s < len(Y_GROUPS):
            y_landed(s)
        if s == MIX_STAGE:
            edges_landed()
        for part in work:
            next(part)
        send_own(s)

    LAG = tuple(3 * d for d in range(gy))
    final = STAGES - 1 + LAG[gy - 2] + FINAL
    for v in range(STAGES + LAG[gy - 1]):
        if v < STAGES:
            own_stage(v)
        for d in range(1, gy):
            if 0 <= v - LAG[d] < STAGES:
                pass_on(d, v - LAG[d])
        for c in range(kept, STAGES):
            if v == final - (c == kept):
                send_held(c)
        if v == final and turned:
            turn()

    halos_left()

    def whole(n_rows, n_lanes, low=0, high=STAGES):
        return slab.at[run_of(low, high), :, pl.ds(0, n_rows), pl.ds(0, n_lanes)]

    if paired:
        if turned:
            landed(gather_recv.at[PAIR_TURNED], whole(rows, lanes, kept))

            for link, end in ((1, 0), (0, gy - 1)):
                @pl.when(j == end)
                def _():
                    slot = gather_recv.at[number(link, i, pair, kept)]
                    landed(slot, whole(rows, lanes, kept))
        landed(gather_recv.at[BULK], whole(gy * rows, lanes, 0, kept))
        if turned and gy > 2:
            landed(gather_recv.at[BULK_TURNED], whole((gy - 2) * rows, lanes, kept))
    else:
        for d in range(1, gx):
            def row(bj, carry, d=d):
                @pl.when(i - d >= 0)
                def _():
                    for c in range(STAGES):
                        arrive(2, i - d, bj, c)

                        @pl.when(i + 1 < gx)
                        def _():
                            send(2, i - d, bj, c)

                @pl.when(i + d < gx)
                def _():
                    for c in range(STAGES):
                        arrive(3, i + d, bj, c)

                        @pl.when(i > 0)
                        def _():
                            send(3, i + d, bj, c)

                return carry

            lax.fori_loop(0, gy, row, 0)

    for n in range(1, gy):
        @pl.when(j == n - 1)
        def _():
            left(line_send.at[0], whole(n * rows, lanes))

        @pl.when(j == gy - n)
        def _():
            left(line_send.at[1], whole(n * rows, lanes))

    if paired:
        left(line_send.at[2], whole((gy - 1) * rows, lanes))
        left(line_send.at[SENT_PAIR], whole(rows, lanes, 0, kept))
        if turned:
            left(line_send.at[SENT_TURNED], whole(rows, lanes, kept))
    else:
        for n in range(1, gx):
            @pl.when(i == n - 1)
            def _():
                left(line_send.at[2], whole(gy * rows, n * lanes))

            @pl.when(i == gx - n)
            def _():
                left(line_send.at[3], whole(gy * rows, n * lanes))


def put_out(ns_in, na_in, slab_in, ns_out, na_out, slab_out, sem):
    place = 0
    for first, size in RUNS:
        pltpu.make_async_copy(
            slab_in.at[pl.ds(place, size)], slab_out.at[pl.ds(first, size)], sem.at[0]
        ).start()
        place += size
    pltpu.make_async_copy(ns_in, ns_out, sem.at[1]).start()
    pltpu.make_async_copy(na_in, na_out, sem.at[2]).start()
    pltpu.make_async_copy(slab_in, slab_out, sem.at[0]).wait()
    pltpu.make_async_copy(ns_in, ns_out, sem.at[1]).wait()
    pltpu.make_async_copy(na_in, na_out, sem.at[2]).wait()


def shards(sizes, section, base, accum):
    gx, gy, gz = sizes
    fields, planes, rows, lanes = section.shape
    slots = 1 if gx == 2 else 2
    arrivals = (gy - 1) * STAGES + 4 if gx == 2 and gy % 2 == 0 else gx * gy * STAGES
    any_spec = pl.BlockSpec(memory_space=pl.ANY)
    block = jax.ShapeDtypeStruct(section.shape, jnp.float32)
    slab = jax.ShapeDtypeStruct((fields, planes, gy * rows, gx * lanes), jnp.float32)
    dma = pltpu.SemaphoreType.DMA
    staged = pl.pallas_call(
        functools.partial(section_kernel, sizes),
        out_shape=tuple(pltpu.VMEM(a.shape, a.dtype) for a in (block, block, slab)),
        in_specs=[pl.BlockSpec(memory_space=pltpu.HBM)] * 3,
        out_specs=(pl.BlockSpec(memory_space=pltpu.VMEM),) * 3,
        scratch_shapes=[
            pltpu.VMEM((fields, planes + 4, rows + 2 * PAD, lanes), jnp.float32),
            pltpu.VMEM((slots, planes + 4, rows + 2 * PAD, lanes), jnp.float32),
            pltpu.VMEM((MIXED_YZ, 4, 8, lanes), jnp.float32),
            pltpu.VMEM((1, planes, rows, lanes), jnp.float32),
            pltpu.VMEM((2,) + section.shape, jnp.float32),
            dma((2,)),
            dma((3,)),
            dma((STAGES + len(Y_GROUPS) + 5,)),
            dma((5,)),
            dma((arrivals,)),
            pltpu.SemaphoreType.REGULAR,
        ],
        compiler_params=pltpu.CompilerParams(collective_id=0, has_side_effects=True, vmem_limit_bytes=24 << 20),
    )(*(pltpu.with_memory_space_constraint(x, pltpu.HBM) for x in (section, base, accum)))
    return pl.pallas_call(
        put_out,
        out_shape=(block, block, slab),
        in_specs=[pl.BlockSpec(memory_space=pltpu.VMEM)] * 3,
        out_specs=(any_spec,) * 3,
        scratch_shapes=[dma((3,))],
        compiler_params=pltpu.CompilerParams(vmem_limit_bytes=8 << 20),
    )(*staged)


def solution(mesh):
    sizes = tuple(mesh.shape[name] for name in ("gx", "gy", "gz"))
    spec = P(None, "gz", "gy", "gx")
    return jax.shard_map(
        functools.partial(shards, sizes),
        mesh=mesh,
        in_specs=(spec, spec, spec),
        out_specs=(spec, spec, P(None, "gz", None, None)),
        check_vma=False,
    )
```

```python
import functools

import jax
import jax.numpy as jnp
from jax import lax
from jax.experimental import pallas as pl
from jax.experimental.pallas import tpu as pltpu
from jax.sharding import PartitionSpec as P

STEP_DT = 0.25
DISSIPATE = 0.1
DRIVER_ETA = 2.0
KAPPA_ONE = 0.1
PAIR_SLOT = ((0, 1, 2), (1, 3, 4), (2, 4, 5))
PAIR_LIST = ((0, 0), (0, 1), (0, 2), (1, 1), (1, 2), (2, 2))
MESH = pl.DeviceIdType.MESH
RUNS = ((17, 1), (19, 2), (0, 1), (18, 1), (1, 7), (14, 3), (8, 6), (21, 4))
ORDER = tuple(first + n for first, size in RUNS for n in range(size))
PLACE = tuple(ORDER.index(field) for field in range(len(ORDER)))
MIXED = (17, 19, 20, 0, 18)
MIXED_YZ = 4
SIZES = (1, 4, 3, 3, 1, 4, 5, 4)
STAGES = len(SIZES)
FIRST = tuple(sum(SIZES[:s]) for s in range(STAGES + 1))
MIX_STAGE = next(s for s in range(STAGES) if FIRST[s + 1] > PLACE[7])
TURNED = 3
FINAL = 0
Y_GROUPS = ((0, 1), (1, 2), (2, STAGES))
EARLY = 4
PAD = 8


def first_of(m2, m1, p1, p2):
    return (8.0 / 12.0) * (p1 - m1) - (1.0 / 12.0) * (p2 - m2)


def rates_of_plane(plane, rows, lanes, xb, tb, emit):
    lane = lax.broadcasted_iota(jnp.int32, (rows, lanes), 1)
    quad = lane & 3
    edge_one = (lane < 1) | (lane >= lanes - 1)
    edge_two = (lane < 2) | (lane >= lanes - 2)

    def cell(field, dz=0, dy=0):
        return xb[PLACE[field], plane + 2 + dz, PAD + dy : PAD + dy + rows, :]

    def strip(dz=0, dy=0):
        def side(slot):
            return tb[slot, plane + 2 + dz, PAD + dy : PAD + dy + rows, :]

        if tb.shape[0] == 1:
            return side(0)
        return jnp.where(quad < 2, side(0), side(1))

    def facing(edge):
        return jnp.where(
            quad < 2, pltpu.roll(edge, lanes - 2, 1), pltpu.roll(edge, 2, 1)
        )

    def inner(edge):
        return jnp.where(
            quad == 1, pltpu.roll(edge, 1, 1), pltpu.roll(edge, lanes - 1, 1)
        )

    def x_line(field, value, edge, edge_in):
        turn = (lanes - 2 - 4 * field) % lanes
        two = pltpu.roll(edge, turn, 1)
        one = pltpu.roll(edge_in, turn, 1)
        m2 = jnp.where(edge_two & (lane < 64), two, pltpu.roll(value, 2, 1))
        m1 = jnp.where(edge_one & (lane < 64), one, pltpu.roll(value, 1, 1))
        p1 = jnp.where(edge_one & (lane >= 64), one, pltpu.roll(value, lanes - 1, 1))
        p2 = jnp.where(edge_two & (lane >= 64), two, pltpu.roll(value, lanes - 2, 1))
        return m2, m1, p1, p2

    def y_line(read):
        return tuple(read(0, dy) for dy in (-2, -1, 1, 2))

    def z_line(read):
        return tuple(read(dz, 0) for dz in (-2, -1, 1, 2))

    edge = facing(strip())
    edge_in = inner(edge)

    centre, grad, curve, lap, mixed = {}, {}, {}, {}, {}
    need_lap = (0, 1, 2, 3, 4, 5, 6, 17, 18, 19, 20)
    shift = [cell(18), cell(19), cell(20)]
    advected = {}
    for field in range(len(ORDER)):
        centre[field] = cell(field)

    def differentiate(field):
        value = centre[field]
        read = functools.partial(cell, field)
        lines = [x_line(field, value, edge, edge_in), y_line(read), z_line(read)]
        near = [m1 + p1 for _, m1, p1, _ in lines]
        far = [m2 + p2 for m2, _, _, p2 in lines]
        near_sum = near[0] + near[1] + near[2]
        far_sum = far[0] + far[1] + far[2]
        smooth = far_sum - 4.0 * near_sum + 18.0 * value
        grads = [first_of(*line) for line in lines]
        grad[field] = grads
        advected[field] = (
            shift[0] * grads[0] + shift[1] * grads[1] + shift[2] * grads[2]
            - (DISSIPATE / 16.0) * smooth
        )
        if field in need_lap:
            lap[field] = (16.0 / 12.0) * near_sum - (1.0 / 12.0) * far_sum - 7.5 * value
        if field in MIXED:
            for axis in range(3):
                if field in (0, 17) or field == 18 + axis:
                    curve[field, axis] = (
                        (16.0 / 12.0) * near[axis] - (1.0 / 12.0) * far[axis] - 2.5 * value
                    )

    def mix():
        edge_y = facing(first_of(*y_line(strip)))
        edge_y_in = inner(edge_y)
        edge_z = facing(first_of(*z_line(strip)))
        edge_z_in = inner(edge_z)
        for field in MIXED:
            grads = grad[field]
            if field != 20:
                mixed[field, 0, 1] = first_of(*x_line(field, grads[1], edge_y, edge_y_in))
            if field != 19:
                mixed[field, 0, 2] = first_of(*x_line(field, grads[2], edge_z, edge_z_in))
            if field != 18:
                mixed[field, 1, 2] = first_of(
                    *(
                        first_of(*(cell(field, dz, dy) for dy in (-2, -1, 1, 2)))
                        for dz in (-2, -1, 1, 2)
                    )
                )

    def second(field, one, two):
        if one == two:
            return curve[field, one]
        return mixed[field, min(one, two), max(one, two)]

    def sym(table, one, two):
        return table[PAIR_SLOT[one][two]]

    metric = [centre[1 + k] for k in range(6)]
    traceless = [centre[8 + k] for k in range(6)]
    inverse = [
        (2.0 - metric[k]) if one == two else -metric[k]
        for k, (one, two) in enumerate(PAIR_LIST)
    ]

    def contract(left, right):
        diag = left[0] * right[0] + left[3] * right[3] + left[5] * right[5]
        off = left[1] * right[1] + left[2] * right[2] + left[4] * right[4]
        return diag + 2.0 * off

    def lie_of(table, one, two):
        total = None
        for k in range(3):
            if one == two:
                term = 2.0 * (sym(table, one, k) * grad[18 + k][one])
            else:
                term = (
                    sym(table, one, k) * grad[18 + k][two]
                    + sym(table, two, k) * grad[18 + k][one]
                )
            total = term if total is None else total + term
        return total

    chi, trace, lapse, theta = centre[0], centre[7], centre[17], centre[24]
    shared, gauges = {}, {}

    def once(name, make):
        if name not in shared:
            shared[name] = make()
        return shared[name]

    def third_div():
        div = grad[18][0] + grad[19][1] + grad[20][2]
        return (2.0 / 3.0) * div

    def lapse_terms():
        mix()
        lapse_dd = [second(17, one, two) for one, two in PAIR_LIST]
        return lapse_dd, contract(inverse, lapse_dd)

    def ricci_terms():
        half_over = 0.5 * once("over", lambda: 1.0 / chi)
        ricci = []
        for k, (one, two) in enumerate(PAIR_LIST):
            conf = second(0, one, two)
            if one == two:
                conf = conf + lap[0]
                grads_g = grad[14 + one][one]
            else:
                grads_g = 0.5 * (grad[14 + two][one] + grad[14 + one][two])
            ricci.append(-0.5 * lap[1 + k] + grads_g + conf * half_over)
        return ricci, contract(inverse, ricci)

    def rate_of(field):
        rate = advected[field]
        if field == 17:
            return rate - 2.0 * lapse * (trace - 2.0 * theta)
        if field in (18, 19, 20):
            return rate + 0.75 * centre[field + 3]
        third = once("div", third_div)
        if field == 0:
            return rate + (2.0 / 3.0) * chi * (lapse * trace) - chi * third
        if field in range(1, 7):
            k = field - 1
            one, two = PAIR_LIST[k]
            lie = lie_of(metric, one, two)
            return rate - 2.0 * lapse * traceless[k] + lie - metric[k] * third
        lapse_dd, lapse_trace = once("lapse", lapse_terms)
        squares = once("squares", lambda: contract(traceless, traceless))
        if field == 7:
            return (
                rate
                - chi * lapse_trace
                + lapse * (squares + trace * trace * (1.0 / 3.0))
                + KAPPA_ONE * lapse * theta
            )
        if field in (14, 15, 16):
            one = field - 14
            a_lapse = sum(sym(traceless, one, k) * grad[17][k] for k in range(3))
            a_chi = sum(sym(traceless, one, k) * grad[0][k] for k in range(3))
            g_trace = sum(sym(inverse, one, k) * grad[7][k] for k in range(3))
            b_mixed = sum(second(18 + k, one, k) for k in range(3))
            g_shift = sum(centre[14 + k] * grad[18 + one][k] for k in range(3))
            over_chi = once("over", lambda: 1.0 / chi)
            gauges[one] = (
                -2.0 * a_lapse
                - lapse * ((4.0 / 3.0) * g_trace + 3.0 * (a_chi * over_chi))
                + lap[18 + one]
                + b_mixed * (1.0 / 3.0)
                + centre[14 + one] * third
                - g_shift
            )
            return rate + gauges[one]
        if field in (21, 22, 23):
            return rate + gauges[field - 21] - DRIVER_ETA * centre[field]
        ricci, ricci_trace = once("ricci", ricci_terms)
        if field == 24:
            return (
                rate
                + 0.5 * lapse * (chi * ricci_trace + (2.0 / 3.0) * trace * trace - squares)
                - 2.0 * KAPPA_ONE * lapse * theta
            )
        k = field - 8
        one, two = PAIR_LIST[k]
        third_trace = once("trace", lambda: (lapse * ricci_trace - lapse_trace) * (1.0 / 3.0))
        free = lapse * ricci[k] - lapse_dd[k] - metric[k] * third_trace
        product = sum(
            sym(traceless, one, m) * sym(traceless, m, two) for m in range(3)
        )
        return (
            rate
            + chi * free
            + lapse * (trace * traceless[k] - 2.0 * product)
            + lie_of(traceless, one, two)
            - traceless[k] * third
        )

    for stage in range(STAGES):
        for field in ORDER[FIRST[stage] : FIRST[stage + 1]]:
            differentiate(field)
        for field in ORDER[FIRST[stage] : FIRST[stage + 1]]:
            emit(field, rate_of(field))
        yield


def section_kernel(
    sizes, section, base, accum, ns_out, na_out, slab,
    xb, tb, eb, tile, inputs, local_sem, halo_send, halo_recv,
    line_send, gather_recv, chain,
):
    gx, gy, gz = sizes
    fields, planes, rows, lanes = section.shape
    i, j, k = (lax.axis_index(name) for name in ("gx", "gy", "gz"))

    def device(dx=0, dy=0, dz=0):
        return (
            lax.rem(i + dx + gx, gx),
            lax.rem(j + dy + gy, gy),
            lax.rem(k + dz + gz, gz),
        )

    x_steps = (1,) if gx == 2 else (1, -1)

    def landed(sem, ref):
        pltpu.make_async_remote_copy(
            src_ref=ref, dst_ref=ref, send_sem=sem, recv_sem=sem,
            device_id=device(0, 1, 0), device_id_type=MESH,
        ).wait_recv()

    def left(sem, ref):
        pltpu.make_async_remote_copy(
            src_ref=ref, dst_ref=ref, send_sem=sem, recv_sem=sem,
            device_id=device(0, 1, 0), device_id_type=MESH,
        ).wait_send()

    own_planes, own_rows = pl.ds(2, planes), pl.ds(PAD, rows)
    SENT = dict(z=0, y=0, yz=1, ze=1, x=2, xy=2, xz=2)
    GOT_Z, GOT_Y = 0, STAGES
    GOT_YZ = STAGES + len(Y_GROUPS)
    GOT_X, GOT_XY, GOT_XZ, GOT_ZE = (GOT_YZ + n for n in (1, 2, 3, 4))
    mixed = pl.ds(0, MIXED_YZ)

    def halo(delta, kind, got, src, dst):
        return pltpu.make_async_remote_copy(
            src_ref=src, dst_ref=dst,
            send_sem=halo_send.at[SENT[kind]], recv_sem=halo_recv.at[got],
            device_id=device(*delta), device_id_type=MESH,
        )

    def planes_of(dz):
        if dz == 1:
            return pl.ds(planes, 2), pl.ds(0, 2)
        return pl.ds(2, 2), pl.ds(2 + planes, 2)

    def rows_of(dy):
        if dy == 1:
            return pl.ds(PAD + rows - 2, 2), pl.ds(PAD - 2, 2)
        return pl.ds(PAD, 2), pl.ds(PAD + rows, 2)

    def run_of(low, high):
        return pl.ds(FIRST[low], FIRST[high] - FIRST[low])

    def z_face(stage, dz):
        run = run_of(stage, stage + 1)
        src, dst = planes_of(dz)
        return halo(
            (0, 0, dz), "z", GOT_Z + stage,
            xb.at[run, src, own_rows, :], xb.at[run, dst, own_rows, :],
        )

    def y_face(group, dy):
        run = run_of(*Y_GROUPS[group])
        src, dst = rows_of(dy)
        return halo(
            (0, dy, 0), "y", GOT_Y + group,
            xb.at[run, own_planes, src, :], xb.at[run, own_planes, dst, :],
        )

    def z_edge(dz, dy):
        src, _ = planes_of(dz)
        cut, _ = rows_of(dy)
        place = pl.ds(0 if dz == 1 else 2, 2), pl.ds(0 if dy == 1 else 2, 2)
        return halo(
            (0, 0, dz), "ze", GOT_ZE,
            xb.at[mixed, src, cut, :], eb.at[mixed, place[0], place[1], :],
        )

    def yz_edge(dy, side):
        _, dst = rows_of(dy)
        cut = pl.ds(0, 2) if side == 0 else pl.ds(2 + planes, 2)
        return halo(
            (0, dy, 0), "yz", GOT_YZ,
            eb.at[mixed, pl.ds(2 * side, 2), pl.ds(0 if dy == 1 else 2, 2), :],
            xb.at[mixed, cut, dst, :],
        )

    def xy_edge(slot, dy):
        src, dst = rows_of(dy)
        return halo(
            (0, dy, 0), "xy", GOT_XY,
            tb.at[slot, own_planes, src, :], tb.at[slot, own_planes, dst, :],
        )

    def xz_edge(slot, dz):
        src, dst = planes_of(dz)
        return halo(
            (0, 0, dz), "xz", GOT_XZ,
            tb.at[slot, src, own_rows, :], tb.at[slot, dst, own_rows, :],
        )

    steps, slots = (1, -1), range(len(x_steps))
    z_faces = [[z_face(s, dz) for dz in steps] for s in range(STAGES)]
    y_faces = [[y_face(g, dy) for dy in steps] for g in range(len(Y_GROUPS))]
    z_edges = [z_edge(dz, dy) for dz in steps for dy in steps]
    yz_edges = [yz_edge(dy, side) for dy in steps for side in (0, 1)]
    x_faces = [
        halo((dx, 0, 0), "x", GOT_X, tile.at[0], tb.at[slot, own_planes, own_rows, :])
        for slot, dx in enumerate(x_steps)
    ]
    xy_edges = [xy_edge(slot, dy) for slot in slots for dy in steps]
    xz_edges = [xz_edge(slot, dz) for slot in slots for dz in steps]

    def z_landed(s):
        landed(halo_recv.at[GOT_Z + s], xb.at[run_of(s, s + 1), pl.ds(0, 4), own_rows, :])

    def y_landed(g):
        landed(halo_recv.at[GOT_Y + g], xb.at[run_of(*Y_GROUPS[g]), own_planes, pl.ds(0, 4), :])

    every = pl.ds(0, len(x_steps))

    def x_landed():
        landed(halo_recv.at[GOT_X], tb.at[every, own_planes, own_rows, :])

    def edges_landed():
        landed(halo_recv.at[GOT_YZ], xb.at[mixed, pl.ds(0, 4), pl.ds(0, 4), :])
        landed(halo_recv.at[GOT_XY], tb.at[every, own_planes, pl.ds(0, 4), :])
        landed(halo_recv.at[GOT_XZ], tb.at[every, pl.ds(0, 4), own_rows, :])

    def halos_left():
        left(halo_send.at[SENT["z"]], xb.at[:, pl.ds(0, 4), pl.ds(0, rows + planes), :])
        left(halo_send.at[SENT["yz"]], xb.at[mixed, pl.ds(0, 4), pl.ds(0, 8), :])
        tiles = tb.at[every, pl.ds(0, 4), pl.ds(0, planes * rows // 4 + planes + rows), :]
        left(halo_send.at[SENT["x"]], tiles)

    def start(some):
        for copy in some:
            copy.start()

    loads = []
    place = 0
    for first, size in RUNS:
        loads.append(
            pltpu.make_async_copy(
                section.at[pl.ds(first, size)],
                xb.at[pl.ds(place, size), own_planes, own_rows, :],
                local_sem.at[0],
            )
        )
        place += size
    load_base = pltpu.make_async_copy(base, inputs.at[0], local_sem.at[1])
    load_accum = pltpu.make_async_copy(accum, inputs.at[1], local_sem.at[1])
    chained = gy > 2
    faces = [(0, 0, 1), (0, 0, -1)] + [(dx, 0, 0) for dx in x_steps]
    barrier = pltpu.get_barrier_semaphore()

    def greet(sem, delta):
        pl.semaphore_signal(sem, inc=1, device_id=device(*delta), device_id_type=MESH)

    for delta in faces + [(0, -1, 0)]:
        greet(barrier, delta)
    if chained:
        pl.when(j + 1 < gy)(lambda: greet(barrier, (0, 1, 0)))
    else:
        greet(barrier, (0, 1, 0))
    start(loads)
    load_base.start()
    load_accum.start()

    lane = lax.broadcasted_iota(jnp.int32, (rows, lanes), 1)

    own_cells = xb.at[:, own_planes, own_rows, :]
    pltpu.make_async_copy(own_cells, own_cells, local_sem.at[0]).wait()
    for plane in range(planes):
        packed = jnp.zeros((rows, lanes), jnp.float32)
        for field in range(fields):
            value = xb[PLACE[field], plane + 2, PAD : PAD + rows, :]
            ends = pltpu.roll(value, (4 * field + 2) % lanes, 1)
            packed = jnp.where((lane >> 2) == field, ends, packed)
        tile[0, plane] = packed
    if chained:
        pl.when(j == 0)(lambda: pl.semaphore_wait(barrier, len(faces) + 1))
        pl.when(j > 0)(lambda: pl.semaphore_wait(barrier, len(faces) + 2))
    else:
        pl.semaphore_wait(barrier, len(faces) + 2)
    def far(some):
        pl.when(j == 0)(lambda: start(some))

    def near(some):
        up, down = some[::2], some[1::2]
        start(up)
        pl.when(j > 0)(lambda: start(down))

    if not chained:
        near = start
    else:
        pl.when(j == gy - 2)(lambda: greet(chain, (0, -1, 0)))
    start(z_faces[0])
    near(y_faces[0])
    start(x_faces + z_edges + z_faces[1])
    near(y_faces[1])
    start(z_faces[2])
    near(y_faces[2])
    for s in range(3, EARLY):
        start(z_faces[s])
    if chained:
        @pl.when(j < gy - 2)
        def _():
            pl.semaphore_wait(chain, 1)
            pl.when(j > 0)(lambda: greet(chain, (0, -1, 0)))

        for faces_of in y_faces:
            far(faces_of[1::2])
    pltpu.make_async_copy(inputs, inputs, local_sem.at[1]).wait()

    own_y = pl.ds(pl.multiple_of(j * rows, rows), rows)
    own_x = pl.ds(pl.multiple_of(i * lanes, lanes), lanes)
    paired = gx == 2 and gy % 2 == 0
    turned = TURNED if paired else 0
    kept = STAGES - turned
    pair = j + 1 - 2 * lax.rem(j, 2)
    other = 1 - i
    towards = ((0, 1), (0, -1), (1, 0), (-1, 0))
    TURN, BULK, BULK_TURNED, PAIR_TURNED = ((gy - 1) * STAGES + n for n in range(4))
    SENT_PAIR, SENT_TURNED = 3, 4

    def piece(bi, bj, low, high):
        return slab.at[
            run_of(low, high),
            :,
            pl.ds(pl.multiple_of(bj * rows, rows), rows),
            pl.ds(pl.multiple_of(bi * lanes, lanes), lanes),
        ]

    def line(link, bi, bj, c, sent, got):
        dx, dy = towards[link]
        part = piece(bi, bj, c, c + 1)
        pltpu.make_async_remote_copy(
            src_ref=part,
            dst_ref=part,
            send_sem=line_send.at[sent],
            recv_sem=gather_recv.at[got],
            device_id=device(dx, dy, 0),
            device_id_type=MESH,
        ).start()

    def number(link, bi, bj, c):
        if paired:
            return (bj - link) * STAGES + c
        return (bi * gy + bj) * STAGES + c

    def send(link, bi, bj, c):
        line(link, bi, bj, c, link, number(link, bi, bj, c))

    def arrive(link, bi, bj, c):
        landed(gather_recv.at[number(link, bi, bj, c)], piece(bi, bj, c, c + 1))

    def x_links(body):
        @pl.when(i + 1 < gx)
        def _():
            body(2)

        @pl.when(i > 0)
        def _():
            body(3)

    def cross(bj, c, distance):
        if not paired:
            x_links(lambda link: send(link, i, bj, c))
        elif c < kept:
            if distance == 1:
                line(2, i, bj, c, jnp.where(bj == pair, SENT_PAIR, 2), BULK)
            else:
                line(2, i, bj, c, 2, BULK)
        elif distance == 0:
            line(2, i, bj, c, 2, TURN)
        elif distance == 1:
            pl.when(bj != pair)(lambda: line(2, i, bj, c, 2, BULK_TURNED))
        else:
            line(2, i, bj, c, 2, BULK_TURNED)

    def held(c, ahead):
        if c < kept:
            return False
        return (pair == j + ahead) & ((pair == 0) | (pair == gy - 1))

    def send_own(c):
        @pl.when((j + 1 < gy) & jnp.logical_not(held(c, 1)))
        def _():
            send(0, i, j, c)

        @pl.when((j > 0) & jnp.logical_not(held(c, -1)))
        def _():
            send(1, i, j, c)

        cross(j, c, 0)

    def send_held(c):
        def go(link, ahead):
            pl.when(held(c, ahead))(
                lambda: line(link, i, j, c, link, number(link, i, j, kept))
            )

        go(0, 1)
        go(1, -1)

    def pass_on(d, c, pairs=(False, True)):
        ended = d == 1 and c >= kept

        def below():
            bj = j - d
            arrive(0, i, bj, c)

            @pl.when(j + 1 < gy)
            def _():
                send(0, i, bj, c)

            cross(bj, c, d)

        def above():
            bj = j + d
            arrive(1, i, bj, c)

            @pl.when(j > 0)
            def _():
                send(1, i, bj, c)

            cross(bj, c, d)

        has_below = (j - d >= 0) & (j + 1 < gy) if ended else j - d >= 0
        has_above = (j + d < gy) & (j > 0) if ended else j + d < gy
        if d > 1:
            if True in pairs:
                pl.when(has_below)(below)
                pl.when(has_above)(above)
            return
        for is_pair in pairs:
            pl.when(has_below & ((pair < j) == is_pair))(below)
            pl.when(has_above & ((pair > j) == is_pair))(above)

    def turn():
        landed(gather_recv.at[TURN], piece(other, j, kept, STAGES))
        for c in range(kept, STAGES):
            @pl.when(pair > j)
            def _():
                line(0, other, j, c, SENT_TURNED, PAIR_TURNED)

            @pl.when(pair < j)
            def _():
                line(1, other, j, c, SENT_TURNED, PAIR_TURNED)

    def emit_at(plane):
        def emit(field, rate):
            moved = inputs[0, field, plane] + (0.5 * STEP_DT) * rate
            slab[PLACE[field], plane, own_y, own_x] = moved
            ns_out[field, plane] = moved
            na_out[field, plane] = inputs[1, field, plane] + (STEP_DT / 3.0) * rate

        return emit

    x_landed()
    start(xz_edges + xy_edges)
    for s in range(EARLY, STAGES):
        start(z_faces[s])
    z_landed(0)
    work = [
        rates_of_plane(plane, rows, lanes, xb, tb, emit_at(plane))
        for plane in range(planes)
    ]

    def own_stage(s):
        if s:
            z_landed(s)
        else:
            landed(halo_recv.at[GOT_ZE], eb.at[mixed, pl.ds(0, 4), pl.ds(0, 4), :])
            start(yz_edges)
        if s < len(Y_GROUPS):
            y_landed(s)
        if s == MIX_STAGE:
            edges_landed()
        for part in work:
            next(part)
        send_own(s)

    LAG = tuple(3 * d for d in range(gy))
    final = STAGES - 1 + LAG[gy - 2] + FINAL
    for v in range(STAGES + LAG[gy - 1]):
        if v < STAGES:
            own_stage(v)
        for d in range(1, gy):
            if 0 <= v - LAG[d] < STAGES:
                pass_on(d, v - LAG[d])
        for c in range(kept, STAGES):
            if v == final - (c == kept):
                send_held(c)
        if v == final and turned:
            turn()

    halos_left()

    def whole(n_rows, n_lanes, low=0, high=STAGES):
        return slab.at[run_of(low, high), :, pl.ds(0, n_rows), pl.ds(0, n_lanes)]

    if paired:
        if turned:
            landed(gather_recv.at[PAIR_TURNED], whole(rows, lanes, kept))

            for link, end in ((1, 0), (0, gy - 1)):
                @pl.when(j == end)
                def _():
                    slot = gather_recv.at[number(link, i, pair, kept)]
                    landed(slot, whole(rows, lanes, kept))
        landed(gather_recv.at[BULK], whole(gy * rows, lanes, 0, kept))
        if turned and gy > 2:
            landed(gather_recv.at[BULK_TURNED], whole((gy - 2) * rows, lanes, kept))
    else:
        for d in range(1, gx):
            def row(bj, carry, d=d):
                @pl.when(i - d >= 0)
                def _():
                    for c in range(STAGES):
                        arrive(2, i - d, bj, c)

                        @pl.when(i + 1 < gx)
                        def _():
                            send(2, i - d, bj, c)

                @pl.when(i + d < gx)
                def _():
                    for c in range(STAGES):
                        arrive(3, i + d, bj, c)

                        @pl.when(i > 0)
                        def _():
                            send(3, i + d, bj, c)

                return carry

            lax.fori_loop(0, gy, row, 0)

    for n in range(1, gy):
        @pl.when(j == n - 1)
        def _():
            left(line_send.at[0], whole(n * rows, lanes))

        @pl.when(j == gy - n)
        def _():
            left(line_send.at[1], whole(n * rows, lanes))

    if paired:
        left(line_send.at[2], whole((gy - 1) * rows, lanes))
        left(line_send.at[SENT_PAIR], whole(rows, lanes, 0, kept))
        if turned:
            left(line_send.at[SENT_TURNED], whole(rows, lanes, kept))
    else:
        for n in range(1, gx):
            @pl.when(i == n - 1)
            def _():
                left(line_send.at[2], whole(gy * rows, n * lanes))

            @pl.when(i == gx - n)
            def _():
                left(line_send.at[3], whole(gy * rows, n * lanes))


def put_out(ns_in, na_in, slab_in, ns_out, na_out, slab_out, sem):
    place = 0
    for first, size in RUNS:
        pltpu.make_async_copy(
            slab_in.at[pl.ds(place, size)], slab_out.at[pl.ds(first, size)], sem.at[0]
        ).start()
        place += size
    pltpu.make_async_copy(ns_in, ns_out, sem.at[1]).start()
    pltpu.make_async_copy(na_in, na_out, sem.at[2]).start()
    pltpu.make_async_copy(slab_in, slab_out, sem.at[0]).wait()
    pltpu.make_async_copy(ns_in, ns_out, sem.at[1]).wait()
    pltpu.make_async_copy(na_in, na_out, sem.at[2]).wait()


def shards(sizes, section, base, accum):
    gx, gy, gz = sizes
    fields, planes, rows, lanes = section.shape
    slots = 1 if gx == 2 else 2
    arrivals = (gy - 1) * STAGES + 4 if gx == 2 and gy % 2 == 0 else gx * gy * STAGES
    any_spec = pl.BlockSpec(memory_space=pl.ANY)
    block = jax.ShapeDtypeStruct(section.shape, jnp.float32)
    slab = jax.ShapeDtypeStruct((fields, planes, gy * rows, gx * lanes), jnp.float32)
    dma = pltpu.SemaphoreType.DMA
    staged = pl.pallas_call(
        functools.partial(section_kernel, sizes),
        out_shape=tuple(pltpu.VMEM(a.shape, a.dtype) for a in (block, block, slab)),
        in_specs=[pl.BlockSpec(memory_space=pltpu.HBM)] * 3,
        out_specs=(pl.BlockSpec(memory_space=pltpu.VMEM),) * 3,
        scratch_shapes=[
            pltpu.VMEM((fields, planes + 4, rows + 2 * PAD, lanes), jnp.float32),
            pltpu.VMEM((slots, planes + 4, rows + 2 * PAD, lanes), jnp.float32),
            pltpu.VMEM((MIXED_YZ, 4, 8, lanes), jnp.float32),
            pltpu.VMEM((1, planes, rows, lanes), jnp.float32),
            pltpu.VMEM((2,) + section.shape, jnp.float32),
            dma((2,)),
            dma((3,)),
            dma((STAGES + len(Y_GROUPS) + 5,)),
            dma((5,)),
            dma((arrivals,)),
            pltpu.SemaphoreType.REGULAR,
        ],
        compiler_params=pltpu.CompilerParams(collective_id=0, has_side_effects=True, vmem_limit_bytes=24 << 20),
    )(*(pltpu.with_memory_space_constraint(x, pltpu.HBM) for x in (section, base, accum)))
    return pl.pallas_call(
        put_out,
        out_shape=(block, block, slab),
        in_specs=[pl.BlockSpec(memory_space=pltpu.VMEM)] * 3,
        out_specs=(any_spec,) * 3,
        scratch_shapes=[dma((3,))],
        compiler_params=pltpu.CompilerParams(vmem_limit_bytes=8 << 20),
    )(*staged)


def solution(mesh):
    sizes = tuple(mesh.shape[name] for name in ("gx", "gy", "gz"))
    spec = P(None, "gz", "gy", "gx")
    return jax.shard_map(
        functools.partial(shards, sizes),
        mesh=mesh,
        in_specs=(spec, spec, spec),
        out_specs=(spec, spec, P(None, "gz", None, None)),
        check_vma=False,
    )
```

```python
import functools

import jax
import jax.numpy as jnp
from jax import lax
from jax.experimental import pallas as pl
from jax.experimental.pallas import tpu as pltpu
from jax.sharding import PartitionSpec as P

STEP_DT = 0.25
DISSIPATE = 0.1
DRIVER_ETA = 2.0
KAPPA_ONE = 0.1
PAIR_SLOT = ((0, 1, 2), (1, 3, 4), (2, 4, 5))
PAIR_LIST = ((0, 0), (0, 1), (0, 2), (1, 1), (1, 2), (2, 2))
MESH = pl.DeviceIdType.MESH
RUNS = ((17, 1), (19, 2), (0, 1), (18, 1), (1, 7), (14, 3), (8, 6), (21, 4))
ORDER = tuple(first + n for first, size in RUNS for n in range(size))
PLACE = tuple(ORDER.index(field) for field in range(len(ORDER)))
MIXED = (17, 19, 20, 0, 18)
MIXED_YZ = 4
XZ_LANES = (68, 76, 16)
SIZES = (1, 4, 3, 3, 1, 4, 5, 4)
STAGES = len(SIZES)
FIRST = tuple(sum(SIZES[:s]) for s in range(STAGES + 1))
MIX_STAGE = next(s for s in range(STAGES) if FIRST[s + 1] > PLACE[7])
TURNED = 3
FINAL = 0
Y_GROUPS = ((0, 1), (1, 2), (2, STAGES))
EARLY = 4
PAD = 8


def first_of(m2, m1, p1, p2):
    return (8.0 / 12.0) * (p1 - m1) - (1.0 / 12.0) * (p2 - m2)


def rates_of_plane(plane, rows, lanes, xb, tb, emit):
    lane = lax.broadcasted_iota(jnp.int32, (rows, lanes), 1)
    quad = lane & 3
    edge_one = (lane < 1) | (lane >= lanes - 1)
    edge_two = (lane < 2) | (lane >= lanes - 2)

    def cell(field, dz=0, dy=0):
        return xb[PLACE[field], plane + 2 + dz, PAD + dy : PAD + dy + rows, :]

    def strip(dz=0, dy=0):
        def side(slot):
            return tb[slot, plane + 2 + dz, PAD + dy : PAD + dy + rows, :]

        if tb.shape[0] == 1:
            return side(0)
        return jnp.where(quad < 2, side(0), side(1))

    def facing(edge):
        return jnp.where(
            quad < 2, pltpu.roll(edge, lanes - 2, 1), pltpu.roll(edge, 2, 1)
        )

    def inner(edge):
        return jnp.where(
            quad == 1, pltpu.roll(edge, 1, 1), pltpu.roll(edge, lanes - 1, 1)
        )

    def x_line(field, value, edge, edge_in):
        turn = (lanes - 2 - 4 * field) % lanes
        two = pltpu.roll(edge, turn, 1)
        one = pltpu.roll(edge_in, turn, 1)
        m2 = jnp.where(edge_two & (lane < 64), two, pltpu.roll(value, 2, 1))
        m1 = jnp.where(edge_one & (lane < 64), one, pltpu.roll(value, 1, 1))
        p1 = jnp.where(edge_one & (lane >= 64), one, pltpu.roll(value, lanes - 1, 1))
        p2 = jnp.where(edge_two & (lane >= 64), two, pltpu.roll(value, lanes - 2, 1))
        return m2, m1, p1, p2

    def y_line(read):
        return tuple(read(0, dy) for dy in (-2, -1, 1, 2))

    def z_line(read):
        return tuple(read(dz, 0) for dz in (-2, -1, 1, 2))

    edge = facing(strip())
    edge_in = inner(edge)

    centre, grad, curve, lap, mixed = {}, {}, {}, {}, {}
    need_lap = (0, 1, 2, 3, 4, 5, 6, 17, 18, 19, 20)
    shift = [cell(18), cell(19), cell(20)]
    advected = {}
    for field in range(len(ORDER)):
        centre[field] = cell(field)

    def differentiate(field):
        value = centre[field]
        read = functools.partial(cell, field)
        lines = [x_line(field, value, edge, edge_in), y_line(read), z_line(read)]
        near = [m1 + p1 for _, m1, p1, _ in lines]
        far = [m2 + p2 for m2, _, _, p2 in lines]
        near_sum = near[0] + near[1] + near[2]
        far_sum = far[0] + far[1] + far[2]
        smooth = far_sum - 4.0 * near_sum + 18.0 * value
        grads = [first_of(*line) for line in lines]
        grad[field] = grads
        advected[field] = (
            shift[0] * grads[0] + shift[1] * grads[1] + shift[2] * grads[2]
            - (DISSIPATE / 16.0) * smooth
        )
        if field in need_lap:
            lap[field] = (16.0 / 12.0) * near_sum - (1.0 / 12.0) * far_sum - 7.5 * value
        if field in MIXED:
            for axis in range(3):
                if field in (0, 17) or field == 18 + axis:
                    curve[field, axis] = (
                        (16.0 / 12.0) * near[axis] - (1.0 / 12.0) * far[axis] - 2.5 * value
                    )

    def mix():
        edge_y = facing(first_of(*y_line(strip)))
        edge_y_in = inner(edge_y)
        edge_z = facing(first_of(*z_line(strip)))
        edge_z_in = inner(edge_z)
        for field in MIXED:
            grads = grad[field]
            if field != 20:
                mixed[field, 0, 1] = first_of(*x_line(field, grads[1], edge_y, edge_y_in))
            if field != 19:
                mixed[field, 0, 2] = first_of(*x_line(field, grads[2], edge_z, edge_z_in))
            if field != 18:
                mixed[field, 1, 2] = first_of(
                    *(
                        first_of(*(cell(field, dz, dy) for dy in (-2, -1, 1, 2)))
                        for dz in (-2, -1, 1, 2)
                    )
                )

    def second(field, one, two):
        if one == two:
            return curve[field, one]
        return mixed[field, min(one, two), max(one, two)]

    def sym(table, one, two):
        return table[PAIR_SLOT[one][two]]

    metric = [centre[1 + k] for k in range(6)]
    traceless = [centre[8 + k] for k in range(6)]
    inverse = [
        (2.0 - metric[k]) if one == two else -metric[k]
        for k, (one, two) in enumerate(PAIR_LIST)
    ]

    def contract(left, right):
        diag = left[0] * right[0] + left[3] * right[3] + left[5] * right[5]
        off = left[1] * right[1] + left[2] * right[2] + left[4] * right[4]
        return diag + 2.0 * off

    def lie_of(table, one, two):
        total = None
        for k in range(3):
            if one == two:
                term = 2.0 * (sym(table, one, k) * grad[18 + k][one])
            else:
                term = (
                    sym(table, one, k) * grad[18 + k][two]
                    + sym(table, two, k) * grad[18 + k][one]
                )
            total = term if total is None else total + term
        return total

    chi, trace, lapse, theta = centre[0], centre[7], centre[17], centre[24]
    shared, gauges = {}, {}

    def once(name, make):
        if name not in shared:
            shared[name] = make()
        return shared[name]

    def third_div():
        div = grad[18][0] + grad[19][1] + grad[20][2]
        return (2.0 / 3.0) * div

    def lapse_terms():
        mix()
        lapse_dd = [second(17, one, two) for one, two in PAIR_LIST]
        return lapse_dd, contract(inverse, lapse_dd)

    def ricci_terms():
        half_over = 0.5 * once("over", lambda: 1.0 / chi)
        ricci = []
        for k, (one, two) in enumerate(PAIR_LIST):
            conf = second(0, one, two)
            if one == two:
                conf = conf + lap[0]
                grads_g = grad[14 + one][one]
            else:
                grads_g = 0.5 * (grad[14 + two][one] + grad[14 + one][two])
            ricci.append(-0.5 * lap[1 + k] + grads_g + conf * half_over)
        return ricci, contract(inverse, ricci)

    def rate_of(field):
        rate = advected[field]
        if field == 17:
            return rate - 2.0 * lapse * (trace - 2.0 * theta)
        if field in (18, 19, 20):
            return rate + 0.75 * centre[field + 3]
        third = once("div", third_div)
        if field == 0:
            return rate + (2.0 / 3.0) * chi * (lapse * trace) - chi * third
        if field in range(1, 7):
            k = field - 1
            one, two = PAIR_LIST[k]
            lie = lie_of(metric, one, two)
            return rate - 2.0 * lapse * traceless[k] + lie - metric[k] * third
        lapse_dd, lapse_trace = once("lapse", lapse_terms)
        squares = once("squares", lambda: contract(traceless, traceless))
        if field == 7:
            return (
                rate
                - chi * lapse_trace
                + lapse * (squares + trace * trace * (1.0 / 3.0))
                + KAPPA_ONE * lapse * theta
            )
        if field in (14, 15, 16):
            one = field - 14
            a_lapse = sum(sym(traceless, one, k) * grad[17][k] for k in range(3))
            a_chi = sum(sym(traceless, one, k) * grad[0][k] for k in range(3))
            g_trace = sum(sym(inverse, one, k) * grad[7][k] for k in range(3))
            b_mixed = sum(second(18 + k, one, k) for k in range(3))
            g_shift = sum(centre[14 + k] * grad[18 + one][k] for k in range(3))
            over_chi = once("over", lambda: 1.0 / chi)
            gauges[one] = (
                -2.0 * a_lapse
                - lapse * ((4.0 / 3.0) * g_trace + 3.0 * (a_chi * over_chi))
                + lap[18 + one]
                + b_mixed * (1.0 / 3.0)
                + centre[14 + one] * third
                - g_shift
            )
            return rate + gauges[one]
        if field in (21, 22, 23):
            return rate + gauges[field - 21] - DRIVER_ETA * centre[field]
        ricci, ricci_trace = once("ricci", ricci_terms)
        if field == 24:
            return (
                rate
                + 0.5 * lapse * (chi * ricci_trace + (2.0 / 3.0) * trace * trace - squares)
                - 2.0 * KAPPA_ONE * lapse * theta
            )
        k = field - 8
        one, two = PAIR_LIST[k]
        third_trace = once("trace", lambda: (lapse * ricci_trace - lapse_trace) * (1.0 / 3.0))
        free = lapse * ricci[k] - lapse_dd[k] - metric[k] * third_trace
        product = sum(
            sym(traceless, one, m) * sym(traceless, m, two) for m in range(3)
        )
        return (
            rate
            + chi * free
            + lapse * (trace * traceless[k] - 2.0 * product)
            + lie_of(traceless, one, two)
            - traceless[k] * third
        )

    for stage in range(STAGES):
        for field in ORDER[FIRST[stage] : FIRST[stage + 1]]:
            differentiate(field)
        for field in ORDER[FIRST[stage] : FIRST[stage + 1]]:
            emit(field, rate_of(field))
        yield


def section_kernel(
    sizes, section, base, accum, ns_out, na_out, slab,
    xb, tb, eb, pb, qb, tile, inputs, local_sem, halo_send, halo_recv,
    line_send, gather_recv, chain,
):
    gx, gy, gz = sizes
    fields, planes, rows, lanes = section.shape
    i, j, k = (lax.axis_index(name) for name in ("gx", "gy", "gz"))

    def device(dx=0, dy=0, dz=0):
        return (
            lax.rem(i + dx + gx, gx),
            lax.rem(j + dy + gy, gy),
            lax.rem(k + dz + gz, gz),
        )

    x_steps = (1,) if gx == 2 else (1, -1)

    def landed(sem, ref):
        pltpu.make_async_remote_copy(
            src_ref=ref, dst_ref=ref, send_sem=sem, recv_sem=sem,
            device_id=device(0, 1, 0), device_id_type=MESH,
        ).wait_recv()

    def left(sem, ref):
        pltpu.make_async_remote_copy(
            src_ref=ref, dst_ref=ref, send_sem=sem, recv_sem=sem,
            device_id=device(0, 1, 0), device_id_type=MESH,
        ).wait_send()

    own_planes, own_rows = pl.ds(2, planes), pl.ds(PAD, rows)
    SENT = dict(z=0, y=0, yz=1, ze=1, x=2, xy=2, xz=3)
    GOT_Z, GOT_Y = 0, STAGES
    GOT_YZ = STAGES + len(Y_GROUPS)
    GOT_X, GOT_XY, GOT_XZ, GOT_ZE = (GOT_YZ + n for n in (1, 2, 3, 4))
    mixed = pl.ds(0, MIXED_YZ)

    def halo(delta, kind, got, src, dst):
        return pltpu.make_async_remote_copy(
            src_ref=src, dst_ref=dst,
            send_sem=halo_send.at[SENT[kind]], recv_sem=halo_recv.at[got],
            device_id=device(*delta), device_id_type=MESH,
        )

    def planes_of(dz):
        if dz == 1:
            return pl.ds(planes, 2), pl.ds(0, 2)
        return pl.ds(2, 2), pl.ds(2 + planes, 2)

    def rows_of(dy):
        if dy == 1:
            return pl.ds(PAD + rows - 2, 2), pl.ds(PAD - 2, 2)
        return pl.ds(PAD, 2), pl.ds(PAD + rows, 2)

    def run_of(low, high):
        return pl.ds(FIRST[low], FIRST[high] - FIRST[low])

    def z_face(stage, dz):
        run = run_of(stage, stage + 1)
        src, dst = planes_of(dz)
        return halo(
            (0, 0, dz), "z", GOT_Z + stage,
            xb.at[run, src, own_rows, :], xb.at[run, dst, own_rows, :],
        )

    def y_face(group, dy):
        run = run_of(*Y_GROUPS[group])
        src, dst = rows_of(dy)
        return halo(
            (0, dy, 0), "y", GOT_Y + group,
            xb.at[run, own_planes, src, :], xb.at[run, own_planes, dst, :],
        )

    def z_edge(dz, dy):
        src, _ = planes_of(dz)
        cut, _ = rows_of(dy)
        place = pl.ds(0 if dz == 1 else 2, 2), pl.ds(0 if dy == 1 else 2, 2)
        return halo(
            (0, 0, dz), "ze", GOT_ZE,
            xb.at[mixed, src, cut, :], eb.at[mixed, place[0], place[1], :],
        )

    def yz_edge(dy, side):
        _, dst = rows_of(dy)
        cut = pl.ds(0, 2) if side == 0 else pl.ds(2 + planes, 2)
        return halo(
            (0, dy, 0), "yz", GOT_YZ,
            eb.at[mixed, pl.ds(2 * side, 2), pl.ds(0 if dy == 1 else 2, 2), :],
            xb.at[mixed, cut, dst, :],
        )

    def xy_edge(slot, dy):
        src, dst = rows_of(dy)
        return halo(
            (0, dy, 0), "xy", GOT_XY,
            tb.at[slot, own_planes, src, :], tb.at[slot, own_planes, dst, :],
        )

    tiles8 = rows // 8
    packed_rows = pl.ds(0, tiles8)

    def xz_edge(slot, dz):
        cut = pl.ds(planes - 2 if dz == 1 else 0, 2)
        return halo(
            (0, 0, dz), "xz", GOT_XZ,
            pb.at[slot, cut, packed_rows, :],
            qb.at[slot, pl.ds(0 if dz == 1 else 2, 2), packed_rows, :],
        )

    lane8 = lax.broadcasted_iota(jnp.int32, (8, lanes), 1)
    row8 = lax.broadcasted_iota(jnp.int32, (8, lanes), 0)
    low, spare, width = XZ_LANES

    def pack_edges():
        for slot in slots:
            for plane in range(planes):
                for t in range(tiles8):
                    value = tb[slot, 2 + plane, PAD + 8 * t : PAD + 8 * t + 8, :]
                    first = (lane8 >= spare) & (lane8 < spare + 4)
                    value = jnp.where(first, pltpu.roll(value, spare, 1), value)
                    inside = (lane8 >= low) & (lane8 < low + width)
                    value = jnp.where(inside, value, 0.0)
                    value = pltpu.roll(value, 0, 1, stride=width, stride_axis=0)
                    pb[slot, plane, t : t + 1, :] = jnp.sum(value, axis=0, keepdims=True)

    def unpack_edges():
        for slot in slots:
            for n, plane in enumerate((0, 1, 2 + planes, 3 + planes)):
                for t in range(tiles8):
                    packed = jnp.broadcast_to(qb[slot, n, t : t + 1, :], (8, lanes))
                    value = packed
                    for row in range(1, 8):
                        here = pltpu.roll(packed, lanes - width * row, 1)
                        value = jnp.where(row8 == row, here, value)
                    first = pltpu.roll(value, lanes - spare, 1)
                    value = jnp.where(lane8 < 4, first, value)
                    tb[slot, plane, PAD + 8 * t : PAD + 8 * t + 8, :] = value

    steps, slots = (1, -1), range(len(x_steps))
    z_faces = [[z_face(s, dz) for dz in steps] for s in range(STAGES)]
    y_faces = [[y_face(g, dy) for dy in steps] for g in range(len(Y_GROUPS))]
    z_edges = [z_edge(dz, dy) for dz in steps for dy in steps]
    yz_edges = [yz_edge(dy, side) for dy in steps for side in (0, 1)]
    x_faces = [
        halo((dx, 0, 0), "x", GOT_X, tile.at[0], tb.at[slot, own_planes, own_rows, :])
        for slot, dx in enumerate(x_steps)
    ]
    xy_edges = [xy_edge(slot, dy) for slot in slots for dy in steps]
    xz_edges = [xz_edge(slot, dz) for slot in slots for dz in steps]

    def z_landed(s):
        landed(halo_recv.at[GOT_Z + s], xb.at[run_of(s, s + 1), pl.ds(0, 4), own_rows, :])

    def y_landed(g):
        landed(halo_recv.at[GOT_Y + g], xb.at[run_of(*Y_GROUPS[g]), own_planes, pl.ds(0, 4), :])

    every = pl.ds(0, len(x_steps))

    def x_landed():
        landed(halo_recv.at[GOT_X], tb.at[every, own_planes, own_rows, :])

    def edges_landed():
        landed(halo_recv.at[GOT_YZ], xb.at[mixed, pl.ds(0, 4), pl.ds(0, 4), :])
        landed(halo_recv.at[GOT_XY], tb.at[every, own_planes, pl.ds(0, 4), :])

    def halos_left():
        left(halo_send.at[SENT["z"]], xb.at[:, pl.ds(0, 4), pl.ds(0, rows + planes), :])
        left(halo_send.at[SENT["yz"]], xb.at[mixed, pl.ds(0, 4), pl.ds(0, 8), :])
        left(halo_send.at[SENT["x"]], tb.at[every, pl.ds(0, planes), pl.ds(0, rows + 4), :])
        left(halo_send.at[SENT["xz"]], qb.at[every, pl.ds(0, 4), packed_rows, :])

    def start(some):
        for copy in some:
            copy.start()

    loads = []
    place = 0
    for first, size in RUNS:
        loads.append(
            pltpu.make_async_copy(
                section.at[pl.ds(first, size)],
                xb.at[pl.ds(place, size), own_planes, own_rows, :],
                local_sem.at[0],
            )
        )
        place += size
    load_base = pltpu.make_async_copy(base, inputs.at[0], local_sem.at[1])
    load_accum = pltpu.make_async_copy(accum, inputs.at[1], local_sem.at[1])
    chained = gy > 2
    faces = [(0, 0, 1), (0, 0, -1)] + [(dx, 0, 0) for dx in x_steps]
    barrier = pltpu.get_barrier_semaphore()

    def greet(sem, delta):
        pl.semaphore_signal(sem, inc=1, device_id=device(*delta), device_id_type=MESH)

    for delta in faces + [(0, -1, 0)]:
        greet(barrier, delta)
    if chained:
        pl.when(j + 1 < gy)(lambda: greet(barrier, (0, 1, 0)))
    else:
        greet(barrier, (0, 1, 0))
    start(loads)
    load_base.start()
    load_accum.start()

    lane = lax.broadcasted_iota(jnp.int32, (rows, lanes), 1)

    own_cells = xb.at[:, own_planes, own_rows, :]
    pltpu.make_async_copy(own_cells, own_cells, local_sem.at[0]).wait()
    for plane in range(planes):
        packed = jnp.zeros((rows, lanes), jnp.float32)
        for field in range(fields):
            value = xb[PLACE[field], plane + 2, PAD : PAD + rows, :]
            ends = pltpu.roll(value, (4 * field + 2) % lanes, 1)
            packed = jnp.where((lane >> 2) == field, ends, packed)
        tile[0, plane] = packed
    if chained:
        pl.when(j == 0)(lambda: pl.semaphore_wait(barrier, len(faces) + 1))
        pl.when(j > 0)(lambda: pl.semaphore_wait(barrier, len(faces) + 2))
    else:
        pl.semaphore_wait(barrier, len(faces) + 2)
    def far(some):
        pl.when(j == 0)(lambda: start(some))

    def near(some):
        up, down = some[::2], some[1::2]
        start(up)
        pl.when(j > 0)(lambda: start(down))

    if not chained:
        near = start
    else:
        pl.when(j == gy - 2)(lambda: greet(chain, (0, -1, 0)))
    start(z_faces[0])
    near(y_faces[0])
    start(x_faces + z_edges + z_faces[1])
    near(y_faces[1])
    start(z_faces[2])
    near(y_faces[2])
    for s in range(3, EARLY):
        start(z_faces[s])
    if chained:
        @pl.when(j < gy - 2)
        def _():
            pl.semaphore_wait(chain, 1)
            pl.when(j > 0)(lambda: greet(chain, (0, -1, 0)))

        for faces_of in y_faces:
            far(faces_of[1::2])
    pltpu.make_async_copy(inputs, inputs, local_sem.at[1]).wait()

    own_y = pl.ds(pl.multiple_of(j * rows, rows), rows)
    own_x = pl.ds(pl.multiple_of(i * lanes, lanes), lanes)
    paired = gx == 2 and gy % 2 == 0
    turned = TURNED if paired else 0
    kept = STAGES - turned
    pair = j + 1 - 2 * lax.rem(j, 2)
    other = 1 - i
    towards = ((0, 1), (0, -1), (1, 0), (-1, 0))
    TURN, BULK, BULK_TURNED, PAIR_TURNED = ((gy - 1) * STAGES + n for n in range(4))
    SENT_PAIR, SENT_TURNED = 3, 4

    def piece(bi, bj, low, high):
        return slab.at[
            run_of(low, high),
            :,
            pl.ds(pl.multiple_of(bj * rows, rows), rows),
            pl.ds(pl.multiple_of(bi * lanes, lanes), lanes),
        ]

    def line(link, bi, bj, c, sent, got):
        dx, dy = towards[link]
        part = piece(bi, bj, c, c + 1)
        pltpu.make_async_remote_copy(
            src_ref=part,
            dst_ref=part,
            send_sem=line_send.at[sent],
            recv_sem=gather_recv.at[got],
            device_id=device(dx, dy, 0),
            device_id_type=MESH,
        ).start()

    def number(link, bi, bj, c):
        if paired:
            return (bj - link) * STAGES + c
        return (bi * gy + bj) * STAGES + c

    def send(link, bi, bj, c):
        line(link, bi, bj, c, link, number(link, bi, bj, c))

    def arrive(link, bi, bj, c):
        landed(gather_recv.at[number(link, bi, bj, c)], piece(bi, bj, c, c + 1))

    def x_links(body):
        @pl.when(i + 1 < gx)
        def _():
            body(2)

        @pl.when(i > 0)
        def _():
            body(3)

    def cross(bj, c, distance):
        if not paired:
            x_links(lambda link: send(link, i, bj, c))
        elif c < kept:
            if distance == 1:
                line(2, i, bj, c, jnp.where(bj == pair, SENT_PAIR, 2), BULK)
            else:
                line(2, i, bj, c, 2, BULK)
        elif distance == 0:
            line(2, i, bj, c, 2, TURN)
        elif distance == 1:
            pl.when(bj != pair)(lambda: line(2, i, bj, c, 2, BULK_TURNED))
        else:
            line(2, i, bj, c, 2, BULK_TURNED)

    def held(c, ahead):
        if c < kept:
            return False
        return (pair == j + ahead) & ((pair == 0) | (pair == gy - 1))

    def send_own(c):
        @pl.when((j + 1 < gy) & jnp.logical_not(held(c, 1)))
        def _():
            send(0, i, j, c)

        @pl.when((j > 0) & jnp.logical_not(held(c, -1)))
        def _():
            send(1, i, j, c)

        cross(j, c, 0)

    def send_held(c):
        def go(link, ahead):
            pl.when(held(c, ahead))(
                lambda: line(link, i, j, c, link, number(link, i, j, kept))
            )

        go(0, 1)
        go(1, -1)

    def pass_on(d, c, pairs=(False, True)):
        ended = d == 1 and c >= kept

        def below():
            bj = j - d
            arrive(0, i, bj, c)

            @pl.when(j + 1 < gy)
            def _():
                send(0, i, bj, c)

            cross(bj, c, d)

        def above():
            bj = j + d
            arrive(1, i, bj, c)

            @pl.when(j > 0)
            def _():
                send(1, i, bj, c)

            cross(bj, c, d)

        has_below = (j - d >= 0) & (j + 1 < gy) if ended else j - d >= 0
        has_above = (j + d < gy) & (j > 0) if ended else j + d < gy
        if d > 1:
            if True in pairs:
                pl.when(has_below)(below)
                pl.when(has_above)(above)
            return
        for is_pair in pairs:
            pl.when(has_below & ((pair < j) == is_pair))(below)
            pl.when(has_above & ((pair > j) == is_pair))(above)

    def turn():
        landed(gather_recv.at[TURN], piece(other, j, kept, STAGES))
        for c in range(kept, STAGES):
            @pl.when(pair > j)
            def _():
                line(0, other, j, c, SENT_TURNED, PAIR_TURNED)

            @pl.when(pair < j)
            def _():
                line(1, other, j, c, SENT_TURNED, PAIR_TURNED)

    def emit_at(plane):
        def emit(field, rate):
            moved = inputs[0, field, plane] + (0.5 * STEP_DT) * rate
            slab[PLACE[field], plane, own_y, own_x] = moved
            ns_out[field, plane] = moved
            na_out[field, plane] = inputs[1, field, plane] + (STEP_DT / 3.0) * rate

        return emit

    x_landed()
    start(xy_edges)
    pack_edges()
    start(xz_edges)
    for s in range(EARLY, STAGES):
        start(z_faces[s])
    z_landed(0)
    work = [
        rates_of_plane(plane, rows, lanes, xb, tb, emit_at(plane))
        for plane in range(planes)
    ]

    def own_stage(s):
        if s:
            z_landed(s)
        else:
            landed(halo_recv.at[GOT_ZE], eb.at[mixed, pl.ds(0, 4), pl.ds(0, 4), :])
            start(yz_edges)
        if s < len(Y_GROUPS):
            y_landed(s)
        if s == MIX_STAGE:
            edges_landed()
        for part in work:
            next(part)
        send_own(s)
        if s == MIX_STAGE - 1:
            landed(halo_recv.at[GOT_XZ], qb.at[every, pl.ds(0, 4), packed_rows, :])
            unpack_edges()

    LAG = tuple(3 * d for d in range(gy))
    final = STAGES - 1 + LAG[gy - 2] + FINAL
    for v in range(STAGES + LAG[gy - 1]):
        if v < STAGES:
            own_stage(v)
        for d in range(1, gy):
            if 0 <= v - LAG[d] < STAGES:
                pass_on(d, v - LAG[d])
        for c in range(kept, STAGES):
            if v == final - (c == kept):
                send_held(c)
        if v == final and turned:
            turn()

    halos_left()

    def whole(n_rows, n_lanes, low=0, high=STAGES):
        return slab.at[run_of(low, high), :, pl.ds(0, n_rows), pl.ds(0, n_lanes)]

    if paired:
        if turned:
            landed(gather_recv.at[PAIR_TURNED], whole(rows, lanes, kept))

            for link, end in ((1, 0), (0, gy - 1)):
                @pl.when(j == end)
                def _():
                    slot = gather_recv.at[number(link, i, pair, kept)]
                    landed(slot, whole(rows, lanes, kept))
        landed(gather_recv.at[BULK], whole(gy * rows, lanes, 0, kept))
        if turned and gy > 2:
            landed(gather_recv.at[BULK_TURNED], whole((gy - 2) * rows, lanes, kept))
    else:
        for d in range(1, gx):
            def row(bj, carry, d=d):
                @pl.when(i - d >= 0)
                def _():
                    for c in range(STAGES):
                        arrive(2, i - d, bj, c)

                        @pl.when(i + 1 < gx)
                        def _():
                            send(2, i - d, bj, c)

                @pl.when(i + d < gx)
                def _():
                    for c in range(STAGES):
                        arrive(3, i + d, bj, c)

                        @pl.when(i > 0)
                        def _():
                            send(3, i + d, bj, c)

                return carry

            lax.fori_loop(0, gy, row, 0)

    for n in range(1, gy):
        @pl.when(j == n - 1)
        def _():
            left(line_send.at[0], whole(n * rows, lanes))

        @pl.when(j == gy - n)
        def _():
            left(line_send.at[1], whole(n * rows, lanes))

    if paired:
        left(line_send.at[2], whole((gy - 1) * rows, lanes))
        left(line_send.at[SENT_PAIR], whole(rows, lanes, 0, kept))
        if turned:
            left(line_send.at[SENT_TURNED], whole(rows, lanes, kept))
    else:
        for n in range(1, gx):
            @pl.when(i == n - 1)
            def _():
                left(line_send.at[2], whole(gy * rows, n * lanes))

            @pl.when(i == gx - n)
            def _():
                left(line_send.at[3], whole(gy * rows, n * lanes))


def put_out(ns_in, na_in, slab_in, ns_out, na_out, slab_out, sem):
    place = 0
    for first, size in RUNS:
        pltpu.make_async_copy(
            slab_in.at[pl.ds(place, size)], slab_out.at[pl.ds(first, size)], sem.at[0]
        ).start()
        place += size
    pltpu.make_async_copy(ns_in, ns_out, sem.at[1]).start()
    pltpu.make_async_copy(na_in, na_out, sem.at[2]).start()
    pltpu.make_async_copy(slab_in, slab_out, sem.at[0]).wait()
    pltpu.make_async_copy(ns_in, ns_out, sem.at[1]).wait()
    pltpu.make_async_copy(na_in, na_out, sem.at[2]).wait()


def shards(sizes, section, base, accum):
    gx, gy, gz = sizes
    fields, planes, rows, lanes = section.shape
    slots = 1 if gx == 2 else 2
    arrivals = (gy - 1) * STAGES + 4 if gx == 2 and gy % 2 == 0 else gx * gy * STAGES
    any_spec = pl.BlockSpec(memory_space=pl.ANY)
    block = jax.ShapeDtypeStruct(section.shape, jnp.float32)
    slab = jax.ShapeDtypeStruct((fields, planes, gy * rows, gx * lanes), jnp.float32)
    dma = pltpu.SemaphoreType.DMA
    staged = pl.pallas_call(
        functools.partial(section_kernel, sizes),
        out_shape=tuple(pltpu.VMEM(a.shape, a.dtype) for a in (block, block, slab)),
        in_specs=[pl.BlockSpec(memory_space=pltpu.HBM)] * 3,
        out_specs=(pl.BlockSpec(memory_space=pltpu.VMEM),) * 3,
        scratch_shapes=[
            pltpu.VMEM((fields, planes + 4, rows + 2 * PAD, lanes), jnp.float32),
            pltpu.VMEM((slots, planes + 4, rows + 2 * PAD, lanes), jnp.float32),
            pltpu.VMEM((MIXED_YZ, 4, 8, lanes), jnp.float32),
            pltpu.VMEM((slots, planes, 8, lanes), jnp.float32),
            pltpu.VMEM((slots, 4, 8, lanes), jnp.float32),
            pltpu.VMEM((1, planes, rows, lanes), jnp.float32),
            pltpu.VMEM((2,) + section.shape, jnp.float32),
            dma((2,)),
            dma((4,)),
            dma((STAGES + len(Y_GROUPS) + 5,)),
            dma((5,)),
            dma((arrivals,)),
            pltpu.SemaphoreType.REGULAR,
        ],
        compiler_params=pltpu.CompilerParams(collective_id=0, has_side_effects=True, vmem_limit_bytes=24 << 20),
    )(*(pltpu.with_memory_space_constraint(x, pltpu.HBM) for x in (section, base, accum)))
    return pl.pallas_call(
        put_out,
        out_shape=(block, block, slab),
        in_specs=[pl.BlockSpec(memory_space=pltpu.VMEM)] * 3,
        out_specs=(any_spec,) * 3,
        scratch_shapes=[dma((3,))],
        compiler_params=pltpu.CompilerParams(vmem_limit_bytes=8 << 20),
    )(*staged)


def solution(mesh):
    sizes = tuple(mesh.shape[name] for name in ("gx", "gy", "gz"))
    spec = P(None, "gz", "gy", "gx")
    return jax.shard_map(
        functools.partial(shards, sizes),
        mesh=mesh,
        in_specs=(spec, spec, spec),
        out_specs=(spec, spec, P(None, "gz", None, None)),
        check_vma=False,
    )
```

```python
import functools

import jax
import jax.numpy as jnp
from jax import lax
from jax.experimental import pallas as pl
from jax.experimental.pallas import tpu as pltpu
from jax.sharding import PartitionSpec as P

STEP_DT = 0.25
DISSIPATE = 0.1
DRIVER_ETA = 2.0
KAPPA_ONE = 0.1
PAIR_SLOT = ((0, 1, 2), (1, 3, 4), (2, 4, 5))
PAIR_LIST = ((0, 0), (0, 1), (0, 2), (1, 1), (1, 2), (2, 2))
MESH = pl.DeviceIdType.MESH
RUNS = ((17, 1), (19, 2), (0, 1), (18, 1), (1, 7), (14, 3), (8, 6), (21, 4))
ORDER = tuple(first + n for first, size in RUNS for n in range(size))
PLACE = tuple(ORDER.index(field) for field in range(len(ORDER)))
MIXED = (17, 19, 20, 0, 18)
MIXED_YZ = 4
XZ_LANES = (68, 76, 16)
SIZES = (1, 4, 3, 3, 1, 4, 5, 4)
STAGES = len(SIZES)
FIRST = tuple(sum(SIZES[:s]) for s in range(STAGES + 1))
MIX_STAGE = next(s for s in range(STAGES) if FIRST[s + 1] > PLACE[7])
TURNED = 3
FINAL = 0
Y_GROUPS = ((0, 1), (1, 2), (2, STAGES))
EARLY = 4
PAD = 8


def first_of(m2, m1, p1, p2):
    return (8.0 / 12.0) * (p1 - m1) - (1.0 / 12.0) * (p2 - m2)


def rates_of_plane(plane, rows, lanes, xb, tb, emit):
    lane = lax.broadcasted_iota(jnp.int32, (rows, lanes), 1)
    quad = lane & 3
    edge_one = (lane < 1) | (lane >= lanes - 1)
    edge_two = (lane < 2) | (lane >= lanes - 2)

    def cell(field, dz=0, dy=0):
        return xb[PLACE[field], plane + 2 + dz, PAD + dy : PAD + dy + rows, :]

    def strip(dz=0, dy=0):
        def side(slot):
            return tb[slot, plane + 2 + dz, PAD + dy : PAD + dy + rows, :]

        if tb.shape[0] == 1:
            return side(0)
        return jnp.where(quad < 2, side(0), side(1))

    def facing(edge):
        return jnp.where(
            quad < 2, pltpu.roll(edge, lanes - 2, 1), pltpu.roll(edge, 2, 1)
        )

    def inner(edge):
        return jnp.where(
            quad == 1, pltpu.roll(edge, 1, 1), pltpu.roll(edge, lanes - 1, 1)
        )

    def x_line(field, value, edge, edge_in):
        turn = (lanes - 2 - 4 * field) % lanes
        two = pltpu.roll(edge, turn, 1)
        one = pltpu.roll(edge_in, turn, 1)
        m2 = jnp.where(edge_two & (lane < 64), two, pltpu.roll(value, 2, 1))
        m1 = jnp.where(edge_one & (lane < 64), one, pltpu.roll(value, 1, 1))
        p1 = jnp.where(edge_one & (lane >= 64), one, pltpu.roll(value, lanes - 1, 1))
        p2 = jnp.where(edge_two & (lane >= 64), two, pltpu.roll(value, lanes - 2, 1))
        return m2, m1, p1, p2

    def y_line(read):
        return tuple(read(0, dy) for dy in (-2, -1, 1, 2))

    def z_line(read):
        return tuple(read(dz, 0) for dz in (-2, -1, 1, 2))

    edge = facing(strip())
    edge_in = inner(edge)

    centre, grad, curve, lap, mixed = {}, {}, {}, {}, {}
    need_lap = (0, 1, 2, 3, 4, 5, 6, 17, 18, 19, 20)
    shift = [cell(18), cell(19), cell(20)]
    advected = {}
    for field in range(len(ORDER)):
        centre[field] = cell(field)

    def differentiate(field):
        value = centre[field]
        read = functools.partial(cell, field)
        lines = [x_line(field, value, edge, edge_in), y_line(read), z_line(read)]
        near = [m1 + p1 for _, m1, p1, _ in lines]
        far = [m2 + p2 for m2, _, _, p2 in lines]
        near_sum = near[0] + near[1] + near[2]
        far_sum = far[0] + far[1] + far[2]
        smooth = far_sum - 4.0 * near_sum + 18.0 * value
        grads = [first_of(*line) for line in lines]
        grad[field] = grads
        advected[field] = (
            shift[0] * grads[0] + shift[1] * grads[1] + shift[2] * grads[2]
            - (DISSIPATE / 16.0) * smooth
        )
        if field in need_lap:
            lap[field] = (16.0 / 12.0) * near_sum - (1.0 / 12.0) * far_sum - 7.5 * value
        if field in MIXED:
            for axis in range(3):
                if field in (0, 17) or field == 18 + axis:
                    curve[field, axis] = (
                        (16.0 / 12.0) * near[axis] - (1.0 / 12.0) * far[axis] - 2.5 * value
                    )

    def mix():
        edge_y = facing(first_of(*y_line(strip)))
        edge_y_in = inner(edge_y)
        edge_z = facing(first_of(*z_line(strip)))
        edge_z_in = inner(edge_z)
        for field in MIXED:
            grads = grad[field]
            if field != 20:
                mixed[field, 0, 1] = first_of(*x_line(field, grads[1], edge_y, edge_y_in))
            if field != 19:
                mixed[field, 0, 2] = first_of(*x_line(field, grads[2], edge_z, edge_z_in))
            if field != 18:
                mixed[field, 1, 2] = first_of(
                    *(
                        first_of(*(cell(field, dz, dy) for dy in (-2, -1, 1, 2)))
                        for dz in (-2, -1, 1, 2)
                    )
                )

    def second(field, one, two):
        if one == two:
            return curve[field, one]
        return mixed[field, min(one, two), max(one, two)]

    def sym(table, one, two):
        return table[PAIR_SLOT[one][two]]

    metric = [centre[1 + k] for k in range(6)]
    traceless = [centre[8 + k] for k in range(6)]
    inverse = [
        (2.0 - metric[k]) if one == two else -metric[k]
        for k, (one, two) in enumerate(PAIR_LIST)
    ]

    def contract(left, right):
        diag = left[0] * right[0] + left[3] * right[3] + left[5] * right[5]
        off = left[1] * right[1] + left[2] * right[2] + left[4] * right[4]
        return diag + 2.0 * off

    def lie_of(table, one, two):
        total = None
        for k in range(3):
            if one == two:
                term = 2.0 * (sym(table, one, k) * grad[18 + k][one])
            else:
                term = (
                    sym(table, one, k) * grad[18 + k][two]
                    + sym(table, two, k) * grad[18 + k][one]
                )
            total = term if total is None else total + term
        return total

    chi, trace, lapse, theta = centre[0], centre[7], centre[17], centre[24]
    shared, gauges = {}, {}

    def once(name, make):
        if name not in shared:
            shared[name] = make()
        return shared[name]

    def third_div():
        div = grad[18][0] + grad[19][1] + grad[20][2]
        return (2.0 / 3.0) * div

    def lapse_terms():
        mix()
        lapse_dd = [second(17, one, two) for one, two in PAIR_LIST]
        return lapse_dd, contract(inverse, lapse_dd)

    def ricci_terms():
        half_over = 0.5 * once("over", lambda: 1.0 / chi)
        ricci = []
        for k, (one, two) in enumerate(PAIR_LIST):
            conf = second(0, one, two)
            if one == two:
                conf = conf + lap[0]
                grads_g = grad[14 + one][one]
            else:
                grads_g = 0.5 * (grad[14 + two][one] + grad[14 + one][two])
            ricci.append(-0.5 * lap[1 + k] + grads_g + conf * half_over)
        return ricci, contract(inverse, ricci)

    def rate_of(field):
        rate = advected[field]
        if field == 17:
            return rate - 2.0 * lapse * (trace - 2.0 * theta)
        if field in (18, 19, 20):
            return rate + 0.75 * centre[field + 3]
        third = once("div", third_div)
        if field == 0:
            return rate + (2.0 / 3.0) * chi * (lapse * trace) - chi * third
        if field in range(1, 7):
            k = field - 1
            one, two = PAIR_LIST[k]
            lie = lie_of(metric, one, two)
            return rate - 2.0 * lapse * traceless[k] + lie - metric[k] * third
        lapse_dd, lapse_trace = once("lapse", lapse_terms)
        squares = once("squares", lambda: contract(traceless, traceless))
        if field == 7:
            return (
                rate
                - chi * lapse_trace
                + lapse * (squares + trace * trace * (1.0 / 3.0))
                + KAPPA_ONE * lapse * theta
            )
        if field in (14, 15, 16):
            one = field - 14
            a_lapse = sum(sym(traceless, one, k) * grad[17][k] for k in range(3))
            a_chi = sum(sym(traceless, one, k) * grad[0][k] for k in range(3))
            g_trace = sum(sym(inverse, one, k) * grad[7][k] for k in range(3))
            b_mixed = sum(second(18 + k, one, k) for k in range(3))
            g_shift = sum(centre[14 + k] * grad[18 + one][k] for k in range(3))
            over_chi = once("over", lambda: 1.0 / chi)
            gauges[one] = (
                -2.0 * a_lapse
                - lapse * ((4.0 / 3.0) * g_trace + 3.0 * (a_chi * over_chi))
                + lap[18 + one]
                + b_mixed * (1.0 / 3.0)
                + centre[14 + one] * third
                - g_shift
            )
            return rate + gauges[one]
        if field in (21, 22, 23):
            return rate + gauges[field - 21] - DRIVER_ETA * centre[field]
        ricci, ricci_trace = once("ricci", ricci_terms)
        if field == 24:
            return (
                rate
                + 0.5 * lapse * (chi * ricci_trace + (2.0 / 3.0) * trace * trace - squares)
                - 2.0 * KAPPA_ONE * lapse * theta
            )
        k = field - 8
        one, two = PAIR_LIST[k]
        third_trace = once("trace", lambda: (lapse * ricci_trace - lapse_trace) * (1.0 / 3.0))
        free = lapse * ricci[k] - lapse_dd[k] - metric[k] * third_trace
        product = sum(
            sym(traceless, one, m) * sym(traceless, m, two) for m in range(3)
        )
        return (
            rate
            + chi * free
            + lapse * (trace * traceless[k] - 2.0 * product)
            + lie_of(traceless, one, two)
            - traceless[k] * third
        )

    for stage in range(STAGES):
        for field in ORDER[FIRST[stage] : FIRST[stage + 1]]:
            differentiate(field)
        for field in ORDER[FIRST[stage] : FIRST[stage + 1]]:
            emit(field, rate_of(field))
        yield


def section_kernel(
    sizes, section, base, accum, ns_out, na_out, slab,
    xb, tb, eb, pb, qb, tile, inputs, local_sem, halo_send, halo_recv,
    line_send, gather_recv, chain,
):
    gx, gy, gz = sizes
    fields, planes, rows, lanes = section.shape
    i, j, k = (lax.axis_index(name) for name in ("gx", "gy", "gz"))

    def device(dx=0, dy=0, dz=0):
        return (
            lax.rem(i + dx + gx, gx),
            lax.rem(j + dy + gy, gy),
            lax.rem(k + dz + gz, gz),
        )

    x_steps = (1,) if gx == 2 else (1, -1)

    def landed(sem, ref):
        pltpu.make_async_remote_copy(
            src_ref=ref, dst_ref=ref, send_sem=sem, recv_sem=sem,
            device_id=device(0, 1, 0), device_id_type=MESH,
        ).wait_recv()

    def left(sem, ref):
        pltpu.make_async_remote_copy(
            src_ref=ref, dst_ref=ref, send_sem=sem, recv_sem=sem,
            device_id=device(0, 1, 0), device_id_type=MESH,
        ).wait_send()

    own_planes, own_rows = pl.ds(2, planes), pl.ds(PAD, rows)
    SENT = dict(z=0, y=0, yz=1, ze=1, x=2, xy=2, xz=3)
    GOT_Z, GOT_Y = 0, STAGES
    GOT_YZ = STAGES + len(Y_GROUPS)
    GOT_X, GOT_XY, GOT_XZ, GOT_ZE = (GOT_YZ + n for n in (1, 2, 3, 4))
    mixed = pl.ds(0, MIXED_YZ)

    def halo(delta, kind, got, src, dst):
        return pltpu.make_async_remote_copy(
            src_ref=src, dst_ref=dst,
            send_sem=halo_send.at[SENT[kind]], recv_sem=halo_recv.at[got],
            device_id=device(*delta), device_id_type=MESH,
        )

    def planes_of(dz):
        if dz == 1:
            return pl.ds(planes, 2), pl.ds(0, 2)
        return pl.ds(2, 2), pl.ds(2 + planes, 2)

    def rows_of(dy):
        if dy == 1:
            return pl.ds(PAD + rows - 2, 2), pl.ds(PAD - 2, 2)
        return pl.ds(PAD, 2), pl.ds(PAD + rows, 2)

    def run_of(low, high):
        return pl.ds(FIRST[low], FIRST[high] - FIRST[low])

    def z_face(stage, dz):
        run = run_of(stage, stage + 1)
        src, dst = planes_of(dz)
        return halo(
            (0, 0, dz), "z", GOT_Z + stage,
            xb.at[run, src, own_rows, :], xb.at[run, dst, own_rows, :],
        )

    def y_face(group, dy):
        run = run_of(*Y_GROUPS[group])
        src, dst = rows_of(dy)
        return halo(
            (0, dy, 0), "y", GOT_Y + group,
            xb.at[run, own_planes, src, :], xb.at[run, own_planes, dst, :],
        )

    def z_edge(dz, dy):
        src, _ = planes_of(dz)
        cut, _ = rows_of(dy)
        place = pl.ds(0 if dz == 1 else 2, 2), pl.ds(0 if dy == 1 else 2, 2)
        return halo(
            (0, 0, dz), "ze", GOT_ZE,
            xb.at[mixed, src, cut, :], eb.at[mixed, place[0], place[1], :],
        )

    def yz_edge(dy, side):
        _, dst = rows_of(dy)
        cut = pl.ds(0, 2) if side == 0 else pl.ds(2 + planes, 2)
        return halo(
            (0, dy, 0), "yz", GOT_YZ,
            eb.at[mixed, pl.ds(2 * side, 2), pl.ds(0 if dy == 1 else 2, 2), :],
            xb.at[mixed, cut, dst, :],
        )

    def xy_edge(slot, dy):
        src, dst = rows_of(dy)
        return halo(
            (0, dy, 0), "xy", GOT_XY,
            tb.at[slot, own_planes, src, :], tb.at[slot, own_planes, dst, :],
        )

    tiles8 = rows // 8
    packed_rows = pl.ds(0, tiles8)

    def xz_edge(slot, dz):
        cut = pl.ds(planes - 2 if dz == 1 else 0, 2)
        return halo(
            (0, 0, dz), "xz", GOT_XZ,
            pb.at[slot, cut, packed_rows, :],
            qb.at[slot, pl.ds(0 if dz == 1 else 2, 2), packed_rows, :],
        )

    lane8 = lax.broadcasted_iota(jnp.int32, (8, lanes), 1)
    row8 = lax.broadcasted_iota(jnp.int32, (8, lanes), 0)
    low, spare, width = XZ_LANES

    def pack_edges():
        for slot in slots:
            for plane in range(planes):
                for t in range(tiles8):
                    value = tb[slot, 2 + plane, PAD + 8 * t : PAD + 8 * t + 8, :]
                    first = (lane8 >= spare) & (lane8 < spare + 4)
                    value = jnp.where(first, pltpu.roll(value, spare, 1), value)
                    inside = (lane8 >= low) & (lane8 < low + width)
                    value = jnp.where(inside, value, 0.0)
                    value = pltpu.roll(value, 0, 1, stride=width, stride_axis=0)
                    pb[slot, plane, t : t + 1, :] = jnp.sum(value, axis=0, keepdims=True)

    def unpack_edges():
        for slot in slots:
            for n, plane in enumerate((0, 1, 2 + planes, 3 + planes)):
                for t in range(tiles8):
                    packed = jnp.broadcast_to(qb[slot, n, t : t + 1, :], (8, lanes))
                    value = packed
                    for row in range(1, 8):
                        here = pltpu.roll(packed, lanes - width * row, 1)
                        value = jnp.where(row8 == row, here, value)
                    first = pltpu.roll(value, lanes - spare, 1)
                    value = jnp.where(lane8 < 4, first, value)
                    tb[slot, plane, PAD + 8 * t : PAD + 8 * t + 8, :] = value

    steps, slots = (1, -1), range(len(x_steps))
    z_faces = [[z_face(s, dz) for dz in steps] for s in range(STAGES)]
    y_faces = [[y_face(g, dy) for dy in steps] for g in range(len(Y_GROUPS))]
    z_edges = [z_edge(dz, dy) for dz in steps for dy in steps]
    yz_edges = [yz_edge(dy, side) for dy in steps for side in (0, 1)]
    x_faces = [
        halo((dx, 0, 0), "x", GOT_X, tile.at[0], tb.at[slot, own_planes, own_rows, :])
        for slot, dx in enumerate(x_steps)
    ]
    xy_edges = [xy_edge(slot, dy) for slot in slots for dy in steps]
    xz_edges = [xz_edge(slot, dz) for slot in slots for dz in steps]

    def z_landed(s):
        landed(halo_recv.at[GOT_Z + s], xb.at[run_of(s, s + 1), pl.ds(0, 4), own_rows, :])

    def y_landed(g):
        landed(halo_recv.at[GOT_Y + g], xb.at[run_of(*Y_GROUPS[g]), own_planes, pl.ds(0, 4), :])

    every = pl.ds(0, len(x_steps))

    def x_landed():
        landed(halo_recv.at[GOT_X], tb.at[every, own_planes, own_rows, :])

    def edges_landed():
        landed(halo_recv.at[GOT_YZ], xb.at[mixed, pl.ds(0, 4), pl.ds(0, 4), :])
        landed(halo_recv.at[GOT_XY], tb.at[every, own_planes, pl.ds(0, 4), :])

    def halos_left():
        left(halo_send.at[SENT["z"]], xb.at[:, pl.ds(0, 4), pl.ds(0, rows + planes), :])
        left(halo_send.at[SENT["yz"]], xb.at[mixed, pl.ds(0, 4), pl.ds(0, 8), :])
        left(halo_send.at[SENT["x"]], tb.at[every, pl.ds(0, planes), pl.ds(0, rows + 4), :])
        left(halo_send.at[SENT["xz"]], qb.at[every, pl.ds(0, 4), packed_rows, :])

    def start(some):
        for copy in some:
            copy.start()

    loads = []
    place = 0
    for first, size in RUNS:
        loads.append(
            pltpu.make_async_copy(
                section.at[pl.ds(first, size)],
                xb.at[pl.ds(place, size), own_planes, own_rows, :],
                local_sem.at[0],
            )
        )
        place += size
    load_base = pltpu.make_async_copy(base, inputs.at[0], local_sem.at[1])
    load_accum = pltpu.make_async_copy(accum, inputs.at[1], local_sem.at[1])
    chained = gy > 2
    faces = [(0, 0, 1), (0, 0, -1)] + [(dx, 0, 0) for dx in x_steps]
    barrier = pltpu.get_barrier_semaphore()

    def greet(sem, delta):
        pl.semaphore_signal(sem, inc=1, device_id=device(*delta), device_id_type=MESH)

    for delta in faces + [(0, -1, 0)]:
        greet(barrier, delta)
    if chained:
        pl.when(j + 1 < gy)(lambda: greet(barrier, (0, 1, 0)))
    else:
        greet(barrier, (0, 1, 0))
    start(loads)
    load_base.start()
    load_accum.start()

    lane = lax.broadcasted_iota(jnp.int32, (rows, lanes), 1)

    own_cells = xb.at[:, own_planes, own_rows, :]
    pltpu.make_async_copy(own_cells, own_cells, local_sem.at[0]).wait()
    for plane in range(planes):
        packed = jnp.zeros((rows, lanes), jnp.float32)
        for field in range(fields):
            value = xb[PLACE[field], plane + 2, PAD : PAD + rows, :]
            ends = pltpu.roll(value, (4 * field + 2) % lanes, 1)
            packed = jnp.where((lane >> 2) == field, ends, packed)
        tile[0, plane] = packed
    if chained:
        pl.when(j == 0)(lambda: pl.semaphore_wait(barrier, len(faces) + 1))
        pl.when(j > 0)(lambda: pl.semaphore_wait(barrier, len(faces) + 2))
    else:
        pl.semaphore_wait(barrier, len(faces) + 2)
    def far(some):
        pl.when(j == 0)(lambda: start(some))

    def near(some):
        up, down = some[::2], some[1::2]
        start(up)
        pl.when(j > 0)(lambda: start(down))

    if not chained:
        near = start
    else:
        pl.when(j == gy - 2)(lambda: greet(chain, (0, -1, 0)))
    start(z_faces[0])
    near(y_faces[0])
    start(x_faces + z_edges + z_faces[1])
    near(y_faces[1])
    start(z_faces[2])
    near(y_faces[2])
    for s in range(3, EARLY):
        start(z_faces[s])
    if chained:
        @pl.when(j < gy - 2)
        def _():
            pl.semaphore_wait(chain, 1)
            pl.when(j > 0)(lambda: greet(chain, (0, -1, 0)))

        for faces_of in y_faces:
            far(faces_of[1::2])
    pltpu.make_async_copy(inputs, inputs, local_sem.at[1]).wait()

    own_y = pl.ds(pl.multiple_of(j * rows, rows), rows)
    own_x = pl.ds(pl.multiple_of(i * lanes, lanes), lanes)
    paired = gx == 2 and gy % 2 == 0
    turned = TURNED if paired else 0
    kept = STAGES - turned
    pair = j + 1 - 2 * lax.rem(j, 2)
    other = 1 - i
    towards = ((0, 1), (0, -1), (1, 0), (-1, 0))
    TURN, BULK, BULK_TURNED, PAIR_TURNED = ((gy - 1) * STAGES + n for n in range(4))
    SENT_PAIR, SENT_TURNED = 3, 4

    def piece(bi, bj, low, high):
        return slab.at[
            run_of(low, high),
            :,
            pl.ds(pl.multiple_of(bj * rows, rows), rows),
            pl.ds(pl.multiple_of(bi * lanes, lanes), lanes),
        ]

    def line(link, bi, bj, c, sent, got):
        dx, dy = towards[link]
        part = piece(bi, bj, c, c + 1)
        pltpu.make_async_remote_copy(
            src_ref=part,
            dst_ref=part,
            send_sem=line_send.at[sent],
            recv_sem=gather_recv.at[got],
            device_id=device(dx, dy, 0),
            device_id_type=MESH,
        ).start()

    def number(link, bi, bj, c):
        if paired:
            return (bj - link) * STAGES + c
        return (bi * gy + bj) * STAGES + c

    def send(link, bi, bj, c):
        line(link, bi, bj, c, link, number(link, bi, bj, c))

    def arrive(link, bi, bj, c):
        landed(gather_recv.at[number(link, bi, bj, c)], piece(bi, bj, c, c + 1))

    def x_links(body):
        @pl.when(i + 1 < gx)
        def _():
            body(2)

        @pl.when(i > 0)
        def _():
            body(3)

    def cross(bj, c, distance):
        if not paired:
            x_links(lambda link: send(link, i, bj, c))
        elif c < kept:
            if distance == 1:
                line(2, i, bj, c, jnp.where(bj == pair, SENT_PAIR, 2), BULK)
            else:
                line(2, i, bj, c, 2, BULK)
        elif distance == 0:
            line(2, i, bj, c, 2, TURN)
        elif distance == 1:
            pl.when(bj != pair)(lambda: line(2, i, bj, c, 2, BULK_TURNED))
        else:
            line(2, i, bj, c, 2, BULK_TURNED)

    def held(c, ahead):
        if c < kept:
            return False
        return (pair == j + ahead) & ((pair == 0) | (pair == gy - 1))

    def send_own(c):
        @pl.when((j + 1 < gy) & jnp.logical_not(held(c, 1)))
        def _():
            send(0, i, j, c)

        @pl.when((j > 0) & jnp.logical_not(held(c, -1)))
        def _():
            send(1, i, j, c)

        cross(j, c, 0)

    def send_held(c):
        def go(link, ahead):
            pl.when(held(c, ahead))(
                lambda: line(link, i, j, c, link, number(link, i, j, kept))
            )

        go(0, 1)
        go(1, -1)

    def pass_on(d, c, pairs=(False, True)):
        ended = d == 1 and c >= kept

        def below():
            bj = j - d
            arrive(0, i, bj, c)

            @pl.when(j + 1 < gy)
            def _():
                send(0, i, bj, c)

            cross(bj, c, d)

        def above():
            bj = j + d
            arrive(1, i, bj, c)

            @pl.when(j > 0)
            def _():
                send(1, i, bj, c)

            cross(bj, c, d)

        has_below = (j - d >= 0) & (j + 1 < gy) if ended else j - d >= 0
        has_above = (j + d < gy) & (j > 0) if ended else j + d < gy
        if d > 1:
            if True in pairs:
                pl.when(has_below)(below)
                pl.when(has_above)(above)
            return
        for is_pair in pairs:
            pl.when(has_below & ((pair < j) == is_pair))(below)
            pl.when(has_above & ((pair > j) == is_pair))(above)

    def turn():
        landed(gather_recv.at[TURN], piece(other, j, kept, STAGES))
        for c in range(kept, STAGES):
            @pl.when(pair > j)
            def _():
                line(0, other, j, c, SENT_TURNED, PAIR_TURNED)

            @pl.when(pair < j)
            def _():
                line(1, other, j, c, SENT_TURNED, PAIR_TURNED)

    def emit_at(plane):
        def emit(field, rate):
            moved = inputs[0, field, plane] + (0.5 * STEP_DT) * rate
            slab[PLACE[field], plane, own_y, own_x] = moved
            ns_out[field, plane] = moved
            na_out[field, plane] = inputs[1, field, plane] + (STEP_DT / 3.0) * rate

        return emit

    x_landed()
    start(xy_edges)
    pack_edges()
    start(xz_edges)
    for s in range(EARLY, STAGES - 2):
        start(z_faces[s])
    z_landed(0)
    work = [
        rates_of_plane(plane, rows, lanes, xb, tb, emit_at(plane))
        for plane in range(planes)
    ]

    def own_stage(s):
        if s:
            z_landed(s)
        else:
            landed(halo_recv.at[GOT_ZE], eb.at[mixed, pl.ds(0, 4), pl.ds(0, 4), :])
            start(yz_edges)
        if s < len(Y_GROUPS):
            y_landed(s)
        if s == MIX_STAGE:
            edges_landed()
        for part in work:
            next(part)
        send_own(s)
        if s < 2:
            start(z_faces[STAGES - 2 + s])
        if s == MIX_STAGE - 1:
            landed(halo_recv.at[GOT_XZ], qb.at[every, pl.ds(0, 4), packed_rows, :])
            unpack_edges()

    LAG = tuple(3 * d for d in range(gy))
    final = STAGES - 1 + LAG[gy - 2] + FINAL
    for v in range(STAGES + LAG[gy - 1]):
        if v < STAGES:
            own_stage(v)
        for d in range(1, gy):
            if 0 <= v - LAG[d] < STAGES:
                pass_on(d, v - LAG[d])
        for c in range(kept, STAGES):
            if v == final - (c == kept):
                send_held(c)
        if v == final and turned:
            turn()

    halos_left()

    def whole(n_rows, n_lanes, low=0, high=STAGES):
        return slab.at[run_of(low, high), :, pl.ds(0, n_rows), pl.ds(0, n_lanes)]

    if paired:
        if turned:
            landed(gather_recv.at[PAIR_TURNED], whole(rows, lanes, kept))

            for link, end in ((1, 0), (0, gy - 1)):
                @pl.when(j == end)
                def _():
                    slot = gather_recv.at[number(link, i, pair, kept)]
                    landed(slot, whole(rows, lanes, kept))
        landed(gather_recv.at[BULK], whole(gy * rows, lanes, 0, kept))
        if turned and gy > 2:
            landed(gather_recv.at[BULK_TURNED], whole((gy - 2) * rows, lanes, kept))
    else:
        for d in range(1, gx):
            def row(bj, carry, d=d):
                @pl.when(i - d >= 0)
                def _():
                    for c in range(STAGES):
                        arrive(2, i - d, bj, c)

                        @pl.when(i + 1 < gx)
                        def _():
                            send(2, i - d, bj, c)

                @pl.when(i + d < gx)
                def _():
                    for c in range(STAGES):
                        arrive(3, i + d, bj, c)

                        @pl.when(i > 0)
                        def _():
                            send(3, i + d, bj, c)

                return carry

            lax.fori_loop(0, gy, row, 0)

    for n in range(1, gy):
        @pl.when(j == n - 1)
        def _():
            left(line_send.at[0], whole(n * rows, lanes))

        @pl.when(j == gy - n)
        def _():
            left(line_send.at[1], whole(n * rows, lanes))

    if paired:
        left(line_send.at[2], whole((gy - 1) * rows, lanes))
        left(line_send.at[SENT_PAIR], whole(rows, lanes, 0, kept))
        if turned:
            left(line_send.at[SENT_TURNED], whole(rows, lanes, kept))
    else:
        for n in range(1, gx):
            @pl.when(i == n - 1)
            def _():
                left(line_send.at[2], whole(gy * rows, n * lanes))

            @pl.when(i == gx - n)
            def _():
                left(line_send.at[3], whole(gy * rows, n * lanes))


def put_out(ns_in, na_in, slab_in, ns_out, na_out, slab_out, sem):
    place = 0
    for first, size in RUNS:
        pltpu.make_async_copy(
            slab_in.at[pl.ds(place, size)], slab_out.at[pl.ds(first, size)], sem.at[0]
        ).start()
        place += size
    pltpu.make_async_copy(ns_in, ns_out, sem.at[1]).start()
    pltpu.make_async_copy(na_in, na_out, sem.at[2]).start()
    pltpu.make_async_copy(slab_in, slab_out, sem.at[0]).wait()
    pltpu.make_async_copy(ns_in, ns_out, sem.at[1]).wait()
    pltpu.make_async_copy(na_in, na_out, sem.at[2]).wait()


def shards(sizes, section, base, accum):
    gx, gy, gz = sizes
    fields, planes, rows, lanes = section.shape
    slots = 1 if gx == 2 else 2
    arrivals = (gy - 1) * STAGES + 4 if gx == 2 and gy % 2 == 0 else gx * gy * STAGES
    any_spec = pl.BlockSpec(memory_space=pl.ANY)
    block = jax.ShapeDtypeStruct(section.shape, jnp.float32)
    slab = jax.ShapeDtypeStruct((fields, planes, gy * rows, gx * lanes), jnp.float32)
    dma = pltpu.SemaphoreType.DMA
    staged = pl.pallas_call(
        functools.partial(section_kernel, sizes),
        out_shape=tuple(pltpu.VMEM(a.shape, a.dtype) for a in (block, block, slab)),
        in_specs=[pl.BlockSpec(memory_space=pltpu.HBM)] * 3,
        out_specs=(pl.BlockSpec(memory_space=pltpu.VMEM),) * 3,
        scratch_shapes=[
            pltpu.VMEM((fields, planes + 4, rows + 2 * PAD, lanes), jnp.float32),
            pltpu.VMEM((slots, planes + 4, rows + 2 * PAD, lanes), jnp.float32),
            pltpu.VMEM((MIXED_YZ, 4, 8, lanes), jnp.float32),
            pltpu.VMEM((slots, planes, 8, lanes), jnp.float32),
            pltpu.VMEM((slots, 4, 8, lanes), jnp.float32),
            pltpu.VMEM((1, planes, rows, lanes), jnp.float32),
            pltpu.VMEM((2,) + section.shape, jnp.float32),
            dma((2,)),
            dma((4,)),
            dma((STAGES + len(Y_GROUPS) + 5,)),
            dma((5,)),
            dma((arrivals,)),
            pltpu.SemaphoreType.REGULAR,
        ],
        compiler_params=pltpu.CompilerParams(collective_id=0, has_side_effects=True, vmem_limit_bytes=24 << 20),
    )(*(pltpu.with_memory_space_constraint(x, pltpu.HBM) for x in (section, base, accum)))
    return pl.pallas_call(
        put_out,
        out_shape=(block, block, slab),
        in_specs=[pl.BlockSpec(memory_space=pltpu.VMEM)] * 3,
        out_specs=(any_spec,) * 3,
        scratch_shapes=[dma((3,))],
        compiler_params=pltpu.CompilerParams(vmem_limit_bytes=8 << 20),
    )(*staged)


def solution(mesh):
    sizes = tuple(mesh.shape[name] for name in ("gx", "gy", "gz"))
    spec = P(None, "gz", "gy", "gx")
    return jax.shard_map(
        functools.partial(shards, sizes),
        mesh=mesh,
        in_specs=(spec, spec, spec),
        out_specs=(spec, spec, P(None, "gz", None, None)),
        check_vma=False,
    )
```
